256 devices in a mesh: grp: 2 (over x_hi), tile: 32 (over x_lo, z, core), mem: 4 (over y).
Axes of the slice: x: 4 (x_hi: 2, x_lo: 2; x = x_hi * 2 + x_lo), y: 4, z: 8, core: 2. Of those that a mesh axis runs over, the one named last changes fastest.
Arguments:
- ens_coarse: bfloat16 [2, 80, 128, 128, 128], P('grp', 'mem', None, 'tile'), may hold values from -6 to 6
- col_interp: bfloat16 [256, 128], replicated, may hold values from -0.5 to 0.5
- row_weights: bfloat16 [3, 256], replicated, may hold values from 0.099609375 to 0.8984375
- ctrl_vec: float32 [2, 128, 256, 256], P('grp', None, 'tile'), may hold values from -24 to 24
- band_loc: bfloat16 [256, 24], P('tile'), may hold values from -1.25 to 1.25
- row_loc: bfloat16 [256, 256], replicated, may hold values from -0.375 to 0.375
- level_loc: bfloat16 [128, 128], replicated, may hold values from -0.5 to 0.5
- hx_pert: bfloat16 [2, 80, 262144], P('grp', None, ('tile', 'mem')), may hold values from -3 to 3
- innov: float32 [2, 262144], P('grp', ('tile', 'mem')), may hold values from -48 to 48
- obs_prec: float32 [2, 262144], P('grp', ('tile', 'mem')), may hold values from 0.3 to 3
- obs_region: int32 [2, 262144], P('grp', ('tile', 'mem')), may hold values from 0 to 7
Outputs:
- increment: float32 [2, 128, 256, 256], P('grp', 'mem', 'tile')
- letkf_weights: float32 [256, 80], P('tile')
The draws below stay inside these ranges and needn't reach their ends.
Inputs may be any that keep to these rules, and one draw needn't show every extreme that they name: `obs_region`: the region of an observation among the 8 regions of its block of 8192 observations.
All inputs are finite; a program needn't handle non-finite values.
Results may differ from the reference program's by a relative error of at most 0.018.
Values may be sent and summed in bfloat16 or wider, within the bound.
A program may use at most 128 MiB of HBM per device.

```python
import math
import jax
import jax.numpy as jnp
from jax import lax

MEMBERS = 80
LEV = 128
NREG = 8
FCD = 8
TSLOTS = 2
CR = 128
FR = 256
FC = 256
CC = 128
NOBS = 262144
N_TILE = 32


def place_ends(drawn, own_key, low, largest):
    spot = [jax.random.randint(jax.random.fold_in(own_key, axis), (), 0, length) for axis, length in enumerate(drawn.shape)]
    widest = drawn.shape.index(max(drawn.shape))
    neighbour = spot[:widest] + [(spot[widest] + 1) % drawn.shape[widest]] + spot[widest + 1:]
    return drawn.at[tuple(spot)].set(low).at[tuple(neighbour)].set(largest)


def level_of(rng, extent, split, least, high):
    level = 1.0
    for dim, shards_of in split:
        draws = jax.random.uniform(jax.random.fold_in(jax.random.fold_in(rng, 6), dim), (shards_of,), jnp.float32, least / len(split), high / len(split))
        level = level * jnp.repeat(jnp.exp(draws), extent[dim] // shards_of).reshape((-1,) + (1,) * (len(extent) - 1 - dim))
    return level


def noise(stream_key, extent, width, limit, pieces=(), kind=jnp.bfloat16):
    values = width * jax.random.normal(stream_key, extent, jnp.float32)
    if pieces:
        values = values * level_of(stream_key, extent, pieces, -0.22, 0.18)
    return jnp.clip(values, -limit, limit).astype(kind)


def setup_inputs(seed: int = 0) -> dict:
    arg_keys = jax.random.split(jax.random.key(seed), 12)
    return {
        "ens_coarse": noise(arg_keys[0], (TSLOTS, MEMBERS, LEV, CR, CC), 1.0, 6.0, ((0, 2), (1, 4), (3, 32))),
        "col_interp": noise(arg_keys[1], (FC, CC), CC ** -0.5, 0.5),
        "row_weights": jnp.clip(jax.random.uniform(arg_keys[2], (3, FR), jnp.float32, 0.099609375, 0.8984375), 0.099609375, 0.8984375).astype(jnp.bfloat16),
        "ctrl_vec": noise(arg_keys[3], (TSLOTS, LEV, FC, FR), 4.0, 24.0, ((0, 2), (2, 32)), jnp.float32),
        "band_loc": noise(arg_keys[4], (FC, 3 * FCD), (3 * FCD) ** -0.5, 1.25, ((0, 32),)),
        "row_loc": noise(arg_keys[5], (FR, FR), FR ** -0.5, 0.375),
        "level_loc": noise(arg_keys[6], (LEV, LEV), LEV ** -0.5, 0.5),
        "hx_pert": noise(arg_keys[7], (TSLOTS, MEMBERS, NOBS), 0.5, 3.0, ((0, 2), (2, 128))),
        "innov": noise(arg_keys[8], (TSLOTS, NOBS), 8.0, 48.0, ((0, 2), (1, 128)), jnp.float32),
        "obs_prec": jnp.clip(jnp.exp(math.log(3.0) - 2.3025851 * jax.random.uniform(arg_keys[9], (TSLOTS, NOBS), jnp.float32) ** level_of(arg_keys[9], (TSLOTS, NOBS), ((0, 2), (1, 128)), -0.2, 0.2)), 0.3, 3.0),
        "obs_region": place_ends(jax.random.randint(arg_keys[10], (TSLOTS, NOBS), 0, NREG), jax.random.fold_in(arg_keys[10], 1), 0, NREG - 1).astype(jnp.int32),
    }


def to_half(value):
    return lax.optimization_barrier(value.astype(jnp.bfloat16))

def solve_weights(gram_sums, right_side):
    member_count = gram_sums.shape[-1]
    system = gram_sums + (member_count - 1) * jnp.eye(member_count, dtype=jnp.float32)
    factor = jnp.linalg.cholesky(system)
    halfway = lax.linalg.triangular_solve(factor, right_side[..., None], left_side=True, lower=True)
    result = lax.linalg.triangular_solve(factor, halfway, left_side=True, lower=True, transpose_a=True)
    return result[..., 0]

def fine_member(ens_member, col_interp, row_weights):
    coarse_cols = jnp.einsum('tlic,jc->tlij', ens_member.astype(jnp.float32), col_interp.astype(jnp.float32), precision=lax.Precision.HIGHEST)
    padded = jnp.pad(to_half(coarse_cols).astype(jnp.float32), ((0, 0), (0, 0), (1, 1), (0, 0)))
    fine_rows = row_weights.shape[1]
    parent_row = jnp.arange(fine_rows, dtype=jnp.int32) // 2
    weights = row_weights.astype(jnp.float32)
    running = jnp.zeros(padded.shape[:2] + (fine_rows, padded.shape[3]), jnp.float32)
    for offset in range(3):
        running = running + weights[offset][None, None, :, None] * jnp.take(padded, parent_row + offset, axis=2)
    return jnp.swapaxes(to_half(running), 2, 3)

def band_apply(projected, band_loc):
    levels, columns_all, rows_all = projected.shape
    band_width = band_loc.shape[1] // 3
    blocks = columns_all // band_width
    padded = jnp.pad(projected.astype(jnp.float32), ((0, 0), (band_width, band_width), (0, 0)))
    window_index = jnp.arange(blocks, dtype=jnp.int32)[:, None] * band_width + jnp.arange(3 * band_width, dtype=jnp.int32)[None, :]
    windows = jnp.take(padded, window_index, axis=1)
    band_table = band_loc.astype(jnp.float32).reshape(blocks, band_width, 3 * band_width)
    result = jnp.einsum('bjq,lbqr->lbjr', band_table, windows, precision=lax.Precision.HIGHEST)
    return to_half(result.reshape(levels, columns_all, rows_all))

def reference(ens_coarse, col_interp, row_weights, ctrl_vec, band_loc, row_loc, level_loc, hx_pert, innov, obs_prec, obs_region):
    members = ens_coarse.shape[1]
    row_table = row_loc.astype(jnp.float32)
    level_table = level_loc.astype(jnp.float32)

    def one_member(running, ens_member):
        refined = fine_member(ens_member, col_interp, row_weights)
        slot_term = to_half(refined.astype(jnp.float32) * ctrl_vec)
        projected = to_half(jnp.sum(slot_term.astype(jnp.float32), axis=0))
        banded = band_apply(projected, band_loc)
        row_mixed = to_half(jnp.einsum('ljs,rs->ljr', banded.astype(jnp.float32), row_table, precision=lax.Precision.HIGHEST))
        localized = to_half(jnp.einsum('lm,mjr->ljr', level_table, row_mixed.astype(jnp.float32), precision=lax.Precision.HIGHEST))
        return (running + refined.astype(jnp.float32) * localized.astype(jnp.float32)[None], None)
    running, unused = lax.scan(one_member, jnp.zeros(ctrl_vec.shape, jnp.float32), jnp.moveaxis(ens_coarse, 1, 0))
    increment = running / (members - 1)
    tile_count = N_TILE
    obs_tile = hx_pert.shape[2] // tile_count

    def one_tile(tile_index):
        obs_start = tile_index * obs_tile
        observed = lax.dynamic_slice_in_dim(hx_pert, obs_start, obs_tile, 2).astype(jnp.float32)
        precision_row = lax.dynamic_slice_in_dim(obs_prec, obs_start, obs_tile, 1)
        innovation = lax.dynamic_slice_in_dim(innov, obs_start, obs_tile, 1)
        region = lax.dynamic_slice_in_dim(obs_region, obs_start, obs_tile, 1)
        weighted = to_half(observed * precision_row[:, None, :]).astype(jnp.float32)
        labels = jnp.arange(NREG, dtype=jnp.int32)
        member_of = (region[:, None, :] == labels[None, :, None]).astype(jnp.float32)
        gram_sums = jnp.einsum('tko,tro,tjo->rkj', weighted, member_of, observed, precision=lax.Precision.HIGHEST)
        right_side = jnp.einsum('tko,tro,to->rk', weighted, member_of, innovation, precision=lax.Precision.HIGHEST)
        return solve_weights(gram_sums, right_side)
    weights = lax.map(one_tile, jnp.arange(tile_count, dtype=jnp.int32))
    return (increment, weights.reshape(tile_count * NREG, members))
```

```python
import functools

import jax
import jax.numpy as jnp
from jax import lax
from jax.experimental import pallas as pl
from jax.experimental.pallas import tpu as pltpu
from jax.sharding import Mesh, PartitionSpec as P

NREG = 8
BF = jnp.bfloat16
F32 = jnp.float32
GR = 16
WIN = 10


def spread_kernel(x_ref, ci_ref, o_ref):
    nb, rows, cols, lev = o_ref.shape[1], o_ref.shape[4], o_ref.shape[5], o_ref.shape[6]
    for i in range(rows):
        fine = lax.dot_general(
            ci_ref[...], x_ref[0, i], (((1,), (1,)), ((), ())), preferred_element_type=F32
        )
        o_ref[0, :, 0, 0, i] = fine.astype(BF).reshape(nb, cols, lev)


def window_start(group, coarse_rows):
    return min(max(group * GR // 2 - 1, 0), coarse_rows - WIN)


def refine_group(c_ref, s_ref, t, group, coarse):
    start = window_start(group, coarse)
    cols, lev = c_ref.shape[-2], c_ref.shape[-1]
    window = c_ref[t, pl.ds(start, WIN)].reshape(WIN * cols, lev)
    return jnp.dot(s_ref[group], window, preferred_element_type=F32)


def project_kernel(c_ref, s_ref, ctrl_ref, lo_ref, hi_ref):
    coarse, cols, lev = c_ref.shape[1:]
    half = cols // 2
    for group in range(s_ref.shape[0]):
        rows = pl.ds(group * GR, GR)
        total = None
        for t in range(2):
            fine = refine_group(c_ref, s_ref, t, group, coarse).astype(BF)
            term = fine.astype(F32).reshape(cols, GR, lev) * ctrl_ref[t, :, rows, :].astype(F32)
            total = term if total is None else total + term
        total = total.astype(BF)
        lo_ref[0, :, rows, :] = total[:half]
        hi_ref[0, :, rows, :] = total[half:]


def localize_kernel(
    c_ref, s_ref, lo_ref, hi_ref, left_ref, right_ref, band_ref, row_ref, lev_ref, o_ref, fine, banded, acc
):
    coarse, cols, lev = c_ref.shape[1:]
    k = pl.program_id(0)
    half = cols // 2

    for group in range(s_ref.shape[0]):
        rows = pl.ds(group * GR, GR)
        for t in range(2):
            fine[t, :, rows, :] = (
                refine_group(c_ref, s_ref, t, group, coarse).astype(BF).reshape(cols, GR, lev)
            )
        parts = [ref[0, :, rows, :].reshape(half * GR, lev) for ref in (left_ref, lo_ref, hi_ref, right_ref)]
        stacked = jnp.concatenate(parts, axis=0)
        mixed = jnp.dot(band_ref[...], stacked, preferred_element_type=F32)
        banded[:, rows, :] = mixed.astype(BF).reshape(cols, GR, lev)

    def column(j, carry):
        mixed = jnp.dot(row_ref[...], banded[j], preferred_element_type=F32).astype(BF)
        local = jnp.dot(mixed, lev_ref[...], preferred_element_type=F32)
        for t in range(2):
            term = fine[t, j].astype(F32) * local
            acc[t, j] = jnp.where(k == 0, term, acc[t, j] + term)
        return carry

    lax.fori_loop(0, cols, column, 0)

    @pl.when(k == pl.num_programs(0) - 1)
    def _():
        nl, cn, jn, ll = o_ref.shape[1:5]

        def flip(j, carry):
            for t in range(2):
                turned = acc[t, j].T
                for q in range(nl):
                    o_ref[t, q, j // jn, j % jn] = turned[q * ll : (q + 1) * ll].astype(o_ref.dtype)
            return carry

        lax.fori_loop(0, cols, flip, 0)


def row_stencils(row_weights, coarse_rows, cols):
    fine_rows = row_weights.shape[1]
    groups = fine_rows // GR
    weights = row_weights.reshape(3, groups, GR)
    starts = jnp.array([window_start(g, coarse_rows) for g in range(groups)])
    fine_row = jnp.arange(fine_rows).reshape(groups, GR)
    coarse_row = starts[:, None] + jnp.arange(WIN)[None, :]
    total = jnp.zeros((groups, GR, WIN), BF)
    for s in range(3):
        hit = coarse_row[:, None, :] == (fine_row // 2 + s - 1)[:, :, None]
        total = total + jnp.where(hit, weights[s][:, :, None], jnp.zeros((), BF))
    eye = jnp.eye(cols, dtype=BF)
    full = eye[None, :, None, None, :] * total[:, None, :, :, None]
    return full.reshape(groups, cols * GR, WIN * cols)


def band_matrix(band):
    cols, width = band.shape
    step = width // 3
    pieces = []
    for b in range(cols // step):
        rows = band[b * step : (b + 1) * step]
        pieces.append(jnp.pad(rows, ((0, 0), (b * step, cols - step - b * step))))
    full = jnp.concatenate(pieces, axis=0)
    eye = jnp.eye(GR, dtype=BF)
    big = full[:, None, :, None] * eye[None, :, None, :]
    return big.reshape(cols * GR, full.shape[1] * GR)


def solve_weights(gram_sums, right_side):
    member_count = gram_sums.shape[-1]
    system = gram_sums + (member_count - 1) * jnp.eye(member_count, dtype=F32)
    factor = jnp.linalg.cholesky(system)
    halfway = lax.linalg.triangular_solve(factor, right_side[..., None], left_side=True, lower=True)
    result = lax.linalg.triangular_solve(
        factor, halfway, left_side=True, lower=True, transpose_a=True
    )
    return result[..., 0]


def letkf(hx_pert, innov, obs_prec, obs_region):
    observed = hx_pert[0]
    members = observed.shape[0]
    weighted = (observed * obs_prec[0][None, :]).astype(BF)
    labels = lax.broadcasted_iota(jnp.int32, (NREG, observed.shape[1]), 0)
    member_of = obs_region[0][None, :] == labels
    masked = jnp.where(member_of[:, None, :], weighted[None], jnp.zeros((), BF))
    gram = jnp.einsum("rko,jo->rkj", masked, observed, preferred_element_type=F32)
    innov_rows = jnp.where(member_of, innov[0][None, :], 0.0)
    right = jnp.dot(innov_rows, weighted.astype(F32).T)
    packed = jnp.concatenate([gram.reshape(NREG, -1), right], axis=1)
    arrived = lax.all_to_all(packed[:, None], ("xh", "y"), split_axis=0, concat_axis=0, tiled=True)
    total = jnp.sum(arrived, axis=0)
    size = members * members
    own = solve_weights(total[:, :size].reshape(-1, members, members), total[:, size:])
    return lax.all_gather(own, ("xh", "y"), axis=0, tiled=True)


def body(
    ens_coarse,
    col_interp,
    row_weights,
    ctrl_vec,
    band_loc,
    row_loc,
    level_loc,
    hx_pert,
    innov,
    obs_prec,
    obs_region,
):
    nxh, nxl, nz, nc, ny = (lax.axis_size(a) for a in ("xh", "xl", "z", "c", "y"))
    _, members, lev, own_rows, coarse_cols = ens_coarse.shape
    fine_cols = col_interp.shape[0]
    fine_rows = row_weights.shape[1]
    blocks = nxl * nz
    cols = fine_cols // blocks
    group = members // (nxh * nc)
    tiles = nxl * nz * nc
    coarse = tiles * own_rows
    total_members = hx_pert.shape[1]

    by_row = jnp.transpose(ens_coarse[0], (0, 2, 1, 3))
    spread = pl.pallas_call(
        spread_kernel,
        grid=(members,),
        in_specs=[
            pl.BlockSpec((1, own_rows, lev, coarse_cols), lambda k: (k, 0, 0, 0)),
            pl.BlockSpec((fine_cols, coarse_cols), lambda k: (0, 0)),
        ],
        out_specs=pl.BlockSpec(
            (1, blocks, 1, 1, own_rows, cols, lev),
            lambda k: (k // (nc * group), 0, (k // group) % nc, k % group, 0, 0, 0),
        ),
        out_shape=jax.ShapeDtypeStruct((nxh, blocks, nc, group, own_rows, cols, lev), BF),
        compiler_params=pltpu.CompilerParams(dimension_semantics=("arbitrary",)),
        cost_estimate=pl.CostEstimate(flops=2 * members * own_rows * lev * coarse_cols * fine_cols, bytes_accessed=8000000, transcendentals=0),
    )(by_row, col_interp)
    spread = spread.reshape(nxh * tiles, group, own_rows, cols, lev)
    arrived = lax.all_to_all(spread, ("xh", "xl", "z", "c"), split_axis=0, concat_axis=0, tiled=True)
    arrived = arrived.reshape(nxh, tiles, group, own_rows, cols, lev)

    turned = jnp.transpose(ctrl_vec[0].astype(BF), (1, 2, 0))
    ctrl = lax.all_gather(turned, ("xh", "c"), axis=0)
    ctrl = ctrl.reshape(nxh, cols, fine_rows, lev)
    band = lax.all_gather(band_loc, "c", axis=0, tiled=True)

    stencils = row_stencils(row_weights, coarse, cols)
    band_full = band_matrix(band)
    lev_t = level_loc.T

    half = cols // 2
    field = jax.ShapeDtypeStruct((group, half, fine_rows, lev), BF)
    field_spec = pl.BlockSpec((1, half, fine_rows, lev), lambda k: (k, 0, 0, 0))
    c_spec = pl.BlockSpec((nxh, tiles, 1, own_rows, cols, lev), lambda k: (0, 0, k, 0, 0, 0))
    params = pltpu.CompilerParams(dimension_semantics=("arbitrary",), vmem_limit_bytes=56 << 20)

    def whole(a):
        return pl.BlockSpec(a.shape, lambda k, n=a.ndim: (0,) * n)

    def flat(c_ref):
        return c_ref.reshape(nxh, coarse, cols, lev)

    def project(c_ref, *rest):
        project_kernel(flat(c_ref), *rest)

    def localize(c_ref, *rest):
        localize_kernel(flat(c_ref), *rest)

    lo, hi = pl.pallas_call(
        project,
        grid=(group,),
        in_specs=[c_spec, whole(stencils), whole(ctrl)],
        out_specs=[field_spec, field_spec],
        out_shape=[field, field],
        compiler_params=params,
    )(arrived, stencils, ctrl)

    up = [(i, i + 1) for i in range(blocks - 1)]
    down = [(i + 1, i) for i in range(blocks - 1)]
    left = lax.ppermute(hi, ("xl", "z"), up)
    right = lax.ppermute(lo, ("xl", "z"), down)

    partial = pl.pallas_call(
        localize,
        grid=(group,),
        in_specs=[c_spec, whole(stencils)]
        + [field_spec] * 4
        + [whole(band_full), whole(row_loc), whole(lev_t)],
        out_specs=pl.BlockSpec(
            (nxh, ny, nc, cols // nc, lev // ny, fine_rows), lambda k: (0, 0, 0, 0, 0, 0)
        ),
        out_shape=jax.ShapeDtypeStruct((nxh, ny, nc, cols // nc, lev // ny, fine_rows), BF),
        scratch_shapes=[
            pltpu.VMEM((nxh, cols, fine_rows, lev), BF),
            pltpu.VMEM((cols, fine_rows, lev), BF),
            pltpu.VMEM((nxh, cols, fine_rows, lev), F32),
        ],
        compiler_params=params,
    )(arrived, stencils, lo, hi, left, right, band_full, row_loc, lev_t)
    partial = partial.reshape(nxh * ny * nc, cols // nc, lev // ny, fine_rows)
    pieces = lax.all_to_all(partial, ("xh", "y", "c"), split_axis=0, concat_axis=0, tiled=True)
    increment = jnp.sum(pieces.astype(F32), axis=0) / (total_members - 1)
    increment = jnp.transpose(increment, (1, 0, 2))

    weights = letkf(hx_pert, innov, obs_prec, obs_region)
    return (increment[None], weights)


def solution(mesh):
    shape = (2, 2, mesh.shape["tile"] // 4, 2, mesh.shape["mem"])
    fine_mesh = Mesh(mesh.devices.reshape(shape), ("xh", "xl", "z", "c", "y"))
    tile = ("xl", "z", "c")
    obs = (*tile, "y")
    placed = (
        P("xh", "y", None, tile, None),
        P(),
        P(),
        P("xh", None, tile, None),
        P(tile, None),
        P(),
        P(),
        P("xh", None, obs),
        P("xh", obs),
        P("xh", obs),
        P("xh", obs),
    )
    return jax.shard_map(
        body,
        mesh=fine_mesh,
        in_specs=placed,
        out_specs=(P("xh", "y", tile, None), P(tile, None)),
        check_vma=False,
    )
```

```python
import functools

import jax
import jax.numpy as jnp
from jax import lax
from jax.experimental import pallas as pl
from jax.experimental.pallas import tpu as pltpu
from jax.sharding import Mesh, PartitionSpec as P

NREG = 8
BF = jnp.bfloat16
F32 = jnp.float32
GR = 16
WIN = 10


def from_everyone(value, axes):
    copies = jnp.broadcast_to(value, (lax.axis_size(axes), *value.shape))
    return lax.all_to_all(copies, axes, split_axis=0, concat_axis=0, tiled=True)


MESH = pl.DeviceIdType.MESH


def one_hot(shape, of_row, of_col):
    row = lax.broadcasted_iota(jnp.int32, shape, 0)
    col = lax.broadcasted_iota(jnp.int32, shape, 1)
    return (of_row(row) == of_col(col)).astype(BF)


def window_start(group, coarse_rows):
    return min(max(group * GR // 2 - 1, 0), coarse_rows - WIN)


def main_kernel(sizes, refs):
    nxh, nxl, nz, nc, ny, scale = sizes
    x_ref, ci_ref, rwt_ref, cq_ref, band_ref, row_ref, lev_ref, o_ref, *refs = refs
    perm, sent, land, sten, stage, ctrl, bands, bandf, field, halo, fine, banded, acc, *refs = refs
    parts, sums, total, moved, *sems = refs
    (s_go, s_in, h_go, h_in, c_go, c_in, f_go, f_in, b_go, b_in, p_go, p_in, m_go, m_in) = sems

    nk, ndest, own_rows, cols, lev = sent.shape
    coarse = land.shape[2]
    groups = sten.shape[0]
    half = cols // 2
    blocks = nz * nc
    xh, xl, z, c, y = (lax.axis_index(a) for a in ("xh", "xl", "z", "c", "y"))
    block = z * nc + c
    tile = xl * blocks + block
    me = (xh * nxl + xl) * blocks + block
    team = (xh * nxl + xl) * ny + y

    def at_dest(d):
        m, b = d // blocks, d % blocks
        return {"xh": m // nxl, "xl": m % nxl, "z": b // nc, "c": b % nc}

    def at_team(p):
        m = p // ny
        return {"xh": m // nxl, "xl": m % nxl, "y": p % ny}

    barrier = pltpu.get_barrier_semaphore()

    def greet(n, carry):
        pl.semaphore_signal(
            barrier, inc=1, device_id=at_dest((me + n) % ndest), device_id_type=MESH
        )
        return carry

    lax.fori_loop(1, ndest, greet, 0)
    nteam = nxh * nxl * ny

    def greet_team(n, carry):
        p = (team + n) % nteam

        @pl.when(p % ny != y)
        def _():
            pl.semaphore_signal(barrier, inc=1, device_id=at_team(p), device_id_type=MESH)

        return carry

    lax.fori_loop(1, nteam, greet_team, 0)

    flat = own_rows * lev
    perm[...] = one_hot(
        (flat, flat), lambda p: (p % lev) * own_rows + p // lev, lambda q: q
    )

    def spread(k, carry):
        def group_of(m, carry):
            by_row = jnp.dot(
                perm[...], x_ref[m * nk + k], preferred_element_type=F32
            ).astype(BF)
            out = lax.dot_general(
                ci_ref[...], by_row, (((1,), (1,)), ((), ())), preferred_element_type=F32
            ).astype(BF)
            for i in range(own_rows):
                sent[k, pl.ds(m * blocks, blocks), i] = out[:, i * lev : (i + 1) * lev].reshape(
                    blocks, cols, lev
                )
            return carry

        return lax.fori_loop(0, nxh * nxl, group_of, carry)

    def send(k):
        def one(n, carry):
            d = (me + n) % ndest
            pltpu.make_async_remote_copy(
                src_ref=sent.at[k, d],
                dst_ref=land.at[k, xh, pl.ds(tile * own_rows, own_rows)],
                send_sem=s_go.at[k],
                recv_sem=s_in.at[k],
                device_id=at_dest(d),
                device_id_type=MESH,
            ).start()
            return carry

        lax.fori_loop(1, ndest, one, 0)
        land[k, xh, pl.ds(tile * own_rows, own_rows)] = sent[k, me]

    def wait_bytes(ref, sem):
        pltpu.make_async_copy(ref, ref, sem).wait()

    spread(0, 0)
    pl.semaphore_wait(barrier, ndest - 1 + nteam - nxh * nxl)

    to_xl, to_z, to_c = c, (xl * nz + z) // nc, (xl * nz + z) % nc
    home = (to_xl == xl) & (to_z == z) & (to_c == c)
    quarter = pltpu.make_async_remote_copy(
        src_ref=cq_ref,
        dst_ref=stage,
        send_sem=c_go,
        recv_sem=c_in,
        device_id={"xl": to_xl, "z": to_z, "c": to_c},
        device_id_type=MESH,
    )

    @pl.when(jnp.logical_not(home))
    def _():
        quarter.start()

    @pl.when(home)
    def _():
        stage[...] = cq_ref[...]

    for side in range(nxl):
        here = (to_z == z) & (to_c == c) & (xl == side)

        @pl.when(jnp.logical_not(here))
        def _():
            pltpu.make_async_remote_copy(
                src_ref=band_ref,
                dst_ref=bands.at[c],
                send_sem=b_go.at[side],
                recv_sem=b_in.at[c],
                device_id={"xl": side, "z": to_z, "c": to_c},
                device_id_type=MESH,
            ).start()

        @pl.when(here)
        def _():
            bands[c] = band_ref[...]

    send(0)
    spread(1, 0)
    send(1)

    @pl.when(jnp.logical_not(home))
    def _():
        quarter.wait()

    quarter_cols = cq_ref.shape[0]
    slot = xh * cols + xl * half + y * quarter_cols

    def forward(n, carry):
        p = (team + n) % nteam
        pltpu.make_async_remote_copy(
            src_ref=stage,
            dst_ref=ctrl.at[pl.ds(slot, quarter_cols)],
            send_sem=f_go,
            recv_sem=f_in,
            device_id=at_team(p),
            device_id_type=MESH,
        ).start()
        return carry

    lax.fori_loop(1, nteam, forward, 0)
    ctrl[pl.ds(slot, quarter_cols)] = stage[...]
    lax.fori_loop(2, nk, spread, 0)

    span = WIN * cols
    p_id = lax.broadcasted_iota(jnp.int32, (cols * GR, span), 0)
    q_id = lax.broadcasted_iota(jnp.int32, (cols * GR, span), 1)
    same = q_id % cols == p_id // GR

    def stencil(g, carry):
        take = (
            lax.broadcasted_iota(jnp.int32, (cols * GR, groups * GR), 1)
            == lax.broadcasted_iota(jnp.int32, (cols * GR, groups * GR), 0) % GR + g * GR
        ).astype(BF)
        w = jnp.dot(take, rwt_ref[...], preferred_element_type=F32)
        start = jnp.minimum(jnp.maximum(g * (GR // 2) - 1, 0), coarse - WIN)
        full = jnp.zeros((cols * GR, span), F32)
        for s in range(3):
            wanted = g * (GR // 2) - start + (p_id % GR) // 2 + s - 1
            full = jnp.where(same & (q_id // cols == wanted), w[:, s : s + 1], full)
        sten[g] = full.astype(BF)
        return carry

    lax.fori_loop(0, groups, stencil, 0)

    for side in range(2):
        here = (xl == block // nz) & (z == block % nz) & (c == side)

        @pl.when(jnp.logical_not(here))
        def _():
            wait_bytes(bands.at[side], b_in.at[side])

    narrow = jnp.concatenate(
        [bands[0], pltpu.roll(bands[1], half, 1)], axis=0
    ).astype(BF)
    wide_src = 4 * half * GR
    take_src = one_hot((narrow.shape[1], wide_src), lambda m: m, lambda q: q // GR)
    take_col = one_hot((cols * GR, cols), lambda p: p // GR, lambda j: j)
    wide = jnp.dot(narrow, take_src, preferred_element_type=F32).astype(BF)
    full = jnp.dot(take_col, wide, preferred_element_type=F32)
    p_id2 = lax.broadcasted_iota(jnp.int32, full.shape, 0)
    q_id2 = lax.broadcasted_iota(jnp.int32, full.shape, 1)
    bandf[...] = jnp.where(p_id2 % GR == q_id2 % GR, full, 0.0).astype(BF)

    acc[...] = jnp.zeros_like(acc)

    def refine_group(k, group):
        start = window_start(group, coarse)
        windows = [land[k, t, pl.ds(start, WIN)].reshape(WIN * cols, lev) for t in range(2)]
        out = jnp.dot(
            sten[group], jnp.concatenate(windows, axis=1), preferred_element_type=F32
        ).astype(BF)
        return [out[:, t * lev : (t + 1) * lev].reshape(cols, GR, lev) for t in range(2)]

    def project(k):
        for group in range(groups):
            rows = pl.ds(group * GR, GR)
            first, second = refine_group(k, group)
            both = first.astype(F32) * ctrl[pl.ds(0, cols), rows, :].astype(F32)
            both = both + second.astype(F32) * ctrl[pl.ds(cols, cols), rows, :].astype(F32)
            both = both.astype(BF)
            field[k, 0, :, rows, :] = both[:half]
            field[k, 1, :, rows, :] = both[half:]

    def halo_copy(k, side):
        other = block + 1 if side == 0 else block - 1
        return pltpu.make_async_remote_copy(
            src_ref=field.at[k, 1 - side],
            dst_ref=halo.at[k, side],
            send_sem=h_go.at[k, side],
            recv_sem=h_in.at[k, side],
            device_id={"z": other // nc, "c": other % nc},
            device_id_type=MESH,
        )

    sends = (block < blocks - 1, block > 0)
    gets = (block > 0, block < blocks - 1)

    def localize(k):
        for side in range(2):

            @pl.when(gets[side])
            def _():
                wait_bytes(halo.at[k, side], h_in.at[k, side])

            @pl.when(jnp.logical_not(gets[side]))
            def _():
                halo[k, side] = jnp.zeros(halo.shape[2:], BF)

        for group in range(groups):
            rows = pl.ds(group * GR, GR)
            for t, part in enumerate(refine_group(k, group)):
                fine[t, :, rows, :] = part
        for group in range(0, groups, 2):
            sides = []
            for g in (group, group + 1):
                rows = pl.ds(g * GR, GR)
                pieces = [
                    ref[:, rows, :].reshape(half * GR, lev)
                    for ref in (halo.at[k, 0], field.at[k, 0], field.at[k, 1], halo.at[k, 1])
                ]
                sides.append(jnp.concatenate(pieces, axis=0))
            mixed = jnp.dot(
                bandf[...], jnp.concatenate(sides, axis=1), preferred_element_type=F32
            ).astype(BF)
            for n, g in enumerate((group, group + 1)):
                banded[:, pl.ds(g * GR, GR), :] = mixed[:, n * lev : (n + 1) * lev].reshape(
                    cols, GR, lev
                )
        for j in range(0, cols, 2):
            pair = jnp.concatenate([banded[j], banded[j + 1]], axis=1)
            mixed = jnp.dot(row_ref[...], pair, preferred_element_type=F32).astype(BF)
            local = jnp.dot(mixed, lev_ref[...], preferred_element_type=F32)
            for n in range(2):
                part = local[:, n * lev : (n + 1) * lev]
                for t in range(2):
                    acc[t, j + n] += fine[t, j + n].astype(F32) * part

    def wait_all_but_one(k, sem):
        wait_bytes(sent.at[k, pl.ds(0, ndest - 1)], sem.at[k])

    def step(k, carry):
        @pl.when(k < nk)
        def _():
            wait_all_but_one(k, s_in)

            @pl.when(k == 0)
            def _():
                wait_bytes(ctrl.at[pl.ds(0, (nteam - 1) * quarter_cols)], f_in)

            project(k)
            for side in range(2):

                @pl.when(sends[side])
                def _():
                    halo_copy(k, side).start()

            @pl.when(k + 2 < nk)
            def _():
                send(k + 2)

        @pl.when(k >= 1)
        def _():
            localize(k - 1)

        return carry

    lax.fori_loop(0, nk + 1, step, 0)

    nl, ll = ny, lev // ny

    def flip(j, carry):
        for t in range(2):
            turned = acc[t, j].T.astype(BF)
            for q in range(nl):
                parts[(t * nxl + j // half) * ny + q, j % half] = turned[q * ll : (q + 1) * ll]
        return carry

    lax.fori_loop(0, cols, flip, 0)

    def hand_over(n, carry):
        p = (team + n) % nteam
        pltpu.make_async_remote_copy(
            src_ref=parts.at[p],
            dst_ref=sums.at[team],
            send_sem=p_go,
            recv_sem=p_in,
            device_id=at_team(p),
            device_id_type=MESH,
        ).start()
        return carry

    lax.fori_loop(1, nteam, hand_over, 0)
    sums[team] = parts[team]
    wait_bytes(sums.at[pl.ds(0, nteam - 1)], p_in)
    for j in range(half):
        value = sums[0, j].astype(F32)
        for p in range(1, nteam):
            value = value + sums[p, j].astype(F32)
        total[j] = value * scale

    from_c, from_block = xl, (z * nc + c)
    dest = (tile * 2) % (blocks * nxl) + xl
    d_block = dest % blocks
    stays = dest == tile
    move = pltpu.make_async_remote_copy(
        src_ref=total,
        dst_ref=moved,
        send_sem=m_go,
        recv_sem=m_in,
        device_id={"xl": dest // blocks, "z": d_block // nc, "c": d_block % nc},
        device_id_type=MESH,
    )

    @pl.when(jnp.logical_not(stays))
    def _():
        move.start()

    @pl.when(stays)
    def _():
        moved[...] = total[...]

    def left(k, carry):
        wait_all_but_one(k, s_go)
        for side in range(2):

            @pl.when(sends[side])
            def _():
                wait_bytes(field.at[k, side], h_go.at[k, side])

        return carry

    lax.fori_loop(0, nk, left, 0)
    wait_bytes(ctrl.at[pl.ds(0, (nteam - 1) * quarter_cols)], f_go)
    wait_bytes(sums.at[pl.ds(0, nteam - 1)], p_go)
    for side in range(nxl):
        here = (to_z == z) & (to_c == c) & (xl == side)

        @pl.when(jnp.logical_not(here))
        def _():
            wait_bytes(bands.at[side], b_go.at[side])

    @pl.when(jnp.logical_not(stays))
    def _():
        move.wait()

    o_ref[...] = moved[...]


def solve_weights(gram_sums, right_side):
    member_count = gram_sums.shape[-1]
    system = gram_sums + (member_count - 1) * jnp.eye(member_count, dtype=F32)
    factor = jnp.linalg.cholesky(system)
    halfway = lax.linalg.triangular_solve(factor, right_side[..., None], left_side=True, lower=True)
    result = lax.linalg.triangular_solve(
        factor, halfway, left_side=True, lower=True, transpose_a=True
    )
    return result[..., 0]


def letkf(hx_pert, innov, obs_prec, obs_region):
    observed = hx_pert[0]
    members = observed.shape[0]
    weighted = (observed * obs_prec[0][None, :]).astype(BF)
    labels = lax.broadcasted_iota(jnp.int32, (NREG, observed.shape[1]), 0)
    member_of = obs_region[0][None, :] == labels
    masked = jnp.where(member_of[:, None, :], weighted[None], jnp.zeros((), BF))
    gram = jnp.einsum("rko,jo->rkj", masked, observed, preferred_element_type=F32)
    innov_rows = jnp.where(member_of, innov[0][None, :], 0.0)
    right = jnp.dot(innov_rows, weighted.astype(F32).T)
    packed = jnp.concatenate([gram.reshape(NREG, -1), right], axis=1)
    arrived = lax.all_to_all(packed[:, None], ("xh", "y"), split_axis=0, concat_axis=0, tiled=True)
    total = jnp.sum(arrived, axis=0)
    size = members * members
    own = solve_weights(total[:, :size].reshape(-1, members, members), total[:, size:])
    everyone = from_everyone(own, ("xh", "y"))
    return everyone.reshape(NREG, members)


def body(
    ens_coarse,
    col_interp,
    row_weights,
    ctrl_vec,
    band_loc,
    row_loc,
    level_loc,
    hx_pert,
    innov,
    obs_prec,
    obs_region,
):
    nxh, nxl, nz, nc, ny = (lax.axis_size(a) for a in ("xh", "xl", "z", "c", "y"))
    _, members, lev, own_rows, coarse_cols = ens_coarse.shape
    fine_cols = col_interp.shape[0]
    fine_rows = row_weights.shape[1]
    blocks = nz * nc
    cols = fine_cols // blocks
    half = cols // 2
    group = members // (nxh * nxl)
    tiles = nxl * blocks
    coarse = tiles * own_rows
    total_members = hx_pert.shape[1]
    nteam = nxh * nxl * ny
    quarter = half // ny

    x = ens_coarse.reshape(members, lev * own_rows, coarse_cols)
    rwt = jnp.pad(row_weights.T, ((0, 0), (0, 125)))
    mine = lax.dynamic_slice_in_dim(ctrl_vec[0], lax.axis_index("y") * quarter, quarter, 1)
    mine = jnp.transpose(mine.astype(BF), (1, 2, 0))
    band = jnp.pad(band_loc.astype(F32), ((0, 0), (0, 128 - band_loc.shape[1])))
    none = jnp.zeros_like(level_loc)
    lev_two = jnp.block([[level_loc.T, none], [none, level_loc.T]])

    vm = pl.BlockSpec(memory_space=pltpu.VMEM)
    dma = pltpu.SemaphoreType.DMA
    increment = pl.pallas_call(
        lambda *refs: main_kernel((nxh, nxl, nz, nc, ny, 1.0 / (total_members - 1)), refs),
        in_specs=[vm] * 7,
        out_specs=vm,
        out_shape=jax.ShapeDtypeStruct((half, lev // ny, fine_rows), F32),
        scratch_shapes=[
            pltpu.VMEM((own_rows * lev, own_rows * lev), BF),
            pltpu.VMEM((group, nxh * tiles, own_rows, cols, lev), BF),
            pltpu.VMEM((group, nxh, coarse, cols, lev), BF),
            pltpu.VMEM((fine_rows // GR, cols * GR, WIN * cols), BF),
            pltpu.VMEM((quarter, fine_rows, lev), BF),
            pltpu.VMEM((nxh * cols, fine_rows, lev), BF),
            pltpu.VMEM((2, *band.shape), F32),
            pltpu.VMEM((cols * GR, 4 * half * GR), BF),
            pltpu.VMEM((group, 2, half, fine_rows, lev), BF),
            pltpu.VMEM((group, 2, half, fine_rows, lev), BF),
            pltpu.VMEM((nxh, cols, fine_rows, lev), BF),
            pltpu.VMEM((cols, fine_rows, lev), BF),
            pltpu.VMEM((nxh, cols, fine_rows, lev), F32),
            pltpu.VMEM((nteam, half, lev // ny, fine_rows), BF),
            pltpu.VMEM((nteam, half, lev // ny, fine_rows), BF),
            pltpu.VMEM((half, lev // ny, fine_rows), F32),
            pltpu.VMEM((half, lev // ny, fine_rows), F32),
            dma((group,)),
            dma((group,)),
            dma((group, 2)),
            dma((group, 2)),
            dma,
            dma,
            dma,
            dma,
            dma((2,)),
            dma((2,)),
            dma,
            dma,
            dma,
            dma,
        ],
        compiler_params=pltpu.CompilerParams(
            collective_id=0, has_side_effects=True, vmem_limit_bytes=62 << 20
        ),
    )(x, col_interp, rwt, mine, band, row_loc, lev_two)
    increment = jnp.transpose(increment, (1, 0, 2))
    weights = letkf(hx_pert, innov, obs_prec, obs_region)
    return (increment[None], weights)


def solution(mesh):
    shape = (2, 2, mesh.shape["tile"] // 4, 2, mesh.shape["mem"])
    fine_mesh = Mesh(mesh.devices.reshape(shape), ("xh", "xl", "z", "c", "y"))
    tile = ("xl", "z", "c")
    obs = (*tile, "y")
    placed = (
        P("xh", "y", None, tile, None),
        P(),
        P(),
        P("xh", None, tile, None),
        P(tile, None),
        P(),
        P(),
        P("xh", None, obs),
        P("xh", obs),
        P("xh", obs),
        P("xh", obs),
    )
    return jax.shard_map(
        body,
        mesh=fine_mesh,
        in_specs=placed,
        out_specs=(P("xh", "y", tile, None), P(tile, None)),
        check_vma=False,
    )
```

```python
import functools

import jax
import jax.numpy as jnp
from jax import lax
from jax.experimental import pallas as pl
from jax.experimental.pallas import tpu as pltpu
from jax.sharding import Mesh, PartitionSpec as P

NREG = 8
BF = jnp.bfloat16
F32 = jnp.float32
GR = 16
WIN = 10


MESH = pl.DeviceIdType.MESH


def one_hot(shape, of_row, of_col):
    row = lax.broadcasted_iota(jnp.int32, shape, 0)
    col = lax.broadcasted_iota(jnp.int32, shape, 1)
    return (of_row(row) == of_col(col)).astype(BF)


def window_start(group, coarse_rows):
    return min(max(group * GR // 2 - 1, 0), coarse_rows - WIN)


def main_kernel(sizes, refs):
    nxh, nxl, nz, nc, ny, scale = sizes
    x_ref, ci_ref, rwt_ref, cq_ref, band_ref, row_ref, lev_ref, *refs = refs
    hx_ref, innov_ref, prec_ref, region_ref, o_ref, w_ref, *refs = refs
    perm, sent, land, sten, stage, ctrl, bands, bandf, field, halo, fine, banded, acc, *refs = refs
    parts, sums, total, moved, gram, grams, system, answer, answers, *sems = refs
    s_go, s_in, h_go, h_in, c_go, c_in, f_go, f_in, b_go, b_in, p_go, p_in, m_go, m_in, *sems = sems
    g_go, g_in, w_go, w_in = sems

    nk, ndest, own_rows, cols, lev = sent.shape
    coarse = land.shape[2]
    groups = sten.shape[0]
    half = cols // 2
    blocks = nz * nc
    xh, xl, z, c, y = (lax.axis_index(a) for a in ("xh", "xl", "z", "c", "y"))
    block = z * nc + c
    tile = xl * blocks + block
    me = (xh * nxl + xl) * blocks + block
    team = (xh * nxl + xl) * ny + y

    def at_dest(d):
        m, b = d // blocks, d % blocks
        return {"xh": m // nxl, "xl": m % nxl, "z": b // nc, "c": b % nc}

    def at_team(p):
        m = p // ny
        return {"xh": m // nxl, "xl": m % nxl, "y": p % ny}

    barrier = pltpu.get_barrier_semaphore()

    def greet(n, carry):
        pl.semaphore_signal(
            barrier, inc=1, device_id=at_dest((me + n) % ndest), device_id_type=MESH
        )
        return carry

    lax.fori_loop(1, ndest, greet, 0)
    nteam = nxh * nxl * ny

    def greet_team(n, carry):
        p = (team + n) % nteam

        @pl.when(p % ny != y)
        def _():
            pl.semaphore_signal(barrier, inc=1, device_id=at_team(p), device_id_type=MESH)

        return carry

    lax.fori_loop(1, nteam, greet_team, 0)

    flat = own_rows * lev
    perm[...] = one_hot(
        (flat, flat), lambda p: (p % lev) * own_rows + p // lev, lambda q: q
    )

    def spread(k, carry):
        def group_of(m, carry):
            by_row = jnp.dot(
                perm[...], x_ref[m * nk + k], preferred_element_type=F32
            ).astype(BF)
            out = lax.dot_general(
                ci_ref[...], by_row, (((1,), (1,)), ((), ())), preferred_element_type=F32
            ).astype(BF)
            for i in range(own_rows):
                sent[k, pl.ds(m * blocks, blocks), i] = out[:, i * lev : (i + 1) * lev].reshape(
                    blocks, cols, lev
                )
            return carry

        return lax.fori_loop(0, nxh * nxl, group_of, carry)

    def send(k):
        def one(n, carry):
            d = (me + n) % ndest
            pltpu.make_async_remote_copy(
                src_ref=sent.at[k, d],
                dst_ref=land.at[k, xh, pl.ds(tile * own_rows, own_rows)],
                send_sem=s_go.at[k],
                recv_sem=s_in.at[k],
                device_id=at_dest(d),
                device_id_type=MESH,
            ).start()
            return carry

        lax.fori_loop(1, ndest, one, 0)
        land[k, xh, pl.ds(tile * own_rows, own_rows)] = sent[k, me]

    def wait_bytes(ref, sem):
        pltpu.make_async_copy(ref, ref, sem).wait()

    spread(0, 0)
    pl.semaphore_wait(barrier, ndest - 1 + nteam - nxh * nxl)

    to_xl, to_z, to_c = c, (xl * nz + z) // nc, (xl * nz + z) % nc
    home = (to_xl == xl) & (to_z == z) & (to_c == c)
    quarter = pltpu.make_async_remote_copy(
        src_ref=cq_ref,
        dst_ref=stage,
        send_sem=c_go,
        recv_sem=c_in,
        device_id={"xl": to_xl, "z": to_z, "c": to_c},
        device_id_type=MESH,
    )

    @pl.when(jnp.logical_not(home))
    def _():
        quarter.start()

    @pl.when(home)
    def _():
        stage[...] = cq_ref[...]

    for side in range(nxl):
        here = (to_z == z) & (to_c == c) & (xl == side)

        @pl.when(jnp.logical_not(here))
        def _():
            pltpu.make_async_remote_copy(
                src_ref=band_ref,
                dst_ref=bands.at[c],
                send_sem=b_go.at[side],
                recv_sem=b_in.at[c],
                device_id={"xl": side, "z": to_z, "c": to_c},
                device_id_type=MESH,
            ).start()

        @pl.when(here)
        def _():
            bands[c] = band_ref[...]

    send(0)
    spread(1, 0)
    send(1)

    @pl.when(jnp.logical_not(home))
    def _():
        quarter.wait()

    quarter_cols = cq_ref.shape[0]
    slot = xh * cols + xl * half + y * quarter_cols

    def forward(n, carry):
        p = (team + n) % nteam
        pltpu.make_async_remote_copy(
            src_ref=stage,
            dst_ref=ctrl.at[pl.ds(slot, quarter_cols)],
            send_sem=f_go,
            recv_sem=f_in,
            device_id=at_team(p),
            device_id_type=MESH,
        ).start()
        return carry

    lax.fori_loop(1, nteam, forward, 0)
    ctrl[pl.ds(slot, quarter_cols)] = stage[...]
    members, obs = hx_ref.shape
    lanes = gram.shape[2]
    region = xh * ny + y
    nregion = nxh * ny

    def at_region(g):
        return {"xh": g // ny, "y": g % ny}

    weighted = (hx_ref[...].astype(F32) * prec_ref[...]).astype(BF)
    padded = jnp.concatenate([hx_ref[...], jnp.zeros((lanes - members, obs), BF)], axis=0)
    lane = lax.broadcasted_iota(jnp.int32, (members, lanes), 1)
    row_of = lax.broadcasted_iota(jnp.int32, (members, lanes), 0)
    for g in range(nregion):
        inside = region_ref[...] == g
        masked = jnp.where(inside, weighted.astype(F32), 0.0)
        right = jnp.sum(masked * innov_ref[...], axis=1, keepdims=True)
        product = lax.dot_general(
            masked.astype(BF), padded, (((1,), (1,)), ((), ())), preferred_element_type=F32
        )
        gram[g] = jnp.where(lane == members, right, product)

    def hand_gram(n, carry):
        g = (region + n) % nregion
        pltpu.make_async_remote_copy(
            src_ref=gram.at[g],
            dst_ref=grams.at[region],
            send_sem=g_go,
            recv_sem=g_in,
            device_id=at_region(g),
            device_id_type=MESH,
        ).start()
        return carry

    lax.fori_loop(1, nregion, hand_gram, 0)
    grams[region] = gram[region]

    def gather_system():
        wait_bytes(grams.at[pl.ds(0, nregion - 1)], g_in)
        value = grams[0]
        for g in range(1, nregion):
            value = value + grams[g]
        system[...] = value + jnp.where(lane == row_of, members - 1.0, 0.0)

    def eliminate(j, carry):
        value = system[...]
        pivot_row = system[pl.ds(j, 1), :]
        column = jnp.sum(jnp.where(lane == j, value, 0.0), axis=1, keepdims=True)
        pivot = jnp.sum(jnp.where(lane[:1] == j, pivot_row, 0.0), axis=1, keepdims=True)
        scaled = pivot_row / pivot
        system[...] = jnp.where(row_of == j, scaled, value - column * scaled)
        return carry

    def hand_answer():
        solved = jnp.sum(
            jnp.where(lane == members, system[...], 0.0), axis=1, keepdims=True
        )
        across = jnp.sum(jnp.where(lane == row_of, solved, 0.0), axis=0, keepdims=True)
        answer[...] = jnp.broadcast_to(across, answer.shape)

        def one(n, carry):
            pltpu.make_async_remote_copy(
                src_ref=answer,
                dst_ref=answers.at[region],
                send_sem=w_go,
                recv_sem=w_in,
                device_id=at_region((region + n) % nregion),
                device_id_type=MESH,
            ).start()
            return carry

        lax.fori_loop(1, nregion, one, 0)
        answers[region] = answer[...]

    lax.fori_loop(2, nk, spread, 0)

    span = WIN * cols
    p_id = lax.broadcasted_iota(jnp.int32, (cols * GR, span), 0)
    q_id = lax.broadcasted_iota(jnp.int32, (cols * GR, span), 1)
    same = q_id % cols == p_id // GR

    def stencil(g, carry):
        take = (
            lax.broadcasted_iota(jnp.int32, (cols * GR, groups * GR), 1)
            == lax.broadcasted_iota(jnp.int32, (cols * GR, groups * GR), 0) % GR + g * GR
        ).astype(BF)
        w = jnp.dot(take, rwt_ref[...], preferred_element_type=F32)
        start = jnp.minimum(jnp.maximum(g * (GR // 2) - 1, 0), coarse - WIN)
        full = jnp.zeros((cols * GR, span), F32)
        for s in range(3):
            wanted = g * (GR // 2) - start + (p_id % GR) // 2 + s - 1
            full = jnp.where(same & (q_id // cols == wanted), w[:, s : s + 1], full)
        sten[g] = full.astype(BF)
        return carry

    lax.fori_loop(0, groups, stencil, 0)

    for side in range(2):
        here = (xl == block // nz) & (z == block % nz) & (c == side)

        @pl.when(jnp.logical_not(here))
        def _():
            wait_bytes(bands.at[side], b_in.at[side])

    narrow = jnp.concatenate(
        [bands[0], pltpu.roll(bands[1], half, 1)], axis=0
    ).astype(BF)
    wide_src = 4 * half * GR
    take_src = one_hot((narrow.shape[1], wide_src), lambda m: m, lambda q: q // GR)
    take_col = one_hot((cols * GR, cols), lambda p: p // GR, lambda j: j)
    wide = jnp.dot(narrow, take_src, preferred_element_type=F32).astype(BF)
    full = jnp.dot(take_col, wide, preferred_element_type=F32)
    p_id2 = lax.broadcasted_iota(jnp.int32, full.shape, 0)
    q_id2 = lax.broadcasted_iota(jnp.int32, full.shape, 1)
    bandf[...] = jnp.where(p_id2 % GR == q_id2 % GR, full, 0.0).astype(BF)

    acc[...] = jnp.zeros_like(acc)

    def refine_group(k, group):
        start = window_start(group, coarse)
        windows = [land[k, t, pl.ds(start, WIN)].reshape(WIN * cols, lev) for t in range(2)]
        out = jnp.dot(
            sten[group], jnp.concatenate(windows, axis=1), preferred_element_type=F32
        ).astype(BF)
        return [out[:, t * lev : (t + 1) * lev].reshape(cols, GR, lev) for t in range(2)]

    def project(k):
        for group in range(groups):
            rows = pl.ds(group * GR, GR)
            first, second = refine_group(k, group)
            both = first.astype(F32) * ctrl[pl.ds(0, cols), rows, :].astype(F32)
            both = both + second.astype(F32) * ctrl[pl.ds(cols, cols), rows, :].astype(F32)
            both = both.astype(BF)
            field[k, 0, :, rows, :] = both[:half]
            field[k, 1, :, rows, :] = both[half:]

    def halo_copy(k, side):
        other = block + 1 if side == 0 else block - 1
        return pltpu.make_async_remote_copy(
            src_ref=field.at[k, 1 - side],
            dst_ref=halo.at[k, side],
            send_sem=h_go.at[k, side],
            recv_sem=h_in.at[k, side],
            device_id={"z": other // nc, "c": other % nc},
            device_id_type=MESH,
        )

    nl, ll = ny, lev // ny

    def hand_columns(start, count):
        for j in range(start, start + count):
            for t in range(2):
                turned = acc[t, j].T.astype(BF)
                for q in range(nl):
                    p = (t * nxl + j // half) * ny + q
                    parts[p, j % half] = turned[q * ll : (q + 1) * ll]
        for j in range(start, start + count):
            for t in range(2):
                for q in range(nl):
                    p = (t * nxl + j // half) * ny + q

                    @pl.when(p != team)
                    def _():
                        pltpu.make_async_remote_copy(
                            src_ref=parts.at[p, j % half],
                            dst_ref=sums.at[team, j % half],
                            send_sem=p_go,
                            recv_sem=p_in,
                            device_id=at_team(p),
                            device_id_type=MESH,
                        ).start()

    sends = (block < blocks - 1, block > 0)
    gets = (block > 0, block < blocks - 1)

    def localize(k):
        for side in range(2):

            @pl.when(gets[side])
            def _():
                wait_bytes(halo.at[k, side], h_in.at[k, side])

            @pl.when(jnp.logical_not(gets[side]))
            def _():
                halo[k, side] = jnp.zeros(halo.shape[2:], BF)

        for group in range(groups):
            rows = pl.ds(group * GR, GR)
            for t, part in enumerate(refine_group(k, group)):
                fine[t, :, rows, :] = part
        for group in range(0, groups, 2):
            sides = []
            for g in (group, group + 1):
                rows = pl.ds(g * GR, GR)
                pieces = [
                    ref[:, rows, :].reshape(half * GR, lev)
                    for ref in (halo.at[k, 0], field.at[k, 0], field.at[k, 1], halo.at[k, 1])
                ]
                sides.append(jnp.concatenate(pieces, axis=0))
            mixed = jnp.dot(
                bandf[...], jnp.concatenate(sides, axis=1), preferred_element_type=F32
            ).astype(BF)
            for n, g in enumerate((group, group + 1)):
                banded[:, pl.ds(g * GR, GR), :] = mixed[:, n * lev : (n + 1) * lev].reshape(
                    cols, GR, lev
                )
        for j in range(0, cols, 2):
            pair = jnp.concatenate([banded[j], banded[j + 1]], axis=1)
            mixed = jnp.dot(row_ref[...], pair, preferred_element_type=F32).astype(BF)
            local = jnp.dot(mixed, lev_ref[...], preferred_element_type=F32)
            for n in range(2):
                part = local[:, n * lev : (n + 1) * lev]
                for t in range(2):
                    acc[t, j + n] += fine[t, j + n].astype(F32) * part

            @pl.when(k == nk - 1)
            def _():
                hand_columns(j, 2)

    def wait_all_but_one(k, sem):
        wait_bytes(sent.at[k, pl.ds(0, ndest - 1)], sem.at[k])

    share = members // (nk - 1)

    def step(k, carry):
        @pl.when(k < nk)
        def _():
            wait_all_but_one(k, s_in)

            @pl.when(k == 0)
            def _():
                wait_bytes(ctrl.at[pl.ds(0, (nteam - 1) * quarter_cols)], f_in)

            project(k)
            for side in range(2):

                @pl.when(sends[side])
                def _():
                    halo_copy(k, side).start()

            @pl.when(k + 2 < nk)
            def _():
                send(k + 2)

            @pl.when(k == 1)
            def _():
                gather_system()

            @pl.when(k >= 1)
            def _():
                lax.fori_loop((k - 1) * share, k * share, eliminate, 0)

            @pl.when(k == nk - 1)
            def _():
                hand_answer()

        @pl.when(k >= 1)
        def _():
            localize(k - 1)

        return carry

    lax.fori_loop(0, nk + 1, step, 0)

    sums[team] = parts[team]
    wait_bytes(sums.at[pl.ds(0, nteam - 1)], p_in)
    for j in range(half):
        value = sums[0, j].astype(F32)
        for p in range(1, nteam):
            value = value + sums[p, j].astype(F32)
        total[j] = value * scale

    dest = (tile * 2) % (blocks * nxl) + xl
    d_block = dest % blocks
    stays = dest == tile
    move = pltpu.make_async_remote_copy(
        src_ref=total,
        dst_ref=moved,
        send_sem=m_go,
        recv_sem=m_in,
        device_id={"xl": dest // blocks, "z": d_block // nc, "c": d_block % nc},
        device_id_type=MESH,
    )

    @pl.when(jnp.logical_not(stays))
    def _():
        move.start()

    @pl.when(stays)
    def _():
        moved[...] = total[...]

    def left(k, carry):
        wait_all_but_one(k, s_go)
        for side in range(2):

            @pl.when(sends[side])
            def _():
                wait_bytes(field.at[k, side], h_go.at[k, side])

        return carry

    lax.fori_loop(0, nk, left, 0)
    wait_bytes(ctrl.at[pl.ds(0, (nteam - 1) * quarter_cols)], f_go)
    wait_bytes(sums.at[pl.ds(0, nteam - 1)], p_go)
    wait_bytes(grams.at[pl.ds(0, nregion - 1)], g_go)
    wait_bytes(answers.at[pl.ds(0, nregion - 1)], w_go)
    wait_bytes(answers.at[pl.ds(0, nregion - 1)], w_in)
    for g in range(nregion):
        w_ref[pl.ds(g, 1), :] = answers[g, :1, :]
    for side in range(nxl):
        here = (to_z == z) & (to_c == c) & (xl == side)

        @pl.when(jnp.logical_not(here))
        def _():
            wait_bytes(bands.at[side], b_go.at[side])

    @pl.when(jnp.logical_not(stays))
    def _():
        move.wait()

    o_ref[...] = moved[...]


def body(
    ens_coarse,
    col_interp,
    row_weights,
    ctrl_vec,
    band_loc,
    row_loc,
    level_loc,
    hx_pert,
    innov,
    obs_prec,
    obs_region,
):
    nxh, nxl, nz, nc, ny = (lax.axis_size(a) for a in ("xh", "xl", "z", "c", "y"))
    _, members, lev, own_rows, coarse_cols = ens_coarse.shape
    fine_cols = col_interp.shape[0]
    fine_rows = row_weights.shape[1]
    blocks = nz * nc
    cols = fine_cols // blocks
    half = cols // 2
    group = members // (nxh * nxl)
    tiles = nxl * blocks
    coarse = tiles * own_rows
    total_members = hx_pert.shape[1]
    nteam = nxh * nxl * ny
    quarter = half // ny
    lanes = 128

    x = ens_coarse.reshape(members, lev * own_rows, coarse_cols)
    rwt = jnp.pad(row_weights.T, ((0, 0), (0, 125)))
    mine = lax.dynamic_slice_in_dim(ctrl_vec[0], lax.axis_index("y") * quarter, quarter, 1)
    mine = jnp.transpose(mine.astype(BF), (1, 2, 0))
    band = jnp.pad(band_loc.astype(F32), ((0, 0), (0, 128 - band_loc.shape[1])))
    none = jnp.zeros_like(level_loc)
    lev_two = jnp.block([[level_loc.T, none], [none, level_loc.T]])

    vm = pl.BlockSpec(memory_space=pltpu.VMEM)
    dma = pltpu.SemaphoreType.DMA
    increment, weights = pl.pallas_call(
        lambda *refs: main_kernel((nxh, nxl, nz, nc, ny, 1.0 / (total_members - 1)), refs),
        in_specs=[vm] * 11,
        out_specs=(vm, vm),
        out_shape=(
            jax.ShapeDtypeStruct((half, lev // ny, fine_rows), F32),
            jax.ShapeDtypeStruct((NREG, lanes), F32),
        ),
        scratch_shapes=[
            pltpu.VMEM((own_rows * lev, own_rows * lev), BF),
            pltpu.VMEM((group, nxh * tiles, own_rows, cols, lev), BF),
            pltpu.VMEM((group, nxh, coarse, cols, lev), BF),
            pltpu.VMEM((fine_rows // GR, cols * GR, WIN * cols), BF),
            pltpu.VMEM((quarter, fine_rows, lev), BF),
            pltpu.VMEM((nxh * cols, fine_rows, lev), BF),
            pltpu.VMEM((2, *band.shape), F32),
            pltpu.VMEM((cols * GR, 4 * half * GR), BF),
            pltpu.VMEM((group, 2, half, fine_rows, lev), BF),
            pltpu.VMEM((group, 2, half, fine_rows, lev), BF),
            pltpu.VMEM((nxh, cols, fine_rows, lev), BF),
            pltpu.VMEM((cols, fine_rows, lev), BF),
            pltpu.VMEM((nxh, cols, fine_rows, lev), F32),
            pltpu.VMEM((nteam, half, lev // ny, fine_rows), BF),
            pltpu.VMEM((nteam, half, lev // ny, fine_rows), BF),
            pltpu.VMEM((half, lev // ny, fine_rows), F32),
            pltpu.VMEM((half, lev // ny, fine_rows), F32),
            pltpu.VMEM((NREG, total_members, lanes), F32),
            pltpu.VMEM((NREG, total_members, lanes), F32),
            pltpu.VMEM((total_members, lanes), F32),
            pltpu.VMEM((8, lanes), F32),
            pltpu.VMEM((NREG, 8, lanes), F32),
            dma((group,)),
            dma((group,)),
            dma((group, 2)),
            dma((group, 2)),
            dma,
            dma,
            dma,
            dma,
            dma((2,)),
            dma((2,)),
            *[dma] * 8,
        ],
        compiler_params=pltpu.CompilerParams(
            collective_id=0, has_side_effects=True, vmem_limit_bytes=62 << 20
        ),
    )(x, col_interp, rwt, mine, band, row_loc, lev_two, hx_pert[0], innov, obs_prec, obs_region)
    increment = jnp.transpose(increment, (1, 0, 2))
    return (increment[None], weights[:, :total_members])


def solution(mesh):
    shape = (2, 2, mesh.shape["tile"] // 4, 2, mesh.shape["mem"])
    fine_mesh = Mesh(mesh.devices.reshape(shape), ("xh", "xl", "z", "c", "y"))
    tile = ("xl", "z", "c")
    obs = (*tile, "y")
    placed = (
        P("xh", "y", None, tile, None),
        P(),
        P(),
        P("xh", None, tile, None),
        P(tile, None),
        P(),
        P(),
        P("xh", None, obs),
        P("xh", obs),
        P("xh", obs),
        P("xh", obs),
    )
    return jax.shard_map(
        body,
        mesh=fine_mesh,
        in_specs=placed,
        out_specs=(P("xh", "y", tile, None), P(tile, None)),
        check_vma=False,
    )
```

```python
import functools

import jax
import jax.numpy as jnp
from jax import lax
from jax.experimental import pallas as pl
from jax.experimental.pallas import tpu as pltpu
from jax.sharding import Mesh, PartitionSpec as P

NREG = 8
BF = jnp.bfloat16
F32 = jnp.float32
GR = 16
WIN = 10


MESH = pl.DeviceIdType.MESH


def one_hot(shape, of_row, of_col):
    row = lax.broadcasted_iota(jnp.int32, shape, 0)
    col = lax.broadcasted_iota(jnp.int32, shape, 1)
    return (of_row(row) == of_col(col)).astype(BF)


def window_start(group, coarse_rows):
    return min(max(group * GR // 2 - 1, 0), coarse_rows - WIN)


def main_kernel(sizes, refs):
    nxh, nxl, nz, nc, ny, scale = sizes
    x_ref, ci_ref, rw_ref, cq_ref, band_in, row_ref, lev_in, *refs = refs
    hx_ref, innov_ref, prec_ref, region_ref, o_ref, w_ref, *refs = refs
    lev_ref, band_ref, rw_all, perm, sent, land, sten, stage, ctrl, bands, bandf, field, halo, fine, banded, acc, *refs = refs
    parts, sums, total, moved, gram, grams, system, answer, answers, *sems = refs
    s_go, s_in, h_go, h_in, c_go, c_in, f_go, f_in, b_go, b_in, p_go, p_in, m_go, m_in, *sems = sems
    g_go, g_in, w_go, w_in = sems

    nk, ndest, own_rows, cols, lev = sent.shape
    coarse = land.shape[2]
    groups = sten.shape[0]
    half = cols // 2
    blocks = nz * nc
    xh, xl, z, c, y = (lax.axis_index(a) for a in ("xh", "xl", "z", "c", "y"))
    block = z * nc + c
    tile = xl * blocks + block
    me = (xh * nxl + xl) * blocks + block
    team = (xh * nxl + xl) * ny + y

    def at_dest(d):
        m, b = d // blocks, d % blocks
        return {"xh": m // nxl, "xl": m % nxl, "z": b // nc, "c": b % nc}

    def at_team(p):
        m = p // ny
        return {"xh": m // nxl, "xl": m % nxl, "y": p % ny}

    barrier = pltpu.get_barrier_semaphore()

    def greet(n, carry):
        pl.semaphore_signal(
            barrier, inc=1, device_id=at_dest((me + n) % ndest), device_id_type=MESH
        )
        return carry

    lax.fori_loop(1, ndest, greet, 0)
    nteam = nxh * nxl * ny

    def greet_team(n, carry):
        p = (team + n) % nteam

        @pl.when(p % ny != y)
        def _():
            pl.semaphore_signal(barrier, inc=1, device_id=at_team(p), device_id_type=MESH)

        return carry

    lax.fori_loop(1, nteam, greet_team, 0)

    flat = own_rows * lev
    perm[...] = one_hot(
        (flat, flat), lambda p: (p % lev) * own_rows + p // lev, lambda q: q
    )

    def spread(k, carry):
        def group_of(m, carry):
            by_row = jnp.dot(
                perm[...], x_ref[m * nk + k], preferred_element_type=F32
            ).astype(BF)
            out = lax.dot_general(
                ci_ref[...], by_row, (((1,), (1,)), ((), ())), preferred_element_type=F32
            ).astype(BF)
            for i in range(own_rows):
                sent[k, pl.ds(m * blocks, blocks), i] = out[:, i * lev : (i + 1) * lev].reshape(
                    blocks, cols, lev
                )
            return carry

        return lax.fori_loop(0, nxh * nxl, group_of, carry)

    def send(k):
        def one(n, carry):
            d = (me + n) % ndest
            pltpu.make_async_remote_copy(
                src_ref=sent.at[k, d],
                dst_ref=land.at[k, xh, pl.ds(tile * own_rows, own_rows)],
                send_sem=s_go.at[k],
                recv_sem=s_in.at[k],
                device_id=at_dest(d),
                device_id_type=MESH,
            ).start()
            return carry

        lax.fori_loop(1, ndest, one, 0)
        land[k, xh, pl.ds(tile * own_rows, own_rows)] = sent[k, me]

    def wait_bytes(ref, sem):
        pltpu.make_async_copy(ref, ref, sem).wait()

    band_ref[...] = jnp.zeros_like(band_ref)
    band_ref[:, : band_in.shape[1]] = band_in[...].astype(F32)
    spread(0, 0)
    pl.semaphore_wait(barrier, ndest - 1 + nteam - nxh * nxl)

    to_xl, to_z, to_c = c, (xl * nz + z) // nc, (xl * nz + z) % nc
    home = (to_xl == xl) & (to_z == z) & (to_c == c)
    quarter = pltpu.make_async_remote_copy(
        src_ref=cq_ref,
        dst_ref=stage,
        send_sem=c_go,
        recv_sem=c_in,
        device_id={"xl": to_xl, "z": to_z, "c": to_c},
        device_id_type=MESH,
    )

    @pl.when(jnp.logical_not(home))
    def _():
        quarter.start()

    @pl.when(home)
    def _():
        stage[...] = cq_ref[...]

    for side in range(nxl):
        here = (to_z == z) & (to_c == c) & (xl == side)

        @pl.when(jnp.logical_not(here))
        def _():
            pltpu.make_async_remote_copy(
                src_ref=band_ref,
                dst_ref=bands.at[c],
                send_sem=b_go.at[side],
                recv_sem=b_in.at[c],
                device_id={"xl": side, "z": to_z, "c": to_c},
                device_id_type=MESH,
            ).start()

        @pl.when(here)
        def _():
            bands[c] = band_ref[...]

    send(0)
    spread(1, 0)
    send(1)

    @pl.when(jnp.logical_not(home))
    def _():
        quarter.wait()

    quarter_cols = cq_ref.shape[0]
    slot = xh * cols + xl * half + y * quarter_cols

    def forward(n, carry):
        p = (team + n) % nteam
        pltpu.make_async_remote_copy(
            src_ref=stage,
            dst_ref=ctrl.at[pl.ds(slot, quarter_cols)],
            send_sem=f_go,
            recv_sem=f_in,
            device_id=at_team(p),
            device_id_type=MESH,
        ).start()
        return carry

    lax.fori_loop(1, nteam, forward, 0)
    ctrl[pl.ds(slot, quarter_cols)] = stage[...]

    def rest(k, carry):
        spread(k, 0)
        send(k)
        return carry

    lax.fori_loop(2, nk, rest, 0)

    members, obs = hx_ref.shape
    lanes = gram.shape[2]
    region = xh * ny + y
    nregion = nxh * ny

    def at_region(g):
        return {"xh": g // ny, "y": g % ny}

    weighted = (hx_ref[...].astype(F32) * prec_ref[...]).astype(BF)
    padded = jnp.concatenate([hx_ref[...], jnp.zeros((lanes - members, obs), BF)], axis=0)
    lane = lax.broadcasted_iota(jnp.int32, (members, lanes), 1)
    row_of = lax.broadcasted_iota(jnp.int32, (members, lanes), 0)
    for g in range(nregion):
        inside = region_ref[...] == g
        masked = jnp.where(inside, weighted.astype(F32), 0.0)
        right = jnp.sum(masked * innov_ref[...], axis=1, keepdims=True)
        product = lax.dot_general(
            masked.astype(BF), padded, (((1,), (1,)), ((), ())), preferred_element_type=F32
        )
        gram[g] = jnp.where(lane == members, right, product)

    def hand_gram(n, carry):
        g = (region + n) % nregion
        pltpu.make_async_remote_copy(
            src_ref=gram.at[g],
            dst_ref=grams.at[region],
            send_sem=g_go,
            recv_sem=g_in,
            device_id=at_region(g),
            device_id_type=MESH,
        ).start()
        return carry

    lax.fori_loop(1, nregion, hand_gram, 0)
    grams[region] = gram[region]

    def gather_system():
        wait_bytes(grams.at[pl.ds(0, nregion - 1)], g_in)
        value = grams[0]
        for g in range(1, nregion):
            value = value + grams[g]
        system[...] = value + jnp.where(lane == row_of, members - 1.0, 0.0)

    def eliminate(j, carry):
        value = system[...]
        pivot_row = system[pl.ds(j, 1), :]
        column = jnp.sum(jnp.where(lane == j, value, 0.0), axis=1, keepdims=True)
        pivot = jnp.sum(jnp.where(lane[:1] == j, pivot_row, 0.0), axis=1, keepdims=True)
        scaled = pivot_row / pivot
        system[...] = jnp.where(row_of == j, scaled, value - column * scaled)
        return carry

    def hand_answer():
        solved = jnp.sum(
            jnp.where(lane == members, system[...], 0.0), axis=1, keepdims=True
        )
        across = jnp.sum(jnp.where(lane == row_of, solved, 0.0), axis=0, keepdims=True)
        answer[...] = jnp.broadcast_to(across, answer.shape)

        def one(n, carry):
            pltpu.make_async_remote_copy(
                src_ref=answer,
                dst_ref=answers.at[region],
                send_sem=w_go,
                recv_sem=w_in,
                device_id=at_region((region + n) % nregion),
                device_id_type=MESH,
            ).start()
            return carry

        lax.fori_loop(1, nregion, one, 0)
        answers[region] = answer[...]

    span = WIN * cols
    p_id = lax.broadcasted_iota(jnp.int32, (cols * GR, span), 0)
    q_id = lax.broadcasted_iota(jnp.int32, (cols * GR, span), 1)
    same = q_id % cols == p_id // GR

    rw_all[...] = jnp.zeros_like(rw_all)
    rw_all[:3, :] = rw_ref[...].astype(F32)
    lev_t = lax.dot_general(
        one_hot((lev, lev), lambda p: p, lambda q: q),
        lev_in[...],
        (((1,), (1,)), ((), ())),
        preferred_element_type=F32,
    ).astype(BF)
    lev_ref[...] = jnp.zeros_like(lev_ref)
    lev_ref[:lev, :lev] = lev_t
    lev_ref[lev:, lev:] = lev_t

    def stencil(g, carry):
        take = (
            lax.broadcasted_iota(jnp.int32, (cols * GR, groups * GR), 1)
            == lax.broadcasted_iota(jnp.int32, (cols * GR, groups * GR), 0) % GR + g * GR
        ).astype(BF)
        w = lax.dot_general(
            take, rw_all[...].astype(BF), (((1,), (1,)), ((), ())), preferred_element_type=F32
        )
        start = jnp.minimum(jnp.maximum(g * (GR // 2) - 1, 0), coarse - WIN)
        full = jnp.zeros((cols * GR, span), F32)
        for s in range(3):
            wanted = g * (GR // 2) - start + (p_id % GR) // 2 + s - 1
            full = jnp.where(same & (q_id // cols == wanted), w[:, s : s + 1], full)
        sten[g] = full.astype(BF)
        return carry

    lax.fori_loop(0, groups, stencil, 0)

    for side in range(2):
        here = (xl == block // nz) & (z == block % nz) & (c == side)

        @pl.when(jnp.logical_not(here))
        def _():
            wait_bytes(bands.at[side], b_in.at[side])

    narrow = jnp.concatenate(
        [bands[0], pltpu.roll(bands[1], half, 1)], axis=0
    ).astype(BF)
    wide_src = 4 * half * GR
    take_src = one_hot((narrow.shape[1], wide_src), lambda m: m, lambda q: q // GR)
    take_col = one_hot((cols * GR, cols), lambda p: p // GR, lambda j: j)
    wide = jnp.dot(narrow, take_src, preferred_element_type=F32).astype(BF)
    full = jnp.dot(take_col, wide, preferred_element_type=F32)
    p_id2 = lax.broadcasted_iota(jnp.int32, full.shape, 0)
    q_id2 = lax.broadcasted_iota(jnp.int32, full.shape, 1)
    bandf[...] = jnp.where(p_id2 % GR == q_id2 % GR, full, 0.0).astype(BF)

    acc[...] = jnp.zeros_like(acc)

    def refine_group(k, group):
        start = window_start(group, coarse)
        windows = [land[k, t, pl.ds(start, WIN)].reshape(WIN * cols, lev) for t in range(2)]
        out = jnp.dot(
            sten[group], jnp.concatenate(windows, axis=1), preferred_element_type=F32
        ).astype(BF)
        return [out[:, t * lev : (t + 1) * lev].reshape(cols, GR, lev) for t in range(2)]

    def project(k):
        for group in range(groups):
            rows = pl.ds(group * GR, GR)
            first, second = refine_group(k, group)
            fine[k % 2, 0, :, rows, :] = first
            fine[k % 2, 1, :, rows, :] = second
            both = first.astype(F32) * ctrl[pl.ds(0, cols), rows, :].astype(F32)
            both = both + second.astype(F32) * ctrl[pl.ds(cols, cols), rows, :].astype(F32)
            both = both.astype(BF)
            field[k, 0, :, rows, :] = both[:half]
            field[k, 1, :, rows, :] = both[half:]

    def halo_copy(k, side):
        other = block + 1 if side == 0 else block - 1
        return pltpu.make_async_remote_copy(
            src_ref=field.at[k, 1 - side],
            dst_ref=halo.at[k, side],
            send_sem=h_go.at[k, side],
            recv_sem=h_in.at[k, side],
            device_id={"z": other // nc, "c": other % nc},
            device_id_type=MESH,
        )

    nl, ll = ny, lev // ny

    def hand_columns(start, count):
        for j in range(start, start + count):
            for t in range(2):
                turned = acc[t, j].T.astype(BF)
                for q in range(nl):
                    p = (t * nxl + j // half) * ny + q
                    parts[p, j % half] = turned[q * ll : (q + 1) * ll]
        for j in range(start, start + count):
            for t in range(2):
                for q in range(nl):
                    p = (t * nxl + j // half) * ny + q

                    @pl.when(p != team)
                    def _():
                        pltpu.make_async_remote_copy(
                            src_ref=parts.at[p, j % half],
                            dst_ref=sums.at[team, j % half],
                            send_sem=p_go,
                            recv_sem=p_in,
                            device_id=at_team(p),
                            device_id_type=MESH,
                        ).start()

    sends = (block < blocks - 1, block > 0)
    gets = (block > 0, block < blocks - 1)

    def localize(k):
        for side in range(2):

            @pl.when(gets[side])
            def _():
                wait_bytes(halo.at[k, side], h_in.at[k, side])

            @pl.when(jnp.logical_not(gets[side]))
            def _():
                halo[k, side] = jnp.zeros(halo.shape[2:], BF)

        for group in range(0, groups, 2):
            sides = []
            for g in (group, group + 1):
                rows = pl.ds(g * GR, GR)
                pieces = [
                    ref[:, rows, :].reshape(half * GR, lev)
                    for ref in (halo.at[k, 0], field.at[k, 0], field.at[k, 1], halo.at[k, 1])
                ]
                sides.append(jnp.concatenate(pieces, axis=0))
            mixed = jnp.dot(
                bandf[...], jnp.concatenate(sides, axis=1), preferred_element_type=F32
            ).astype(BF)
            for n, g in enumerate((group, group + 1)):
                banded[:, pl.ds(g * GR, GR), :] = mixed[:, n * lev : (n + 1) * lev].reshape(
                    cols, GR, lev
                )
        for j in [base + jj for jj in range(0, half, 2) for base in (0, half)]:
            pair = jnp.concatenate([banded[j], banded[j + 1]], axis=1)
            mixed = jnp.dot(row_ref[...], pair, preferred_element_type=F32).astype(BF)
            local = jnp.dot(mixed, lev_ref[...], preferred_element_type=F32)
            for n in range(2):
                part = local[:, n * lev : (n + 1) * lev]
                for t in range(2):
                    acc[t, j + n] += fine[k % 2, t, j + n].astype(F32) * part

            @pl.when(k == nk - 1)
            def _():
                hand_columns(j, 2)

    def wait_all_but_one(k, sem):
        wait_bytes(sent.at[k, pl.ds(0, ndest - 1)], sem.at[k])

    share = members // (nk - 1)

    def step(k, carry):
        @pl.when(k < nk)
        def _():
            wait_all_but_one(k, s_in)

            @pl.when(k == 0)
            def _():
                wait_bytes(ctrl.at[pl.ds(0, (nteam - 1) * quarter_cols)], f_in)

            project(k)
            for side in range(2):

                @pl.when(sends[side])
                def _():
                    halo_copy(k, side).start()

            @pl.when(k == 1)
            def _():
                gather_system()

            @pl.when(k >= 1)
            def _():
                lax.fori_loop((k - 1) * share, k * share, eliminate, 0)

            @pl.when(k == nk - 1)
            def _():
                hand_answer()

        @pl.when(k >= 1)
        def _():
            localize(k - 1)

        return carry

    lax.fori_loop(0, nk + 1, step, 0)

    sums[team] = parts[team]
    wait_bytes(sums.at[pl.ds(0, nteam - 1)], p_in)
    dest = (tile * 2) % (blocks * nxl) + xl
    d_block = dest % blocks
    stays = dest == tile
    for j in range(half):
        value = sums[0, j].astype(F32)
        for p in range(1, nteam):
            value = value + sums[p, j].astype(F32)
        total[j] = (value * scale).astype(BF)

        @pl.when(jnp.logical_not(stays))
        def _():
            pltpu.make_async_remote_copy(
                src_ref=total.at[j],
                dst_ref=moved.at[j],
                send_sem=m_go,
                recv_sem=m_in,
                device_id={"xl": dest // blocks, "z": d_block // nc, "c": d_block % nc},
                device_id_type=MESH,
            ).start()

        @pl.when(stays)
        def _():
            moved[j] = total[j]

    def left(k, carry):
        wait_all_but_one(k, s_go)
        for side in range(2):

            @pl.when(sends[side])
            def _():
                wait_bytes(field.at[k, side], h_go.at[k, side])

        return carry

    lax.fori_loop(0, nk, left, 0)
    wait_bytes(ctrl.at[pl.ds(0, (nteam - 1) * quarter_cols)], f_go)
    wait_bytes(sums.at[pl.ds(0, nteam - 1)], p_go)
    wait_bytes(grams.at[pl.ds(0, nregion - 1)], g_go)
    wait_bytes(answers.at[pl.ds(0, nregion - 1)], w_go)
    wait_bytes(answers.at[pl.ds(0, nregion - 1)], w_in)
    for g in range(nregion):
        w_ref[pl.ds(g, 1), :] = answers[g, :1, :members]
    for side in range(nxl):
        here = (to_z == z) & (to_c == c) & (xl == side)

        @pl.when(jnp.logical_not(here))
        def _():
            wait_bytes(bands.at[side], b_go.at[side])

    @pl.when(jnp.logical_not(stays))
    def _():
        wait_bytes(total, m_go)
        wait_bytes(moved, m_in)

    for j in range(half):
        o_ref[:, j, :] = moved[j].astype(F32)


def body(
    ens_coarse,
    col_interp,
    row_weights,
    ctrl_vec,
    band_loc,
    row_loc,
    level_loc,
    hx_pert,
    innov,
    obs_prec,
    obs_region,
):
    nxh, nxl, nz, nc, ny = (lax.axis_size(a) for a in ("xh", "xl", "z", "c", "y"))
    _, members, lev, own_rows, coarse_cols = ens_coarse.shape
    fine_cols = col_interp.shape[0]
    fine_rows = row_weights.shape[1]
    blocks = nz * nc
    cols = fine_cols // blocks
    half = cols // 2
    group = members // (nxh * nxl)
    tiles = nxl * blocks
    coarse = tiles * own_rows
    total_members = hx_pert.shape[1]
    nteam = nxh * nxl * ny
    quarter = half // ny
    lanes = 128

    x = ens_coarse.reshape(members, lev * own_rows, coarse_cols)
    mine = lax.dynamic_slice_in_dim(ctrl_vec[0], lax.axis_index("y") * quarter, quarter, 1)
    mine = jnp.transpose(mine.astype(BF), (1, 2, 0))

    vm = pl.BlockSpec(memory_space=pltpu.VMEM)
    dma = pltpu.SemaphoreType.DMA
    increment, weights = pl.pallas_call(
        lambda *refs: main_kernel((nxh, nxl, nz, nc, ny, 1.0 / (total_members - 1)), refs),
        in_specs=[vm] * 11,
        out_specs=(vm, vm),
        out_shape=(
            jax.ShapeDtypeStruct((lev // ny, half, fine_rows), F32),
            jax.ShapeDtypeStruct((NREG, total_members), F32),
        ),
        scratch_shapes=[
            pltpu.VMEM((2 * lev, 2 * lev), BF),
            pltpu.VMEM((half, lanes), F32),
            pltpu.VMEM((8, fine_rows), F32),
            pltpu.VMEM((own_rows * lev, own_rows * lev), BF),
            pltpu.VMEM((group, nxh * tiles, own_rows, cols, lev), BF),
            pltpu.VMEM((group, nxh, coarse, cols, lev), BF),
            pltpu.VMEM((fine_rows // GR, cols * GR, WIN * cols), BF),
            pltpu.VMEM((quarter, fine_rows, lev), BF),
            pltpu.VMEM((nxh * cols, fine_rows, lev), BF),
            pltpu.VMEM((2, half, lanes), F32),
            pltpu.VMEM((cols * GR, 4 * half * GR), BF),
            pltpu.VMEM((group, 2, half, fine_rows, lev), BF),
            pltpu.VMEM((group, 2, half, fine_rows, lev), BF),
            pltpu.VMEM((2, nxh, cols, fine_rows, lev), BF),
            pltpu.VMEM((cols, fine_rows, lev), BF),
            pltpu.VMEM((nxh, cols, fine_rows, lev), F32),
            pltpu.VMEM((nteam, half, lev // ny, fine_rows), BF),
            pltpu.VMEM((nteam, half, lev // ny, fine_rows), BF),
            pltpu.VMEM((half, lev // ny, fine_rows), BF),
            pltpu.VMEM((half, lev // ny, fine_rows), BF),
            pltpu.VMEM((NREG, total_members, lanes), F32),
            pltpu.VMEM((NREG, total_members, lanes), F32),
            pltpu.VMEM((total_members, lanes), F32),
            pltpu.VMEM((8, lanes), F32),
            pltpu.VMEM((NREG, 8, lanes), F32),
            dma((group,)),
            dma((group,)),
            dma((group, 2)),
            dma((group, 2)),
            dma,
            dma,
            dma,
            dma,
            dma((2,)),
            dma((2,)),
            *[dma] * 8,
        ],
        compiler_params=pltpu.CompilerParams(
            collective_id=0, has_side_effects=True, vmem_limit_bytes=62 << 20
        ),
    )(x, col_interp, row_weights, mine, band_loc, row_loc, level_loc, hx_pert[0], innov, obs_prec, obs_region)
    return (increment[None], weights)


def solution(mesh):
    shape = (2, 2, mesh.shape["tile"] // 4, 2, mesh.shape["mem"])
    fine_mesh = Mesh(mesh.devices.reshape(shape), ("xh", "xl", "z", "c", "y"))
    tile = ("xl", "z", "c")
    obs = (*tile, "y")
    placed = (
        P("xh", "y", None, tile, None),
        P(),
        P(),
        P("xh", None, tile, None),
        P(tile, None),
        P(),
        P(),
        P("xh", None, obs),
        P("xh", obs),
        P("xh", obs),
        P("xh", obs),
    )
    return jax.shard_map(
        body,
        mesh=fine_mesh,
        in_specs=placed,
        out_specs=(P("xh", "y", tile, None), P(tile, None)),
        check_vma=False,
    )
```

```python
import functools

import jax
import jax.numpy as jnp
from jax import lax
from jax.experimental import pallas as pl
from jax.experimental.pallas import tpu as pltpu
from jax.sharding import Mesh, PartitionSpec as P

NREG = 8
BF = jnp.bfloat16
F32 = jnp.float32
GR = 16
WIN = 10


MESH = pl.DeviceIdType.MESH


def one_hot(shape, of_row, of_col):
    row = lax.broadcasted_iota(jnp.int32, shape, 0)
    col = lax.broadcasted_iota(jnp.int32, shape, 1)
    return (of_row(row) == of_col(col)).astype(BF)


def window_start(group, coarse_rows):
    return min(max(group * GR // 2 - 1, 0), coarse_rows - WIN)


def main_kernel(sizes, refs):
    nxh, nxl, nz, nc, ny, scale = sizes
    x_ref, ci_ref, rw_ref, cq_ref, band_in, row_ref, lev_in, *refs = refs
    hx_ref, innov_ref, prec_ref, region_ref, o_ref, w_ref, *refs = refs
    lev_ref, band_ref, rw_all, perm, sent, land, sten, stage, ctrl, bands, bandf, field, halo, fine, banded, acc, *refs = refs
    parts, sums, total, moved, gram, grams, system, answer, answers, *sems = refs
    s_go, s_in, h_go, h_in, c_go, c_in, f_go, f_in, b_go, b_in, p_go, p_in, m_go, m_in, *sems = sems
    g_go, g_in, w_go, w_in = sems

    nk, ndest, own_rows, cols, lev = sent.shape
    coarse = land.shape[2]
    groups = sten.shape[0]
    half = cols // 2
    blocks = nz * nc
    xh, xl, z, c, y = (lax.axis_index(a) for a in ("xh", "xl", "z", "c", "y"))
    block = z * nc + c
    tile = xl * blocks + block
    me = (xh * nxl + xl) * blocks + block
    team = (xh * nxl + xl) * ny + y

    def at_dest(d):
        m, b = d // blocks, d % blocks
        return {"xh": m // nxl, "xl": m % nxl, "z": b // nc, "c": b % nc}

    def at_team(p):
        m = p // ny
        return {"xh": m // nxl, "xl": m % nxl, "y": p % ny}

    barrier = pltpu.get_barrier_semaphore()

    def greet(n, carry):
        pl.semaphore_signal(
            barrier, inc=1, device_id=at_dest((me + n) % ndest), device_id_type=MESH
        )
        return carry

    lax.fori_loop(1, ndest, greet, 0)
    nteam = nxh * nxl * ny

    def greet_team(n, carry):
        p = (team + n) % nteam

        @pl.when(p % ny != y)
        def _():
            pl.semaphore_signal(barrier, inc=1, device_id=at_team(p), device_id_type=MESH)

        return carry

    lax.fori_loop(1, nteam, greet_team, 0)

    flat = own_rows * lev
    perm[...] = one_hot(
        (flat, flat), lambda p: (p % lev) * own_rows + p // lev, lambda q: q
    )

    def spread(k, carry):
        def group_of(m, carry):
            by_row = jnp.dot(
                perm[...], x_ref[m * nk + k], preferred_element_type=F32
            ).astype(BF)
            out = lax.dot_general(
                ci_ref[...], by_row, (((1,), (1,)), ((), ())), preferred_element_type=F32
            ).astype(BF)
            for i in range(own_rows):
                sent[k, pl.ds(m * blocks, blocks), i] = out[:, i * lev : (i + 1) * lev].reshape(
                    blocks, cols, lev
                )
            return carry

        return lax.fori_loop(0, nxh * nxl, group_of, carry)

    def send(k):
        def one(n, carry):
            d = (me + n) % ndest
            pltpu.make_async_remote_copy(
                src_ref=sent.at[k, d],
                dst_ref=land.at[k, xh, pl.ds(tile * own_rows, own_rows)],
                send_sem=s_go.at[k],
                recv_sem=s_in.at[k],
                device_id=at_dest(d),
                device_id_type=MESH,
            ).start()
            return carry

        lax.fori_loop(1, ndest, one, 0)
        land[k, xh, pl.ds(tile * own_rows, own_rows)] = sent[k, me]

    def wait_bytes(ref, sem):
        pltpu.make_async_copy(ref, ref, sem).wait()

    band_ref[...] = jnp.zeros_like(band_ref)
    band_ref[:, : band_in.shape[1]] = band_in[...].astype(F32)
    spread(0, 0)
    pl.semaphore_wait(barrier, ndest - 1 + nteam - nxh * nxl)

    to_xl, to_z, to_c = c, (xl * nz + z) // nc, (xl * nz + z) % nc
    home = (to_xl == xl) & (to_z == z) & (to_c == c)
    quarter = pltpu.make_async_remote_copy(
        src_ref=cq_ref,
        dst_ref=stage,
        send_sem=c_go,
        recv_sem=c_in,
        device_id={"xl": to_xl, "z": to_z, "c": to_c},
        device_id_type=MESH,
    )

    @pl.when(jnp.logical_not(home))
    def _():
        quarter.start()

    @pl.when(home)
    def _():
        stage[...] = cq_ref[...]

    for side in range(nxl):
        here = (to_z == z) & (to_c == c) & (xl == side)

        @pl.when(jnp.logical_not(here))
        def _():
            pltpu.make_async_remote_copy(
                src_ref=band_ref,
                dst_ref=bands.at[c],
                send_sem=b_go.at[side],
                recv_sem=b_in.at[c],
                device_id={"xl": side, "z": to_z, "c": to_c},
                device_id_type=MESH,
            ).start()

        @pl.when(here)
        def _():
            bands[c] = band_ref[...]

    send(0)
    spread(1, 0)
    send(1)

    @pl.when(jnp.logical_not(home))
    def _():
        quarter.wait()

    quarter_cols = cq_ref.shape[0]
    slot = xh * cols + xl * half + y * quarter_cols

    def forward(n, carry):
        p = (team + n) % nteam
        pltpu.make_async_remote_copy(
            src_ref=stage,
            dst_ref=ctrl.at[pl.ds(slot, quarter_cols)],
            send_sem=f_go,
            recv_sem=f_in,
            device_id=at_team(p),
            device_id_type=MESH,
        ).start()
        return carry

    lax.fori_loop(1, nteam, forward, 0)
    ctrl[pl.ds(slot, quarter_cols)] = stage[...]

    spread(2, 0)
    send(2)
    lax.fori_loop(3, nk, spread, 0)

    members, obs = hx_ref.shape
    lanes = gram.shape[2]
    region = xh * ny + y
    nregion = nxh * ny

    def at_region(g):
        return {"xh": g // ny, "y": g % ny}

    weighted = (hx_ref[...].astype(F32) * prec_ref[...]).astype(BF)
    padded = jnp.concatenate([hx_ref[...], jnp.zeros((lanes - members, obs), BF)], axis=0)
    lane = lax.broadcasted_iota(jnp.int32, (members, lanes), 1)
    row_of = lax.broadcasted_iota(jnp.int32, (members, lanes), 0)
    for g in range(nregion):
        inside = region_ref[...] == g
        masked = jnp.where(inside, weighted.astype(F32), 0.0)
        right = jnp.sum(masked * innov_ref[...], axis=1, keepdims=True)
        product = lax.dot_general(
            masked.astype(BF), padded, (((1,), (1,)), ((), ())), preferred_element_type=F32
        )
        gram[g] = jnp.where(lane == members, right, product)

    def hand_gram(n, carry):
        g = (region + n) % nregion
        pltpu.make_async_remote_copy(
            src_ref=gram.at[g],
            dst_ref=grams.at[region],
            send_sem=g_go,
            recv_sem=g_in,
            device_id=at_region(g),
            device_id_type=MESH,
        ).start()
        return carry

    lax.fori_loop(1, nregion, hand_gram, 0)
    grams[region] = gram[region]

    def gather_system():
        wait_bytes(grams.at[pl.ds(0, nregion - 1)], g_in)
        value = grams[0]
        for g in range(1, nregion):
            value = value + grams[g]
        system[...] = value + jnp.where(lane == row_of, members - 1.0, 0.0)

    def eliminate(j, carry):
        value = system[...]
        pivot_row = system[pl.ds(j, 1), :]
        column = jnp.sum(jnp.where(lane == j, value, 0.0), axis=1, keepdims=True)
        pivot = jnp.sum(jnp.where(lane[:1] == j, pivot_row, 0.0), axis=1, keepdims=True)
        scaled = pivot_row / pivot
        system[...] = jnp.where(row_of == j, scaled, value - column * scaled)
        return carry

    def hand_answer():
        solved = jnp.sum(
            jnp.where(lane == members, system[...], 0.0), axis=1, keepdims=True
        )
        across = jnp.sum(jnp.where(lane == row_of, solved, 0.0), axis=0, keepdims=True)
        answer[...] = jnp.broadcast_to(across, answer.shape)

        def one(n, carry):
            pltpu.make_async_remote_copy(
                src_ref=answer,
                dst_ref=answers.at[region],
                send_sem=w_go,
                recv_sem=w_in,
                device_id=at_region((region + n) % nregion),
                device_id_type=MESH,
            ).start()
            return carry

        lax.fori_loop(1, nregion, one, 0)
        answers[region] = answer[...]

    span = WIN * cols
    p_id = lax.broadcasted_iota(jnp.int32, (cols * GR, span), 0)
    q_id = lax.broadcasted_iota(jnp.int32, (cols * GR, span), 1)
    same = q_id % cols == p_id // GR

    rw_all[...] = jnp.zeros_like(rw_all)
    rw_all[:3, :] = rw_ref[...].astype(F32)
    lev_t = lax.dot_general(
        one_hot((lev, lev), lambda p: p, lambda q: q),
        lev_in[...],
        (((1,), (1,)), ((), ())),
        preferred_element_type=F32,
    ).astype(BF)
    lev_ref[...] = jnp.zeros_like(lev_ref)
    lev_ref[:lev, :lev] = lev_t
    lev_ref[lev:, lev:] = lev_t

    def stencil(g, carry):
        take = (
            lax.broadcasted_iota(jnp.int32, (cols * GR, groups * GR), 1)
            == lax.broadcasted_iota(jnp.int32, (cols * GR, groups * GR), 0) % GR + g * GR
        ).astype(BF)
        w = lax.dot_general(
            take, rw_all[...].astype(BF), (((1,), (1,)), ((), ())), preferred_element_type=F32
        )
        start = jnp.minimum(jnp.maximum(g * (GR // 2) - 1, 0), coarse - WIN)
        full = jnp.zeros((cols * GR, span), F32)
        for s in range(3):
            wanted = g * (GR // 2) - start + (p_id % GR) // 2 + s - 1
            full = jnp.where(same & (q_id // cols == wanted), w[:, s : s + 1], full)
        sten[g] = full.astype(BF)
        return carry

    lax.fori_loop(0, groups, stencil, 0)

    for side in range(2):
        here = (xl == block // nz) & (z == block % nz) & (c == side)

        @pl.when(jnp.logical_not(here))
        def _():
            wait_bytes(bands.at[side], b_in.at[side])

    narrow = jnp.concatenate(
        [bands[0], pltpu.roll(bands[1], half, 1)], axis=0
    ).astype(BF)
    wide_src = 4 * half * GR
    take_src = one_hot((narrow.shape[1], wide_src), lambda m: m, lambda q: q // GR)
    take_col = one_hot((cols * GR, cols), lambda p: p // GR, lambda j: j)
    wide = jnp.dot(narrow, take_src, preferred_element_type=F32).astype(BF)
    full = jnp.dot(take_col, wide, preferred_element_type=F32)
    p_id2 = lax.broadcasted_iota(jnp.int32, full.shape, 0)
    q_id2 = lax.broadcasted_iota(jnp.int32, full.shape, 1)
    bandf[...] = jnp.where(p_id2 % GR == q_id2 % GR, full, 0.0).astype(BF)

    acc[...] = jnp.zeros_like(acc)

    def refine_group(k, group):
        start = window_start(group, coarse)
        windows = [land[k, t, pl.ds(start, WIN)].reshape(WIN * cols, lev) for t in range(2)]
        out = jnp.dot(
            sten[group], jnp.concatenate(windows, axis=1), preferred_element_type=F32
        ).astype(BF)
        return [out[:, t * lev : (t + 1) * lev].reshape(cols, GR, lev) for t in range(2)]

    def project(k):
        for group in range(groups):
            rows = pl.ds(group * GR, GR)
            first, second = refine_group(k, group)
            fine[k % 3, 0, :, rows, :] = first
            fine[k % 3, 1, :, rows, :] = second
            both = first.astype(F32) * ctrl[pl.ds(0, cols), rows, :].astype(F32)
            both = both + second.astype(F32) * ctrl[pl.ds(cols, cols), rows, :].astype(F32)
            both = both.astype(BF)
            field[k, 0, :, rows, :] = both[:half]
            field[k, 1, :, rows, :] = both[half:]

    def halo_copy(k, side):
        other = block + 1 if side == 0 else block - 1
        return pltpu.make_async_remote_copy(
            src_ref=field.at[k, 1 - side],
            dst_ref=halo.at[k, side],
            send_sem=h_go.at[k, side],
            recv_sem=h_in.at[k, side],
            device_id={"z": other // nc, "c": other % nc},
            device_id_type=MESH,
        )

    nl, ll = ny, lev // ny

    def hand_columns(start, count):
        for j in range(start, start + count):
            for t in range(2):
                turned = acc[t, j].T.astype(BF)
                for q in range(nl):
                    p = (t * nxl + j // half) * ny + q
                    parts[p, j % half] = turned[q * ll : (q + 1) * ll]
        for j in range(start, start + count):
            for t in range(2):
                for q in range(nl):
                    p = (t * nxl + j // half) * ny + q

                    @pl.when(p != team)
                    def _():
                        pltpu.make_async_remote_copy(
                            src_ref=parts.at[p, j % half],
                            dst_ref=sums.at[team, j % half],
                            send_sem=p_go,
                            recv_sem=p_in,
                            device_id=at_team(p),
                            device_id_type=MESH,
                        ).start()

    sends = (block < blocks - 1, block > 0)
    gets = (block > 0, block < blocks - 1)

    def localize(k):
        for side in range(2):

            @pl.when(gets[side])
            def _():
                wait_bytes(halo.at[k, side], h_in.at[k, side])

            @pl.when(jnp.logical_not(gets[side]))
            def _():
                halo[k, side] = jnp.zeros(halo.shape[2:], BF)

        for group in range(0, groups, 2):
            sides = []
            for g in (group, group + 1):
                rows = pl.ds(g * GR, GR)
                pieces = [
                    ref[:, rows, :].reshape(half * GR, lev)
                    for ref in (halo.at[k, 0], field.at[k, 0], field.at[k, 1], halo.at[k, 1])
                ]
                sides.append(jnp.concatenate(pieces, axis=0))
            mixed = jnp.dot(
                bandf[...], jnp.concatenate(sides, axis=1), preferred_element_type=F32
            ).astype(BF)
            for n, g in enumerate((group, group + 1)):
                banded[:, pl.ds(g * GR, GR), :] = mixed[:, n * lev : (n + 1) * lev].reshape(
                    cols, GR, lev
                )
        for j in [base + jj for jj in range(0, half, 2) for base in (0, half)]:
            pair = jnp.concatenate([banded[j], banded[j + 1]], axis=1)
            mixed = jnp.dot(row_ref[...], pair, preferred_element_type=F32).astype(BF)
            local = jnp.dot(mixed, lev_ref[...], preferred_element_type=F32)
            for n in range(2):
                part = local[:, n * lev : (n + 1) * lev]
                for t in range(2):
                    acc[t, j + n] += fine[k % 3, t, j + n].astype(F32) * part

            @pl.when(k == nk - 1)
            def _():
                hand_columns(j, 2)

    def wait_all_but_one(k, sem):
        wait_bytes(sent.at[k, pl.ds(0, ndest - 1)], sem.at[k])

    share = -(-members // (nk - 2))

    def step(k, carry):
        @pl.when(k < nk)
        def _():
            wait_all_but_one(k, s_in)

            @pl.when(k == 0)
            def _():
                wait_bytes(ctrl.at[pl.ds(0, (nteam - 1) * quarter_cols)], f_in)

            project(k)
            for side in range(2):

                @pl.when(sends[side])
                def _():
                    halo_copy(k, side).start()

            @pl.when(k + 3 < nk)
            def _():
                send(k + 3)

            @pl.when(k == 1)
            def _():
                gather_system()

            @pl.when(k >= 1)
            def _():
                last = jnp.minimum(k * share, members)
                lax.fori_loop(jnp.minimum((k - 1) * share, members), last, eliminate, 0)

            @pl.when(k == nk - 1)
            def _():
                hand_answer()

        @pl.when(k >= 2)
        def _():
            localize(k - 2)

        return carry

    lax.fori_loop(0, nk + 2, step, 0)

    sums[team] = parts[team]
    wait_bytes(sums.at[pl.ds(0, nteam - 1)], p_in)
    dest = (tile * 2) % (blocks * nxl) + xl
    d_block = dest % blocks
    stays = dest == tile
    for j in range(half):
        value = sums[0, j].astype(F32)
        for p in range(1, nteam):
            value = value + sums[p, j].astype(F32)
        total[j] = (value * scale).astype(BF)

        @pl.when(jnp.logical_not(stays))
        def _():
            pltpu.make_async_remote_copy(
                src_ref=total.at[j],
                dst_ref=moved.at[j],
                send_sem=m_go,
                recv_sem=m_in,
                device_id={"xl": dest // blocks, "z": d_block // nc, "c": d_block % nc},
                device_id_type=MESH,
            ).start()

        @pl.when(stays)
        def _():
            moved[j] = total[j]

    def left(k, carry):
        wait_all_but_one(k, s_go)
        for side in range(2):

            @pl.when(sends[side])
            def _():
                wait_bytes(field.at[k, side], h_go.at[k, side])

        return carry

    lax.fori_loop(0, nk, left, 0)
    wait_bytes(ctrl.at[pl.ds(0, (nteam - 1) * quarter_cols)], f_go)
    wait_bytes(sums.at[pl.ds(0, nteam - 1)], p_go)
    wait_bytes(grams.at[pl.ds(0, nregion - 1)], g_go)
    wait_bytes(answers.at[pl.ds(0, nregion - 1)], w_go)
    wait_bytes(answers.at[pl.ds(0, nregion - 1)], w_in)
    for g in range(nregion):
        w_ref[pl.ds(g, 1), :] = answers[g, :1, :members]
    for side in range(nxl):
        here = (to_z == z) & (to_c == c) & (xl == side)

        @pl.when(jnp.logical_not(here))
        def _():
            wait_bytes(bands.at[side], b_go.at[side])

    @pl.when(jnp.logical_not(stays))
    def _():
        wait_bytes(total, m_go)
        wait_bytes(moved, m_in)

    for j in range(half):
        o_ref[j] = moved[j]


def body(
    ens_coarse,
    col_interp,
    row_weights,
    ctrl_vec,
    band_loc,
    row_loc,
    level_loc,
    hx_pert,
    innov,
    obs_prec,
    obs_region,
):
    nxh, nxl, nz, nc, ny = (lax.axis_size(a) for a in ("xh", "xl", "z", "c", "y"))
    _, members, lev, own_rows, coarse_cols = ens_coarse.shape
    fine_cols = col_interp.shape[0]
    fine_rows = row_weights.shape[1]
    blocks = nz * nc
    cols = fine_cols // blocks
    half = cols // 2
    group = members // (nxh * nxl)
    tiles = nxl * blocks
    coarse = tiles * own_rows
    total_members = hx_pert.shape[1]
    nteam = nxh * nxl * ny
    quarter = half // ny
    lanes = 128

    x = ens_coarse.reshape(members, lev * own_rows, coarse_cols)
    mine = lax.dynamic_slice_in_dim(ctrl_vec[0], lax.axis_index("y") * quarter, quarter, 1)
    mine = jnp.transpose(mine.astype(BF), (1, 2, 0))

    vm = pl.BlockSpec(memory_space=pltpu.VMEM)
    dma = pltpu.SemaphoreType.DMA
    increment, weights = pl.pallas_call(
        lambda *refs: main_kernel((nxh, nxl, nz, nc, ny, 1.0 / (total_members - 1)), refs),
        in_specs=[vm] * 11,
        out_specs=(vm, vm),
        out_shape=(
            jax.ShapeDtypeStruct((half, lev // ny, fine_rows), BF),
            jax.ShapeDtypeStruct((NREG, total_members), F32),
        ),
        scratch_shapes=[
            pltpu.VMEM((2 * lev, 2 * lev), BF),
            pltpu.VMEM((half, lanes), F32),
            pltpu.VMEM((8, fine_rows), F32),
            pltpu.VMEM((own_rows * lev, own_rows * lev), BF),
            pltpu.VMEM((group, nxh * tiles, own_rows, cols, lev), BF),
            pltpu.VMEM((group, nxh, coarse, cols, lev), BF),
            pltpu.VMEM((fine_rows // GR, cols * GR, WIN * cols), BF),
            pltpu.VMEM((quarter, fine_rows, lev), BF),
            pltpu.VMEM((nxh * cols, fine_rows, lev), BF),
            pltpu.VMEM((2, half, lanes), F32),
            pltpu.VMEM((cols * GR, 4 * half * GR), BF),
            pltpu.VMEM((group, 2, half, fine_rows, lev), BF),
            pltpu.VMEM((group, 2, half, fine_rows, lev), BF),
            pltpu.VMEM((3, nxh, cols, fine_rows, lev), BF),
            pltpu.VMEM((cols, fine_rows, lev), BF),
            pltpu.VMEM((nxh, cols, fine_rows, lev), F32),
            pltpu.VMEM((nteam, half, lev // ny, fine_rows), BF),
            pltpu.VMEM((nteam, half, lev // ny, fine_rows), BF),
            pltpu.VMEM((half, lev // ny, fine_rows), BF),
            pltpu.VMEM((half, lev // ny, fine_rows), BF),
            pltpu.VMEM((NREG, total_members, lanes), F32),
            pltpu.VMEM((NREG, total_members, lanes), F32),
            pltpu.VMEM((total_members, lanes), F32),
            pltpu.VMEM((8, lanes), F32),
            pltpu.VMEM((NREG, 8, lanes), F32),
            dma((group,)),
            dma((group,)),
            dma((group, 2)),
            dma((group, 2)),
            dma,
            dma,
            dma,
            dma,
            dma((2,)),
            dma((2,)),
            *[dma] * 8,
        ],
        compiler_params=pltpu.CompilerParams(
            collective_id=0, has_side_effects=True, vmem_limit_bytes=62 << 20
        ),
    )(x, col_interp, row_weights, mine, band_loc, row_loc, level_loc, hx_pert[0], innov, obs_prec, obs_region)
    increment = jnp.transpose(increment, (1, 0, 2)).astype(F32)
    return (increment[None], weights)


def solution(mesh):
    shape = (2, 2, mesh.shape["tile"] // 4, 2, mesh.shape["mem"])
    fine_mesh = Mesh(mesh.devices.reshape(shape), ("xh", "xl", "z", "c", "y"))
    tile = ("xl", "z", "c")
    obs = (*tile, "y")
    placed = (
        P("xh", "y", None, tile, None),
        P(),
        P(),
        P("xh", None, tile, None),
        P(tile, None),
        P(),
        P(),
        P("xh", None, obs),
        P("xh", obs),
        P("xh", obs),
        P("xh", obs),
    )
    return jax.shard_map(
        body,
        mesh=fine_mesh,
        in_specs=placed,
        out_specs=(P("xh", "y", tile, None), P(tile, None)),
        check_vma=False,
    )
```

```python
import functools

import jax
import jax.numpy as jnp
from jax import lax
from jax.experimental import pallas as pl
from jax.experimental.pallas import tpu as pltpu
from jax.sharding import Mesh, PartitionSpec as P

NREG = 8
BF = jnp.bfloat16
F32 = jnp.float32
GR = 16
WIN = 10


MESH = pl.DeviceIdType.MESH


def one_hot(shape, of_row, of_col):
    row = lax.broadcasted_iota(jnp.int32, shape, 0)
    col = lax.broadcasted_iota(jnp.int32, shape, 1)
    return (of_row(row) == of_col(col)).astype(BF)


def window_start(group, coarse_rows):
    return min(max(group * GR // 2 - 1, 0), coarse_rows - WIN)


def main_kernel(sizes, refs):
    nxh, nxl, nz, nc, ny, scale = sizes
    x_ref, ci_ref, rw_ref, cq_ref, band_in, row_ref, lev_in, *refs = refs
    hx_ref, innov_ref, prec_ref, region_ref, o_ref, w_ref, *refs = refs
    lev_ref, band_ref, rw_all, perm, sent, land, sten, stage, ctrl, bands, bandf, field, fine, banded, acc, *refs = refs
    parts, sums, total, moved, gram, grams, system, answer, answers, *sems = refs
    s_go, s_in, h_go, h_in, c_go, c_in, f_go, f_in, b_go, b_in, p_go, p_in, m_go, m_in, *sems = sems
    g_go, g_in, w_go, w_in = sems

    nk, ndest, own_rows, cols, lev = sent.shape
    coarse = land.shape[2]
    groups = sten.shape[0]
    half = cols // 2
    blocks = nz * nc
    xh, xl, z, c, y = (lax.axis_index(a) for a in ("xh", "xl", "z", "c", "y"))
    block = z * nc + c
    tile = xl * blocks + block
    me = (xh * nxl + xl) * blocks + block
    team = (xh * nxl + xl) * ny + y

    def at_dest(d):
        m, b = d // blocks, d % blocks
        return {"xh": m // nxl, "xl": m % nxl, "z": b // nc, "c": b % nc}

    def at_team(p):
        m = p // ny
        return {"xh": m // nxl, "xl": m % nxl, "y": p % ny}

    barrier = pltpu.get_barrier_semaphore()

    def greet(n, carry):
        pl.semaphore_signal(
            barrier, inc=1, device_id=at_dest((me + n) % ndest), device_id_type=MESH
        )
        return carry

    lax.fori_loop(1, ndest, greet, 0)
    nteam = nxh * nxl * ny

    def greet_team(n, carry):
        p = (team + n) % nteam

        @pl.when(p % ny != y)
        def _():
            pl.semaphore_signal(barrier, inc=1, device_id=at_team(p), device_id_type=MESH)

        return carry

    lax.fori_loop(1, nteam, greet_team, 0)

    flat = own_rows * lev
    perm[...] = one_hot(
        (flat, flat), lambda p: (p % lev) * own_rows + p // lev, lambda q: q
    )

    def spread(k, carry):
        def group_of(m, carry):
            by_row = jnp.dot(
                perm[...], x_ref[m * nk + k], preferred_element_type=F32
            ).astype(BF)
            out = lax.dot_general(
                ci_ref[...], by_row, (((1,), (1,)), ((), ())), preferred_element_type=F32
            ).astype(BF)
            for i in range(own_rows):
                sent[k, pl.ds(m * blocks, blocks), i] = out[:, i * lev : (i + 1) * lev].reshape(
                    blocks, cols, lev
                )
            return carry

        return lax.fori_loop(0, nxh * nxl, group_of, carry)

    def send(k):
        def one(n, carry):
            d = (me + n) % ndest
            pltpu.make_async_remote_copy(
                src_ref=sent.at[k, d],
                dst_ref=land.at[k, xh, pl.ds(tile * own_rows, own_rows)],
                send_sem=s_go.at[k],
                recv_sem=s_in.at[k],
                device_id=at_dest(d),
                device_id_type=MESH,
            ).start()
            return carry

        lax.fori_loop(1, ndest, one, 0)
        land[k, xh, pl.ds(tile * own_rows, own_rows)] = sent[k, me]

    def wait_bytes(ref, sem):
        pltpu.make_async_copy(ref, ref, sem).wait()

    band_ref[...] = jnp.zeros_like(band_ref)
    band_ref[:, : band_in.shape[1]] = band_in[...].astype(F32)
    spread(0, 0)
    pl.semaphore_wait(barrier, ndest - 1 + nteam - nxh * nxl)

    to_xl, to_z, to_c = c, (xl * nz + z) // nc, (xl * nz + z) % nc
    home = (to_xl == xl) & (to_z == z) & (to_c == c)
    quarter = pltpu.make_async_remote_copy(
        src_ref=cq_ref,
        dst_ref=stage,
        send_sem=c_go,
        recv_sem=c_in,
        device_id={"xl": to_xl, "z": to_z, "c": to_c},
        device_id_type=MESH,
    )

    @pl.when(jnp.logical_not(home))
    def _():
        quarter.start()

    @pl.when(home)
    def _():
        stage[...] = cq_ref[...]

    for side in range(nxl):
        here = (to_z == z) & (to_c == c) & (xl == side)

        @pl.when(jnp.logical_not(here))
        def _():
            pltpu.make_async_remote_copy(
                src_ref=band_ref,
                dst_ref=bands.at[c],
                send_sem=b_go.at[side],
                recv_sem=b_in.at[c],
                device_id={"xl": side, "z": to_z, "c": to_c},
                device_id_type=MESH,
            ).start()

        @pl.when(here)
        def _():
            bands[c] = band_ref[...]

    send(0)
    spread(1, 0)
    send(1)

    @pl.when(jnp.logical_not(home))
    def _():
        quarter.wait()

    quarter_cols = cq_ref.shape[0]
    slot = xh * cols + xl * half + y * quarter_cols

    def forward(n, carry):
        p = (team + n) % nteam
        pltpu.make_async_remote_copy(
            src_ref=stage,
            dst_ref=ctrl.at[pl.ds(slot, quarter_cols)],
            send_sem=f_go,
            recv_sem=f_in,
            device_id=at_team(p),
            device_id_type=MESH,
        ).start()
        return carry

    lax.fori_loop(1, nteam, forward, 0)
    ctrl[pl.ds(slot, quarter_cols)] = stage[...]

    def rest(k, carry):
        spread(k, 0)
        send(k)
        return carry

    lax.fori_loop(2, nk, rest, 0)

    members, obs = hx_ref.shape
    lanes = gram.shape[2]
    region = xh * ny + y
    nregion = nxh * ny

    def at_region(g):
        return {"xh": g // ny, "y": g % ny}

    weighted = (hx_ref[...].astype(F32) * prec_ref[...]).astype(BF)
    padded = jnp.concatenate([hx_ref[...], jnp.zeros((lanes - members, obs), BF)], axis=0)
    lane = lax.broadcasted_iota(jnp.int32, (members, lanes), 1)
    row_of = lax.broadcasted_iota(jnp.int32, (members, lanes), 0)
    for g in range(nregion):
        inside = region_ref[...] == g
        masked = jnp.where(inside, weighted.astype(F32), 0.0)
        right = jnp.sum(masked * innov_ref[...], axis=1, keepdims=True)
        product = lax.dot_general(
            masked.astype(BF), padded, (((1,), (1,)), ((), ())), preferred_element_type=F32
        )
        gram[g] = jnp.where(lane == members, right, product)

    def hand_gram(n, carry):
        g = (region + n) % nregion
        pltpu.make_async_remote_copy(
            src_ref=gram.at[g],
            dst_ref=grams.at[region],
            send_sem=g_go,
            recv_sem=g_in,
            device_id=at_region(g),
            device_id_type=MESH,
        ).start()
        return carry

    lax.fori_loop(1, nregion, hand_gram, 0)
    grams[region] = gram[region]

    def gather_system():
        wait_bytes(grams.at[pl.ds(0, nregion - 1)], g_in)
        value = grams[0]
        for g in range(1, nregion):
            value = value + grams[g]
        system[...] = value + jnp.where(lane == row_of, members - 1.0, 0.0)

    def eliminate(j, carry):
        value = system[...]
        pivot_row = system[pl.ds(j, 1), :]
        column = jnp.sum(jnp.where(lane == j, value, 0.0), axis=1, keepdims=True)
        pivot = jnp.sum(jnp.where(lane[:1] == j, pivot_row, 0.0), axis=1, keepdims=True)
        scaled = pivot_row / pivot
        system[...] = jnp.where(row_of == j, scaled, value - column * scaled)
        return carry

    def hand_answer():
        solved = jnp.sum(
            jnp.where(lane == members, system[...], 0.0), axis=1, keepdims=True
        )
        across = jnp.sum(jnp.where(lane == row_of, solved, 0.0), axis=0, keepdims=True)
        answer[...] = jnp.broadcast_to(across, answer.shape)

        def one(n, carry):
            pltpu.make_async_remote_copy(
                src_ref=answer,
                dst_ref=answers.at[region],
                send_sem=w_go,
                recv_sem=w_in,
                device_id=at_region((region + n) % nregion),
                device_id_type=MESH,
            ).start()
            return carry

        lax.fori_loop(1, nregion, one, 0)
        answers[region] = answer[...]

    span = WIN * cols
    p_id = lax.broadcasted_iota(jnp.int32, (cols * GR, span), 0)
    q_id = lax.broadcasted_iota(jnp.int32, (cols * GR, span), 1)
    same = q_id % cols == p_id // GR

    rw_all[...] = jnp.zeros_like(rw_all)
    rw_all[:3, :] = rw_ref[...].astype(F32)
    lev_t = lax.dot_general(
        one_hot((lev, lev), lambda p: p, lambda q: q),
        lev_in[...],
        (((1,), (1,)), ((), ())),
        preferred_element_type=F32,
    ).astype(BF)
    lev_ref[...] = jnp.zeros_like(lev_ref)
    lev_ref[:lev, :lev] = lev_t
    lev_ref[lev:, lev:] = lev_t

    def stencil(g, carry):
        take = (
            lax.broadcasted_iota(jnp.int32, (cols * GR, groups * GR), 1)
            == lax.broadcasted_iota(jnp.int32, (cols * GR, groups * GR), 0) % GR + g * GR
        ).astype(BF)
        w = lax.dot_general(
            take, rw_all[...].astype(BF), (((1,), (1,)), ((), ())), preferred_element_type=F32
        )
        start = jnp.minimum(jnp.maximum(g * (GR // 2) - 1, 0), coarse - WIN)
        full = jnp.zeros((cols * GR, span), F32)
        for s in range(3):
            wanted = g * (GR // 2) - start + (p_id % GR) // 2 + s - 1
            full = jnp.where(same & (q_id // cols == wanted), w[:, s : s + 1], full)
        sten[g] = full.astype(BF)
        return carry

    lax.fori_loop(0, groups, stencil, 0)

    for side in range(2):
        here = (xl == block // nz) & (z == block % nz) & (c == side)

        @pl.when(jnp.logical_not(here))
        def _():
            wait_bytes(bands.at[side], b_in.at[side])

    narrow = jnp.concatenate(
        [bands[0], pltpu.roll(bands[1], half, 1)], axis=0
    ).astype(BF)
    wide_src = 4 * half * GR
    take_src = one_hot((narrow.shape[1], wide_src), lambda m: m, lambda q: q // GR)
    take_col = one_hot((cols * GR, cols), lambda p: p // GR, lambda j: j)
    wide = jnp.dot(narrow, take_src, preferred_element_type=F32).astype(BF)
    full = jnp.dot(take_col, wide, preferred_element_type=F32)
    p_id2 = lax.broadcasted_iota(jnp.int32, full.shape, 0)
    q_id2 = lax.broadcasted_iota(jnp.int32, full.shape, 1)
    full = jnp.where(p_id2 % GR == q_id2 % GR, full, 0.0).astype(BF)
    side_rows = half * GR
    for i in range(2):
        bandf[i] = full[i * side_rows : (i + 1) * side_rows, i * side_rows : (i + 3) * side_rows]

    acc[...] = jnp.zeros_like(acc)

    def refine_group(k, group):
        start = window_start(group, coarse)
        windows = [land[k, t, pl.ds(start, WIN)].reshape(WIN * cols, lev) for t in range(2)]
        out = jnp.dot(
            sten[group], jnp.concatenate(windows, axis=1), preferred_element_type=F32
        ).astype(BF)
        return [out[:, t * lev : (t + 1) * lev].reshape(cols, GR, lev) for t in range(2)]

    def project(k):
        for group in range(groups):
            rows = pl.ds(group * GR, GR)
            first, second = refine_group(k, group)
            fine[k, 0, :, rows, :] = first
            fine[k, 1, :, rows, :] = second
            both = first.astype(F32) * ctrl[pl.ds(0, cols), rows, :].astype(F32)
            both = both + second.astype(F32) * ctrl[pl.ds(cols, cols), rows, :].astype(F32)
            both = both.astype(BF)
            field[k, 1, :, rows, :] = both[:half]
            field[k, 2, :, rows, :] = both[half:]

    def halo_copy(k, side):
        other = block + 1 if side == 0 else block - 1
        return pltpu.make_async_remote_copy(
            src_ref=field.at[k, 2 - side],
            dst_ref=field.at[k, 3 * side],
            send_sem=h_go.at[k, side],
            recv_sem=h_in.at[k, side],
            device_id={"z": other // nc, "c": other % nc},
            device_id_type=MESH,
        )

    nl, ll = ny, lev // ny

    def hand_columns(i, start, count):
        for j in range(start, start + count):
            for t in range(2):
                turned = acc[t, i * half + j].T.astype(BF)
                for q in range(nl):
                    parts[(t * nxl + i) * ny + q, j] = turned[q * ll : (q + 1) * ll]
        for j in range(start, start + count):
            for t in range(2):
                for q in range(nl):
                    p = (t * nxl + i) * ny + q

                    @pl.when(p != team)
                    def _():
                        pltpu.make_async_remote_copy(
                            src_ref=parts.at[p, j],
                            dst_ref=sums.at[team, j],
                            send_sem=p_go,
                            recv_sem=p_in,
                            device_id=at_team(p),
                            device_id_type=MESH,
                        ).start()

    sends = (block < blocks - 1, block > 0)
    near = 1 - c
    edge = ((c == 0) & (block == 0)) | ((c == nc - 1) & (block == blocks - 1))

    def localize(k, i, side):
        @pl.when((side == near) | jnp.logical_not(edge))
        def _():
            wait_bytes(field.at[k, 3 * side], h_in.at[k, side])

        @pl.when((side != near) & edge)
        def _():
            field[k, 3 * side] = jnp.zeros(field.shape[2:], BF)

        for group in range(0, groups, 2):
            wide = []
            for g in (group, group + 1):
                rows = pl.ds(g * GR, GR)
                pieces = [field[k, i + n, :, rows, :].reshape(half * GR, lev) for n in range(3)]
                wide.append(jnp.concatenate(pieces, axis=0))
            mixed = jnp.dot(
                bandf[i], jnp.concatenate(wide, axis=1), preferred_element_type=F32
            ).astype(BF)
            for n, g in enumerate((group, group + 1)):
                banded[:, pl.ds(g * GR, GR), :] = mixed[:, n * lev : (n + 1) * lev].reshape(
                    half, GR, lev
                )
        for j in range(0, half, 2):
            pair = jnp.concatenate([banded[j], banded[j + 1]], axis=1)
            mixed = jnp.dot(row_ref[...], pair, preferred_element_type=F32).astype(BF)
            local = jnp.dot(mixed, lev_ref[...], preferred_element_type=F32)
            for n in range(2):
                part = local[:, n * lev : (n + 1) * lev]
                at = i * half + j + n
                for t in range(2):
                    acc[t, at] += fine[k, t, at].astype(F32) * part

            @pl.when(k == nk - 1)
            def _():
                hand_columns(i, j, 2)

    def wait_all_but_one(k, sem):
        wait_bytes(sent.at[k, pl.ds(0, ndest - 1)], sem.at[k])

    share = -(-members // (nk - 2))

    def step(k, carry):
        @pl.when(k < nk)
        def _():
            wait_all_but_one(k, s_in)

            @pl.when(k == 0)
            def _():
                wait_bytes(ctrl.at[pl.ds(0, (nteam - 1) * quarter_cols)], f_in)

            project(k)
            for side in range(2):

                @pl.when(sends[side])
                def _():
                    halo_copy(k, side).start()

            @pl.when(k == 1)
            def _():
                gather_system()

            @pl.when(k >= 1)
            def _():
                last = jnp.minimum(k * share, members)
                lax.fori_loop(jnp.minimum((k - 1) * share, members), last, eliminate, 0)

            @pl.when(k == nk - 1)
            def _():
                hand_answer()

        first = (k >= 1) & (k <= nk)

        @pl.when(k >= 1)
        def _():
            localize(
                jnp.where(first, k - 1, k - 1 - nk),
                jnp.where(first, near, 1 - near),
                jnp.where(first, near, 1 - near),
            )

        return carry

    lax.fori_loop(0, 2 * nk + 1, step, 0)

    sums[team] = parts[team]
    wait_bytes(sums.at[pl.ds(0, nteam - 1)], p_in)
    dest = (tile * 2) % (blocks * nxl) + xl
    d_block = dest % blocks
    stays = dest == tile
    for j in range(half):
        value = sums[0, j].astype(F32)
        for p in range(1, nteam):
            value = value + sums[p, j].astype(F32)
        total[j] = (value * scale).astype(BF)

        @pl.when(jnp.logical_not(stays))
        def _():
            pltpu.make_async_remote_copy(
                src_ref=total.at[j],
                dst_ref=moved.at[j],
                send_sem=m_go,
                recv_sem=m_in,
                device_id={"xl": dest // blocks, "z": d_block // nc, "c": d_block % nc},
                device_id_type=MESH,
            ).start()

        @pl.when(stays)
        def _():
            moved[j] = total[j]

    def left(k, carry):
        wait_all_but_one(k, s_go)
        for side in range(2):

            @pl.when(sends[side])
            def _():
                wait_bytes(field.at[k, side], h_go.at[k, side])

        return carry

    lax.fori_loop(0, nk, left, 0)
    wait_bytes(ctrl.at[pl.ds(0, (nteam - 1) * quarter_cols)], f_go)
    wait_bytes(sums.at[pl.ds(0, nteam - 1)], p_go)
    wait_bytes(grams.at[pl.ds(0, nregion - 1)], g_go)
    wait_bytes(answers.at[pl.ds(0, nregion - 1)], w_go)
    wait_bytes(answers.at[pl.ds(0, nregion - 1)], w_in)
    for g in range(nregion):
        w_ref[pl.ds(g, 1), :] = answers[g, :1, :members]
    for side in range(nxl):
        here = (to_z == z) & (to_c == c) & (xl == side)

        @pl.when(jnp.logical_not(here))
        def _():
            wait_bytes(bands.at[side], b_go.at[side])

    @pl.when(jnp.logical_not(stays))
    def _():
        wait_bytes(total, m_go)
        wait_bytes(moved, m_in)

    for j in range(half):
        o_ref[j] = moved[j]


def body(
    ens_coarse,
    col_interp,
    row_weights,
    ctrl_vec,
    band_loc,
    row_loc,
    level_loc,
    hx_pert,
    innov,
    obs_prec,
    obs_region,
):
    nxh, nxl, nz, nc, ny = (lax.axis_size(a) for a in ("xh", "xl", "z", "c", "y"))
    _, members, lev, own_rows, coarse_cols = ens_coarse.shape
    fine_cols = col_interp.shape[0]
    fine_rows = row_weights.shape[1]
    blocks = nz * nc
    cols = fine_cols // blocks
    half = cols // 2
    group = members // (nxh * nxl)
    tiles = nxl * blocks
    coarse = tiles * own_rows
    total_members = hx_pert.shape[1]
    nteam = nxh * nxl * ny
    quarter = half // ny
    lanes = 128

    x = ens_coarse.reshape(members, lev * own_rows, coarse_cols)
    mine = lax.dynamic_slice_in_dim(ctrl_vec[0], lax.axis_index("y") * quarter, quarter, 1)
    mine = jnp.transpose(mine.astype(BF), (1, 2, 0))

    vm = pl.BlockSpec(memory_space=pltpu.VMEM)
    dma = pltpu.SemaphoreType.DMA
    increment, weights = pl.pallas_call(
        lambda *refs: main_kernel((nxh, nxl, nz, nc, ny, 1.0 / (total_members - 1)), refs),
        in_specs=[vm] * 11,
        out_specs=(vm, vm),
        out_shape=(
            jax.ShapeDtypeStruct((half, lev // ny, fine_rows), BF),
            jax.ShapeDtypeStruct((NREG, total_members), F32),
        ),
        scratch_shapes=[
            pltpu.VMEM((2 * lev, 2 * lev), BF),
            pltpu.VMEM((half, lanes), F32),
            pltpu.VMEM((8, fine_rows), F32),
            pltpu.VMEM((own_rows * lev, own_rows * lev), BF),
            pltpu.VMEM((group, nxh * tiles, own_rows, cols, lev), BF),
            pltpu.VMEM((group, nxh, coarse, cols, lev), BF),
            pltpu.VMEM((fine_rows // GR, cols * GR, WIN * cols), BF),
            pltpu.VMEM((quarter, fine_rows, lev), BF),
            pltpu.VMEM((nxh * cols, fine_rows, lev), BF),
            pltpu.VMEM((2, half, lanes), F32),
            pltpu.VMEM((2, half * GR, 3 * half * GR), BF),
            pltpu.VMEM((group, 4, half, fine_rows, lev), BF),
            pltpu.VMEM((group, nxh, cols, fine_rows, lev), BF),
            pltpu.VMEM((half, fine_rows, lev), BF),
            pltpu.VMEM((nxh, cols, fine_rows, lev), F32),
            pltpu.VMEM((nteam, half, lev // ny, fine_rows), BF),
            pltpu.VMEM((nteam, half, lev // ny, fine_rows), BF),
            pltpu.VMEM((half, lev // ny, fine_rows), BF),
            pltpu.VMEM((half, lev // ny, fine_rows), BF),
            pltpu.VMEM((NREG, total_members, lanes), F32),
            pltpu.VMEM((NREG, total_members, lanes), F32),
            pltpu.VMEM((total_members, lanes), F32),
            pltpu.VMEM((8, lanes), F32),
            pltpu.VMEM((NREG, 8, lanes), F32),
            dma((group,)),
            dma((group,)),
            dma((group, 2)),
            dma((group, 2)),
            dma,
            dma,
            dma,
            dma,
            dma((2,)),
            dma((2,)),
            *[dma] * 8,
        ],
        compiler_params=pltpu.CompilerParams(
            collective_id=0, has_side_effects=True, vmem_limit_bytes=62 << 20
        ),
    )(x, col_interp, row_weights, mine, band_loc, row_loc, level_loc, hx_pert[0], innov, obs_prec, obs_region)
    increment = jnp.transpose(increment, (1, 0, 2)).astype(F32)
    return (increment[None], weights)


def solution(mesh):
    shape = (2, 2, mesh.shape["tile"] // 4, 2, mesh.shape["mem"])
    fine_mesh = Mesh(mesh.devices.reshape(shape), ("xh", "xl", "z", "c", "y"))
    tile = ("xl", "z", "c")
    obs = (*tile, "y")
    placed = (
        P("xh", "y", None, tile, None),
        P(),
        P(),
        P("xh", None, tile, None),
        P(tile, None),
        P(),
        P(),
        P("xh", None, obs),
        P("xh", obs),
        P("xh", obs),
        P("xh", obs),
    )
    return jax.shard_map(
        body,
        mesh=fine_mesh,
        in_specs=placed,
        out_specs=(P("xh", "y", tile, None), P(tile, None)),
        check_vma=False,
    )
```

```python
import functools

import jax
import jax.numpy as jnp
from jax import lax
from jax.experimental import pallas as pl
from jax.experimental.pallas import tpu as pltpu
from jax.sharding import Mesh, PartitionSpec as P

NREG = 8
BF = jnp.bfloat16
F32 = jnp.float32
GR = 16
WIN = 10


MESH = pl.DeviceIdType.MESH


def one_hot(shape, of_row, of_col):
    row = lax.broadcasted_iota(jnp.int32, shape, 0)
    col = lax.broadcasted_iota(jnp.int32, shape, 1)
    return (of_row(row) == of_col(col)).astype(BF)


def window_start(group, coarse_rows):
    return min(max(group * GR // 2 - 1, 0), coarse_rows - WIN)


def main_kernel(sizes, refs):
    nxh, nxl, nz, nc, ny, scale = sizes
    x_ref, ci_ref, rw_ref, cq_ref, band_in, row_ref, lev_in, *refs = refs
    hx_ref, innov_ref, prec_ref, region_ref, o_ref, w_ref, *refs = refs
    lev_ref, band_ref, rw_all, perm, sent, land, sten, stage, ctrl, bands, bandf, field, fine, banded, acc, *refs = refs
    parts, sums, total, moved, turned_out, gram, grams, system, answer, answers, *sems = refs
    s_go, s_in, h_go, h_in, c_go, c_in, f_go, f_in, b_go, b_in, p_go, p_in, m_go, m_in, *sems = sems
    g_go, g_in, w_go, w_in = sems

    nk, ndest, own_rows, cols, lev = sent.shape
    coarse = land.shape[2]
    groups = sten.shape[0]
    half = cols // 2
    blocks = nz * nc
    xh, xl, z, c, y = (lax.axis_index(a) for a in ("xh", "xl", "z", "c", "y"))
    block = z * nc + c
    tile = xl * blocks + block
    me = (xh * nxl + xl) * blocks + block
    team = (xh * nxl + xl) * ny + y

    def at_dest(d):
        m, b = d // blocks, d % blocks
        return {"xh": m // nxl, "xl": m % nxl, "z": b // nc, "c": b % nc}

    def at_team(p):
        m = p // ny
        return {"xh": m // nxl, "xl": m % nxl, "y": p % ny}

    barrier = pltpu.get_barrier_semaphore()

    def greet(n, carry):
        pl.semaphore_signal(
            barrier, inc=1, device_id=at_dest((me + n) % ndest), device_id_type=MESH
        )
        return carry

    lax.fori_loop(1, ndest, greet, 0)
    nteam = nxh * nxl * ny

    def greet_team(n, carry):
        p = (team + n) % nteam

        @pl.when(p % ny != y)
        def _():
            pl.semaphore_signal(barrier, inc=1, device_id=at_team(p), device_id_type=MESH)

        return carry

    lax.fori_loop(1, nteam, greet_team, 0)

    flat = own_rows * lev
    perm[...] = one_hot(
        (flat, flat), lambda p: (p % lev) * own_rows + p // lev, lambda q: q
    )

    def spread(k, carry):
        def group_of(m, carry):
            by_row = jnp.dot(
                perm[...], x_ref[m * nk + k], preferred_element_type=F32
            ).astype(BF)
            out = lax.dot_general(
                ci_ref[...], by_row, (((1,), (1,)), ((), ())), preferred_element_type=F32
            ).astype(BF)
            for i in range(own_rows):
                sent[k, pl.ds(m * blocks, blocks), i] = out[:, i * lev : (i + 1) * lev].reshape(
                    blocks, cols, lev
                )
            return carry

        return lax.fori_loop(0, nxh * nxl, group_of, carry)

    def send(k):
        def one(n, carry):
            d = (me + n) % ndest
            pltpu.make_async_remote_copy(
                src_ref=sent.at[k, d],
                dst_ref=land.at[k, xh, pl.ds(tile * own_rows, own_rows)],
                send_sem=s_go.at[k],
                recv_sem=s_in.at[k],
                device_id=at_dest(d),
                device_id_type=MESH,
            ).start()
            return carry

        lax.fori_loop(1, ndest, one, 0)
        land[k, xh, pl.ds(tile * own_rows, own_rows)] = sent[k, me]

    def wait_bytes(ref, sem):
        pltpu.make_async_copy(ref, ref, sem).wait()

    band_ref[...] = jnp.zeros_like(band_ref)
    band_ref[:, : band_in.shape[1]] = band_in[...].astype(F32)
    spread(0, 0)
    pl.semaphore_wait(barrier, ndest - 1 + nteam - nxh * nxl)

    to_xl, to_z, to_c = c, (xl * nz + z) // nc, (xl * nz + z) % nc
    home = (to_xl == xl) & (to_z == z) & (to_c == c)
    quarter = pltpu.make_async_remote_copy(
        src_ref=cq_ref,
        dst_ref=stage,
        send_sem=c_go,
        recv_sem=c_in,
        device_id={"xl": to_xl, "z": to_z, "c": to_c},
        device_id_type=MESH,
    )

    @pl.when(jnp.logical_not(home))
    def _():
        quarter.start()

    @pl.when(home)
    def _():
        stage[...] = cq_ref[...]

    for side in range(nxl):
        here = (to_z == z) & (to_c == c) & (xl == side)

        @pl.when(jnp.logical_not(here))
        def _():
            pltpu.make_async_remote_copy(
                src_ref=band_ref,
                dst_ref=bands.at[c],
                send_sem=b_go.at[side],
                recv_sem=b_in.at[c],
                device_id={"xl": side, "z": to_z, "c": to_c},
                device_id_type=MESH,
            ).start()

        @pl.when(here)
        def _():
            bands[c] = band_ref[...]

    send(0)
    spread(1, 0)
    send(1)

    @pl.when(jnp.logical_not(home))
    def _():
        quarter.wait()

    quarter_cols = cq_ref.shape[0]
    slot = xh * cols + xl * half + y * quarter_cols

    def forward(n, carry):
        p = (team + n) % nteam
        pltpu.make_async_remote_copy(
            src_ref=stage,
            dst_ref=ctrl.at[pl.ds(slot, quarter_cols)],
            send_sem=f_go,
            recv_sem=f_in,
            device_id=at_team(p),
            device_id_type=MESH,
        ).start()
        return carry

    lax.fori_loop(1, nteam, forward, 0)
    ctrl[pl.ds(slot, quarter_cols)] = stage[...]

    def rest(k, carry):
        spread(k, 0)
        send(k)
        return carry

    lax.fori_loop(2, nk, rest, 0)

    members, obs = hx_ref.shape
    lanes = gram.shape[2]
    region = xh * ny + y
    nregion = nxh * ny

    def at_region(g):
        return {"xh": g // ny, "y": g % ny}

    weighted = (hx_ref[...].astype(F32) * prec_ref[...]).astype(BF)
    padded = jnp.concatenate([hx_ref[...], jnp.zeros((lanes - members, obs), BF)], axis=0)
    lane = lax.broadcasted_iota(jnp.int32, (members, lanes), 1)
    row_of = lax.broadcasted_iota(jnp.int32, (members, lanes), 0)
    for g in range(nregion):
        inside = region_ref[...] == g
        masked = jnp.where(inside, weighted.astype(F32), 0.0)
        right = jnp.sum(masked * innov_ref[...], axis=1, keepdims=True)
        product = lax.dot_general(
            masked.astype(BF), padded, (((1,), (1,)), ((), ())), preferred_element_type=F32
        )
        gram[g] = jnp.where(lane == members, right, product)

    def hand_gram(n, carry):
        g = (region + n) % nregion
        pltpu.make_async_remote_copy(
            src_ref=gram.at[g],
            dst_ref=grams.at[region],
            send_sem=g_go,
            recv_sem=g_in,
            device_id=at_region(g),
            device_id_type=MESH,
        ).start()
        return carry

    lax.fori_loop(1, nregion, hand_gram, 0)
    grams[region] = gram[region]

    def gather_system():
        wait_bytes(grams.at[pl.ds(0, nregion - 1)], g_in)
        value = grams[0]
        for g in range(1, nregion):
            value = value + grams[g]
        system[...] = value + jnp.where(lane == row_of, members - 1.0, 0.0)

    def eliminate(j, carry):
        value = system[...]
        pivot_row = system[pl.ds(j, 1), :]
        column = jnp.sum(jnp.where(lane == j, value, 0.0), axis=1, keepdims=True)
        pivot = jnp.sum(jnp.where(lane[:1] == j, pivot_row, 0.0), axis=1, keepdims=True)
        scaled = pivot_row / pivot
        system[...] = jnp.where(row_of == j, scaled, value - column * scaled)
        return carry

    def hand_answer():
        solved = jnp.sum(
            jnp.where(lane == members, system[...], 0.0), axis=1, keepdims=True
        )
        across = jnp.sum(jnp.where(lane == row_of, solved, 0.0), axis=0, keepdims=True)
        answer[...] = jnp.broadcast_to(across, answer.shape)

        def one(n, carry):
            pltpu.make_async_remote_copy(
                src_ref=answer,
                dst_ref=answers.at[region],
                send_sem=w_go,
                recv_sem=w_in,
                device_id=at_region((region + n) % nregion),
                device_id_type=MESH,
            ).start()
            return carry

        lax.fori_loop(1, nregion, one, 0)
        answers[region] = answer[...]

    span = WIN * cols
    p_id = lax.broadcasted_iota(jnp.int32, (cols * GR, span), 0)
    q_id = lax.broadcasted_iota(jnp.int32, (cols * GR, span), 1)
    same = q_id % cols == p_id // GR

    rw_all[...] = jnp.zeros_like(rw_all)
    rw_all[:3, :] = rw_ref[...].astype(F32)
    lev_t = lax.dot_general(
        one_hot((lev, lev), lambda p: p, lambda q: q),
        lev_in[...],
        (((1,), (1,)), ((), ())),
        preferred_element_type=F32,
    ).astype(BF)
    lev_ref[...] = jnp.zeros_like(lev_ref)
    lev_ref[:lev, :lev] = lev_t
    lev_ref[lev:, lev:] = lev_t

    def stencil(g, carry):
        take = (
            lax.broadcasted_iota(jnp.int32, (cols * GR, groups * GR), 1)
            == lax.broadcasted_iota(jnp.int32, (cols * GR, groups * GR), 0) % GR + g * GR
        ).astype(BF)
        w = lax.dot_general(
            take, rw_all[...].astype(BF), (((1,), (1,)), ((), ())), preferred_element_type=F32
        )
        start = jnp.minimum(jnp.maximum(g * (GR // 2) - 1, 0), coarse - WIN)
        full = jnp.zeros((cols * GR, span), F32)
        for s in range(3):
            wanted = g * (GR // 2) - start + (p_id % GR) // 2 + s - 1
            full = jnp.where(same & (q_id // cols == wanted), w[:, s : s + 1], full)
        sten[g] = full.astype(BF)
        return carry

    lax.fori_loop(0, groups, stencil, 0)

    for side in range(2):
        here = (xl == block // nz) & (z == block % nz) & (c == side)

        @pl.when(jnp.logical_not(here))
        def _():
            wait_bytes(bands.at[side], b_in.at[side])

    narrow = jnp.concatenate(
        [bands[0], pltpu.roll(bands[1], half, 1)], axis=0
    ).astype(BF)
    wide_src = 4 * half * GR
    take_src = one_hot((narrow.shape[1], wide_src), lambda m: m, lambda q: q // GR)
    take_col = one_hot((cols * GR, cols), lambda p: p // GR, lambda j: j)
    wide = jnp.dot(narrow, take_src, preferred_element_type=F32).astype(BF)
    full = jnp.dot(take_col, wide, preferred_element_type=F32)
    p_id2 = lax.broadcasted_iota(jnp.int32, full.shape, 0)
    q_id2 = lax.broadcasted_iota(jnp.int32, full.shape, 1)
    full = jnp.where(p_id2 % GR == q_id2 % GR, full, 0.0).astype(BF)
    side_rows = half * GR
    for i in range(2):
        bandf[i] = full[i * side_rows : (i + 1) * side_rows, i * side_rows : (i + 3) * side_rows]

    acc[...] = jnp.zeros_like(acc)

    def refine_group(k, group):
        start = window_start(group, coarse)
        windows = [land[k, t, pl.ds(start, WIN)].reshape(WIN * cols, lev) for t in range(2)]
        out = jnp.dot(
            sten[group], jnp.concatenate(windows, axis=1), preferred_element_type=F32
        ).astype(BF)
        return [out[:, t * lev : (t + 1) * lev].reshape(cols, GR, lev) for t in range(2)]

    def project(k):
        for group in range(groups):
            rows = pl.ds(group * GR, GR)
            first, second = refine_group(k, group)
            fine[k, 0, :, rows, :] = first
            fine[k, 1, :, rows, :] = second
            both = first.astype(F32) * ctrl[pl.ds(0, cols), rows, :].astype(F32)
            both = both + second.astype(F32) * ctrl[pl.ds(cols, cols), rows, :].astype(F32)
            both = both.astype(BF)
            field[k, 1, :, rows, :] = both[:half]
            field[k, 2, :, rows, :] = both[half:]

    def halo_copy(k, side):
        other = block + 1 if side == 0 else block - 1
        return pltpu.make_async_remote_copy(
            src_ref=field.at[k, 2 - side],
            dst_ref=field.at[k, 3 * side],
            send_sem=h_go.at[k, side],
            recv_sem=h_in.at[k, side],
            device_id={"z": other // nc, "c": other % nc},
            device_id_type=MESH,
        )

    nl, ll = ny, lev // ny

    def hand_columns(i, start, count):
        for j in range(start, start + count):
            for t in range(2):
                turned = acc[t, i * half + j].T.astype(BF)
                for q in range(nl):
                    parts[(t * nxl + i) * ny + q, j] = turned[q * ll : (q + 1) * ll]
        for j in range(start, start + count):
            for t in range(2):
                for q in range(nl):
                    p = (t * nxl + i) * ny + q

                    @pl.when(p != team)
                    def _():
                        pltpu.make_async_remote_copy(
                            src_ref=parts.at[p, j],
                            dst_ref=sums.at[team, j],
                            send_sem=p_go,
                            recv_sem=p_in.at[j],
                            device_id=at_team(p),
                            device_id_type=MESH,
                        ).start()

    sends = (block < blocks - 1, block > 0)
    near = 1 - c
    edge = ((c == 0) & (block == 0)) | ((c == nc - 1) & (block == blocks - 1))

    def localize(k, i, side):
        @pl.when((side == near) | jnp.logical_not(edge))
        def _():
            wait_bytes(field.at[k, 3 * side], h_in.at[k, side])

        @pl.when((side != near) & edge)
        def _():
            field[k, 3 * side] = jnp.zeros(field.shape[2:], BF)

        for group in range(0, groups, 2):
            wide = []
            for g in (group, group + 1):
                rows = pl.ds(g * GR, GR)
                pieces = [field[k, i + n, :, rows, :].reshape(half * GR, lev) for n in range(3)]
                wide.append(jnp.concatenate(pieces, axis=0))
            mixed = jnp.dot(
                bandf[i], jnp.concatenate(wide, axis=1), preferred_element_type=F32
            ).astype(BF)
            for n, g in enumerate((group, group + 1)):
                banded[:, pl.ds(g * GR, GR), :] = mixed[:, n * lev : (n + 1) * lev].reshape(
                    half, GR, lev
                )
        for j in range(0, half, 2):
            pair = jnp.concatenate([banded[j], banded[j + 1]], axis=1)
            mixed = jnp.dot(row_ref[...], pair, preferred_element_type=F32).astype(BF)
            local = jnp.dot(mixed, lev_ref[...], preferred_element_type=F32)
            for n in range(2):
                part = local[:, n * lev : (n + 1) * lev]
                at = i * half + j + n
                for t in range(2):
                    acc[t, at] += fine[k, t, at].astype(F32) * part

            @pl.when(k == nk - 1)
            def _():
                hand_columns(i, j, 2)

    def wait_all_but_one(k, sem):
        wait_bytes(sent.at[k, pl.ds(0, ndest - 1)], sem.at[k])

    dest = (tile * 2) % (blocks * nxl) + xl
    d_block = dest % blocks
    stays = dest == tile

    def finish():
        for j in range(half):
            wait_bytes(sums.at[pl.ds(0, nteam - 1), j], p_in.at[j])
            sums[team, j] = parts[team, j]
            value = sums[0, j].astype(F32)
            for p in range(1, nteam):
                value = value + sums[p, j].astype(F32)
            total[j] = (value * scale).astype(BF)

            @pl.when(jnp.logical_not(stays))
            def _():
                pltpu.make_async_remote_copy(
                    src_ref=total.at[j],
                    dst_ref=moved.at[j],
                    send_sem=m_go,
                    recv_sem=m_in,
                    device_id={"xl": dest // blocks, "z": d_block // nc, "c": d_block % nc},
                    device_id_type=MESH,
                ).start()

            @pl.when(stays)
            def _():
                moved[j] = total[j]

    share = -(-members // (nk - 2))

    def step(k, carry):
        @pl.when(k < nk)
        def _():
            wait_all_but_one(k, s_in)

            @pl.when(k == 0)
            def _():
                wait_bytes(ctrl.at[pl.ds(0, (nteam - 1) * quarter_cols)], f_in)

            project(k)
            for side in range(2):

                @pl.when(sends[side])
                def _():
                    halo_copy(k, side).start()

            @pl.when(k == 1)
            def _():
                gather_system()

            @pl.when(k >= 1)
            def _():
                last = jnp.minimum(k * share, members)
                lax.fori_loop(jnp.minimum((k - 1) * share, members), last, eliminate, 0)

            @pl.when(k == nk - 1)
            def _():
                hand_answer()

        @pl.when((k == 2 * nk) & (xl == near))
        def _():
            finish()

        first = (k >= 1) & (k <= nk)

        @pl.when(k >= 1)
        def _():
            localize(
                jnp.where(first, k - 1, k - 1 - nk),
                jnp.where(first, near, 1 - near),
                jnp.where(first, near, 1 - near),
            )

        return carry

    lax.fori_loop(0, 2 * nk + 1, step, 0)

    @pl.when(xl != near)
    def _():
        finish()

    def left(k, carry):
        wait_all_but_one(k, s_go)
        for side in range(2):

            @pl.when(sends[side])
            def _():
                wait_bytes(field.at[k, side], h_go.at[k, side])

        return carry

    lax.fori_loop(0, nk, left, 0)
    wait_bytes(ctrl.at[pl.ds(0, (nteam - 1) * quarter_cols)], f_go)
    wait_bytes(sums.at[pl.ds(0, nteam - 1)], p_go)
    wait_bytes(grams.at[pl.ds(0, nregion - 1)], g_go)
    wait_bytes(answers.at[pl.ds(0, nregion - 1)], w_go)
    wait_bytes(answers.at[pl.ds(0, nregion - 1)], w_in)
    for g in range(nregion):
        w_ref[pl.ds(g, 1), :] = answers[g, :1, :members]
    for side in range(nxl):
        here = (to_z == z) & (to_c == c) & (xl == side)

        @pl.when(jnp.logical_not(here))
        def _():
            wait_bytes(bands.at[side], b_go.at[side])

    @pl.when(jnp.logical_not(stays))
    def _():
        wait_bytes(total, m_go)
        wait_bytes(moved, m_in)

    for j in range(half):
        turned_out[:, j, :] = moved[j].astype(F32)
    o_ref[...] = turned_out[...].astype(BF)


def body(
    ens_coarse,
    col_interp,
    row_weights,
    ctrl_vec,
    band_loc,
    row_loc,
    level_loc,
    hx_pert,
    innov,
    obs_prec,
    obs_region,
):
    nxh, nxl, nz, nc, ny = (lax.axis_size(a) for a in ("xh", "xl", "z", "c", "y"))
    _, members, lev, own_rows, coarse_cols = ens_coarse.shape
    fine_cols = col_interp.shape[0]
    fine_rows = row_weights.shape[1]
    blocks = nz * nc
    cols = fine_cols // blocks
    half = cols // 2
    group = members // (nxh * nxl)
    tiles = nxl * blocks
    coarse = tiles * own_rows
    total_members = hx_pert.shape[1]
    nteam = nxh * nxl * ny
    quarter = half // ny
    lanes = 128

    x = ens_coarse.reshape(members, lev * own_rows, coarse_cols)
    mine = lax.dynamic_slice_in_dim(ctrl_vec[0], lax.axis_index("y") * quarter, quarter, 1)
    mine = jnp.transpose(mine.astype(BF), (1, 2, 0))

    vm = pl.BlockSpec(memory_space=pltpu.VMEM)
    dma = pltpu.SemaphoreType.DMA
    increment, weights = pl.pallas_call(
        lambda *refs: main_kernel((nxh, nxl, nz, nc, ny, 1.0 / (total_members - 1)), refs),
        in_specs=[vm] * 11,
        out_specs=(vm, vm),
        out_shape=(
            jax.ShapeDtypeStruct((lev // ny, half, fine_rows), BF),
            jax.ShapeDtypeStruct((NREG, total_members), F32),
        ),
        scratch_shapes=[
            pltpu.VMEM((2 * lev, 2 * lev), BF),
            pltpu.VMEM((half, lanes), F32),
            pltpu.VMEM((8, fine_rows), F32),
            pltpu.VMEM((own_rows * lev, own_rows * lev), BF),
            pltpu.VMEM((group, nxh * tiles, own_rows, cols, lev), BF),
            pltpu.VMEM((group, nxh, coarse, cols, lev), BF),
            pltpu.VMEM((fine_rows // GR, cols * GR, WIN * cols), BF),
            pltpu.VMEM((quarter, fine_rows, lev), BF),
            pltpu.VMEM((nxh * cols, fine_rows, lev), BF),
            pltpu.VMEM((2, half, lanes), F32),
            pltpu.VMEM((2, half * GR, 3 * half * GR), BF),
            pltpu.VMEM((group, 4, half, fine_rows, lev), BF),
            pltpu.VMEM((group, nxh, cols, fine_rows, lev), BF),
            pltpu.VMEM((half, fine_rows, lev), BF),
            pltpu.VMEM((nxh, cols, fine_rows, lev), F32),
            pltpu.VMEM((nteam, half, lev // ny, fine_rows), BF),
            pltpu.VMEM((nteam, half, lev // ny, fine_rows), BF),
            pltpu.VMEM((half, lev // ny, fine_rows), BF),
            pltpu.VMEM((half, lev // ny, fine_rows), BF),
            pltpu.VMEM((lev // ny, half, fine_rows), F32),
            pltpu.VMEM((NREG, total_members, lanes), F32),
            pltpu.VMEM((NREG, total_members, lanes), F32),
            pltpu.VMEM((total_members, lanes), F32),
            pltpu.VMEM((8, lanes), F32),
            pltpu.VMEM((NREG, 8, lanes), F32),
            dma((group,)),
            dma((group,)),
            dma((group, 2)),
            dma((group, 2)),
            *[dma] * 4,
            dma((2,)),
            dma((2,)),
            dma,
            dma((half,)),
            *[dma] * 6,
        ],
        compiler_params=pltpu.CompilerParams(
            collective_id=0, has_side_effects=True, vmem_limit_bytes=62 << 20
        ),
    )(x, col_interp, row_weights, mine, band_loc, row_loc, level_loc, hx_pert[0], innov, obs_prec, obs_region)
    return (increment.astype(F32)[None], weights)


def solution(mesh):
    shape = (2, 2, mesh.shape["tile"] // 4, 2, mesh.shape["mem"])
    fine_mesh = Mesh(mesh.devices.reshape(shape), ("xh", "xl", "z", "c", "y"))
    tile = ("xl", "z", "c")
    obs = (*tile, "y")
    placed = (
        P("xh", "y", None, tile, None),
        P(),
        P(),
        P("xh", None, tile, None),
        P(tile, None),
        P(),
        P(),
        P("xh", None, obs),
        P("xh", obs),
        P("xh", obs),
        P("xh", obs),
    )
    return jax.shard_map(
        body,
        mesh=fine_mesh,
        in_specs=placed,
        out_specs=(P("xh", "y", tile, None), P(tile, None)),
        check_vma=False,
    )
```

```python
import functools

import jax
import jax.numpy as jnp
from jax import lax
from jax.experimental import pallas as pl
from jax.experimental.pallas import tpu as pltpu
from jax.sharding import Mesh, PartitionSpec as P

NREG = 8
BF = jnp.bfloat16
F32 = jnp.float32
GR = 16
WIN = 10


MESH = pl.DeviceIdType.MESH


def one_hot(shape, of_row, of_col):
    row = lax.broadcasted_iota(jnp.int32, shape, 0)
    col = lax.broadcasted_iota(jnp.int32, shape, 1)
    return (of_row(row) == of_col(col)).astype(BF)


def window_start(group, coarse_rows):
    return min(max(group * GR // 2 - 1, 0), coarse_rows - WIN)


def main_kernel(sizes, refs):
    nxh, nxl, nz, nc, ny, scale = sizes
    x_ref, ci_ref, rw_ref, cq_ref, band_in, row_ref, lev_in, *refs = refs
    hx_ref, innov_ref, prec_ref, region_ref, o_ref, w_ref, *refs = refs
    lev_ref, band_ref, rw_all, perm, sent, land, sten, stage, ctrl, bands, bandf, field, fine, banded, acc, *refs = refs
    parts, sums, total, moved, turned_out, gram, grams, system, answer, answers, *sems = refs
    s_go, s_in, h_go, h_in, c_go, c_in, f_go, f_in, b_go, b_in, p_go, p_in, m_go, m_in, *sems = sems
    g_go, g_in, w_go, w_in = sems

    nk, ndest, own_rows, cols, lev = sent.shape
    coarse = land.shape[2]
    groups = sten.shape[0]
    half = cols // 2
    blocks = nz * nc
    xh, xl, z, c, y = (lax.axis_index(a) for a in ("xh", "xl", "z", "c", "y"))
    shift = nz // 2
    block = (z + nz - shift) % nz * nc + c
    tile = xl * blocks + z * nc + c

    def z_of(b):
        return (b // nc + shift) % nz

    me = (xh * nxl + xl) * blocks + block
    team = (xh * nxl + xl) * ny + y

    def at_dest(d):
        m, b = d // blocks, d % blocks
        return {"xh": m // nxl, "xl": m % nxl, "z": z_of(b), "c": b % nc}

    def at_team(p):
        m = p // ny
        return {"xh": m // nxl, "xl": m % nxl, "y": p % ny}

    barrier = pltpu.get_barrier_semaphore()

    def greet(n, carry):
        pl.semaphore_signal(
            barrier, inc=1, device_id=at_dest((me + n) % ndest), device_id_type=MESH
        )
        return carry

    lax.fori_loop(1, ndest, greet, 0)
    nteam = nxh * nxl * ny

    def greet_team(n, carry):
        p = (team + n) % nteam

        @pl.when(p % ny != y)
        def _():
            pl.semaphore_signal(barrier, inc=1, device_id=at_team(p), device_id_type=MESH)

        return carry

    lax.fori_loop(1, nteam, greet_team, 0)

    flat = own_rows * lev
    perm[...] = one_hot(
        (flat, flat), lambda p: (p % lev) * own_rows + p // lev, lambda q: q
    )

    def spread(k, carry):
        def group_of(m, carry):
            by_row = jnp.dot(
                perm[...], x_ref[m * nk + k], preferred_element_type=F32
            ).astype(BF)
            out = lax.dot_general(
                ci_ref[...], by_row, (((1,), (1,)), ((), ())), preferred_element_type=F32
            ).astype(BF)
            for i in range(own_rows):
                sent[k, pl.ds(m * blocks, blocks), i] = out[:, i * lev : (i + 1) * lev].reshape(
                    blocks, cols, lev
                )
            return carry

        return lax.fori_loop(0, nxh * nxl, group_of, carry)

    def send(k):
        def one(n, carry):
            d = (me + n) % ndest
            pltpu.make_async_remote_copy(
                src_ref=sent.at[k, d],
                dst_ref=land.at[k, xh, pl.ds(tile * own_rows, own_rows)],
                send_sem=s_go.at[k],
                recv_sem=s_in.at[k],
                device_id=at_dest(d),
                device_id_type=MESH,
            ).start()
            return carry

        lax.fori_loop(1, ndest, one, 0)
        land[k, xh, pl.ds(tile * own_rows, own_rows)] = sent[k, me]

    def wait_bytes(ref, sem):
        pltpu.make_async_copy(ref, ref, sem).wait()

    band_ref[...] = jnp.zeros_like(band_ref)
    band_ref[:, : band_in.shape[1]] = band_in[...].astype(F32)
    spread(0, 0)
    pl.semaphore_wait(barrier, ndest - 1 + nteam - nxh * nxl)

    to_xl, to_z, to_c = c, z_of(xl * nz + z), (xl * nz + z) % nc
    home = (to_xl == xl) & (to_z == z) & (to_c == c)
    quarter = pltpu.make_async_remote_copy(
        src_ref=cq_ref,
        dst_ref=stage,
        send_sem=c_go,
        recv_sem=c_in,
        device_id={"xl": to_xl, "z": to_z, "c": to_c},
        device_id_type=MESH,
    )

    @pl.when(jnp.logical_not(home))
    def _():
        quarter.start()

    @pl.when(home)
    def _():
        stage[...] = cq_ref[...]

    for side in range(nxl):
        here = (to_z == z) & (to_c == c) & (xl == side)

        @pl.when(jnp.logical_not(here))
        def _():
            pltpu.make_async_remote_copy(
                src_ref=band_ref,
                dst_ref=bands.at[c],
                send_sem=b_go.at[side],
                recv_sem=b_in.at[c],
                device_id={"xl": side, "z": to_z, "c": to_c},
                device_id_type=MESH,
            ).start()

        @pl.when(here)
        def _():
            bands[c] = band_ref[...]

    send(0)
    spread(1, 0)
    send(1)

    @pl.when(jnp.logical_not(home))
    def _():
        quarter.wait()

    quarter_cols = cq_ref.shape[0]
    slot = xh * cols + xl * half + y * quarter_cols

    def forward(n, carry):
        p = (team + n) % nteam
        pltpu.make_async_remote_copy(
            src_ref=stage,
            dst_ref=ctrl.at[pl.ds(slot, quarter_cols)],
            send_sem=f_go,
            recv_sem=f_in,
            device_id=at_team(p),
            device_id_type=MESH,
        ).start()
        return carry

    lax.fori_loop(1, nteam, forward, 0)
    ctrl[pl.ds(slot, quarter_cols)] = stage[...]

    def rest(k, carry):
        spread(k, 0)
        send(k)
        return carry

    lax.fori_loop(2, nk, rest, 0)

    members, obs = hx_ref.shape
    lanes = gram.shape[2]
    region = xh * ny + y
    nregion = nxh * ny

    def at_region(g):
        return {"xh": g // ny, "y": g % ny}

    weighted = (hx_ref[...].astype(F32) * prec_ref[...]).astype(BF)
    padded = jnp.concatenate([hx_ref[...], jnp.zeros((lanes - members, obs), BF)], axis=0)
    lane = lax.broadcasted_iota(jnp.int32, (members, lanes), 1)
    row_of = lax.broadcasted_iota(jnp.int32, (members, lanes), 0)
    for g in range(nregion):
        inside = region_ref[...] == g
        masked = jnp.where(inside, weighted.astype(F32), 0.0)
        right = jnp.sum(masked * innov_ref[...], axis=1, keepdims=True)
        product = lax.dot_general(
            masked.astype(BF), padded, (((1,), (1,)), ((), ())), preferred_element_type=F32
        )
        gram[g] = jnp.where(lane == members, right, product)

    def hand_gram(n, carry):
        g = (region + n) % nregion
        pltpu.make_async_remote_copy(
            src_ref=gram.at[g],
            dst_ref=grams.at[region],
            send_sem=g_go,
            recv_sem=g_in,
            device_id=at_region(g),
            device_id_type=MESH,
        ).start()
        return carry

    lax.fori_loop(1, nregion, hand_gram, 0)
    grams[region] = gram[region]

    def gather_system():
        wait_bytes(grams.at[pl.ds(0, nregion - 1)], g_in)
        value = grams[0]
        for g in range(1, nregion):
            value = value + grams[g]
        system[...] = value + jnp.where(lane == row_of, members - 1.0, 0.0)

    def eliminate(j, carry):
        value = system[...]
        pivot_row = system[pl.ds(j, 1), :]
        column = jnp.sum(jnp.where(lane == j, value, 0.0), axis=1, keepdims=True)
        pivot = jnp.sum(jnp.where(lane[:1] == j, pivot_row, 0.0), axis=1, keepdims=True)
        scaled = pivot_row / pivot
        system[...] = jnp.where(row_of == j, scaled, value - column * scaled)
        return carry

    def hand_answer():
        solved = jnp.sum(
            jnp.where(lane == members, system[...], 0.0), axis=1, keepdims=True
        )
        across = jnp.sum(jnp.where(lane == row_of, solved, 0.0), axis=0, keepdims=True)
        answer[...] = jnp.broadcast_to(across, answer.shape)

        def one(n, carry):
            pltpu.make_async_remote_copy(
                src_ref=answer,
                dst_ref=answers.at[region],
                send_sem=w_go,
                recv_sem=w_in,
                device_id=at_region((region + n) % nregion),
                device_id_type=MESH,
            ).start()
            return carry

        lax.fori_loop(1, nregion, one, 0)
        answers[region] = answer[...]

    span = WIN * cols
    p_id = lax.broadcasted_iota(jnp.int32, (cols * GR, span), 0)
    q_id = lax.broadcasted_iota(jnp.int32, (cols * GR, span), 1)
    same = q_id % cols == p_id // GR

    rw_all[...] = jnp.zeros_like(rw_all)
    rw_all[:3, :] = rw_ref[...].astype(F32)
    lev_t = lax.dot_general(
        one_hot((lev, lev), lambda p: p, lambda q: q),
        lev_in[...],
        (((1,), (1,)), ((), ())),
        preferred_element_type=F32,
    ).astype(BF)
    lev_ref[...] = jnp.zeros_like(lev_ref)
    lev_ref[:lev, :lev] = lev_t
    lev_ref[lev:, lev:] = lev_t

    def stencil(g, carry):
        take = (
            lax.broadcasted_iota(jnp.int32, (cols * GR, groups * GR), 1)
            == lax.broadcasted_iota(jnp.int32, (cols * GR, groups * GR), 0) % GR + g * GR
        ).astype(BF)
        w = lax.dot_general(
            take, rw_all[...].astype(BF), (((1,), (1,)), ((), ())), preferred_element_type=F32
        )
        start = jnp.minimum(jnp.maximum(g * (GR // 2) - 1, 0), coarse - WIN)
        full = jnp.zeros((cols * GR, span), F32)
        for s in range(3):
            wanted = g * (GR // 2) - start + (p_id % GR) // 2 + s - 1
            full = jnp.where(same & (q_id // cols == wanted), w[:, s : s + 1], full)
        sten[g] = full.astype(BF)
        return carry

    lax.fori_loop(0, groups, stencil, 0)

    for side in range(2):
        here = (xl == block // nz) & (z == block % nz) & (c == side)

        @pl.when(jnp.logical_not(here))
        def _():
            wait_bytes(bands.at[side], b_in.at[side])

    narrow = jnp.concatenate(
        [bands[0], pltpu.roll(bands[1], half, 1)], axis=0
    ).astype(BF)
    wide_src = 4 * half * GR
    take_src = one_hot((narrow.shape[1], wide_src), lambda m: m, lambda q: q // GR)
    take_col = one_hot((cols * GR, cols), lambda p: p // GR, lambda j: j)
    wide = jnp.dot(narrow, take_src, preferred_element_type=F32).astype(BF)
    full = jnp.dot(take_col, wide, preferred_element_type=F32)
    p_id2 = lax.broadcasted_iota(jnp.int32, full.shape, 0)
    q_id2 = lax.broadcasted_iota(jnp.int32, full.shape, 1)
    full = jnp.where(p_id2 % GR == q_id2 % GR, full, 0.0).astype(BF)
    side_rows = half * GR
    for i in range(2):
        bandf[i] = full[i * side_rows : (i + 1) * side_rows, i * side_rows : (i + 3) * side_rows]

    acc[...] = jnp.zeros_like(acc)

    def refine_group(k, group):
        start = window_start(group, coarse)
        windows = [land[k, t, pl.ds(start, WIN)].reshape(WIN * cols, lev) for t in range(2)]
        out = jnp.dot(
            sten[group], jnp.concatenate(windows, axis=1), preferred_element_type=F32
        ).astype(BF)
        return [out[:, t * lev : (t + 1) * lev].reshape(cols, GR, lev) for t in range(2)]

    def project(k):
        for group in range(groups):
            rows = pl.ds(group * GR, GR)
            first, second = refine_group(k, group)
            fine[k, 0, :, rows, :] = first
            fine[k, 1, :, rows, :] = second
            both = first.astype(F32) * ctrl[pl.ds(0, cols), rows, :].astype(F32)
            both = both + second.astype(F32) * ctrl[pl.ds(cols, cols), rows, :].astype(F32)
            both = both.astype(BF)
            field[k, 1, :, rows, :] = both[:half]
            field[k, 2, :, rows, :] = both[half:]

    def halo_copy(k, side):
        other = block + 1 if side == 0 else block - 1
        return pltpu.make_async_remote_copy(
            src_ref=field.at[k, 2 - side],
            dst_ref=field.at[k, 3 * side],
            send_sem=h_go.at[k, side],
            recv_sem=h_in.at[k, side],
            device_id={"z": z_of(other), "c": other % nc},
            device_id_type=MESH,
        )

    nl, ll = ny, lev // ny

    def hand_columns(i, start, count):
        for j in range(start, start + count):
            for t in range(2):
                turned = acc[t, i * half + j].T.astype(BF)
                for q in range(nl):
                    parts[(t * nxl + i) * ny + q, j] = turned[q * ll : (q + 1) * ll]
        for j in range(start, start + count):
            for t in range(2):
                for q in range(nl):
                    p = (t * nxl + i) * ny + q

                    @pl.when(p != team)
                    def _():
                        pltpu.make_async_remote_copy(
                            src_ref=parts.at[p, j],
                            dst_ref=sums.at[team, j],
                            send_sem=p_go,
                            recv_sem=p_in.at[j],
                            device_id=at_team(p),
                            device_id_type=MESH,
                        ).start()

    sends = (block < blocks - 1, block > 0)
    near = 1 - c
    edge = ((c == 0) & (block == 0)) | ((c == nc - 1) & (block == blocks - 1))

    def localize(k, i, side):
        @pl.when((side == near) | jnp.logical_not(edge))
        def _():
            wait_bytes(field.at[k, 3 * side], h_in.at[k, side])

        @pl.when((side != near) & edge)
        def _():
            field[k, 3 * side] = jnp.zeros(field.shape[2:], BF)

        for group in range(0, groups, 2):
            wide = []
            for g in (group, group + 1):
                rows = pl.ds(g * GR, GR)
                pieces = [field[k, i + n, :, rows, :].reshape(half * GR, lev) for n in range(3)]
                wide.append(jnp.concatenate(pieces, axis=0))
            mixed = jnp.dot(
                bandf[i], jnp.concatenate(wide, axis=1), preferred_element_type=F32
            ).astype(BF)
            for n, g in enumerate((group, group + 1)):
                banded[:, pl.ds(g * GR, GR), :] = mixed[:, n * lev : (n + 1) * lev].reshape(
                    half, GR, lev
                )
        for j in range(0, half, 2):
            pair = jnp.concatenate([banded[j], banded[j + 1]], axis=1)
            mixed = jnp.dot(row_ref[...], pair, preferred_element_type=F32).astype(BF)
            local = jnp.dot(mixed, lev_ref[...], preferred_element_type=F32)
            for n in range(2):
                part = local[:, n * lev : (n + 1) * lev]
                at = i * half + j + n
                for t in range(2):
                    acc[t, at] += fine[k, t, at].astype(F32) * part

            @pl.when(k == nk - 1)
            def _():
                hand_columns(i, j, 2)

    def wait_all_but_one(k, sem):
        wait_bytes(sent.at[k, pl.ds(0, ndest - 1)], sem.at[k])

    dest = block * nxl + xl
    d_block = dest % blocks
    stays = dest == tile

    def finish():
        for j in range(half):
            wait_bytes(sums.at[pl.ds(0, nteam - 1), j], p_in.at[j])
            sums[team, j] = parts[team, j]
            value = sums[0, j].astype(F32)
            for p in range(1, nteam):
                value = value + sums[p, j].astype(F32)
            total[j] = (value * scale).astype(BF)

            @pl.when(jnp.logical_not(stays))
            def _():
                pltpu.make_async_remote_copy(
                    src_ref=total.at[j],
                    dst_ref=moved.at[j],
                    send_sem=m_go,
                    recv_sem=m_in,
                    device_id={"xl": dest // blocks, "z": d_block // nc, "c": d_block % nc},
                    device_id_type=MESH,
                ).start()

            @pl.when(stays)
            def _():
                moved[j] = total[j]

    share = -(-members // (nk - 2))

    def step(k, carry):
        @pl.when(k < nk)
        def _():
            wait_all_but_one(k, s_in)

            @pl.when(k == 0)
            def _():
                wait_bytes(ctrl.at[pl.ds(0, (nteam - 1) * quarter_cols)], f_in)

            project(k)
            for side in range(2):

                @pl.when(sends[side])
                def _():
                    halo_copy(k, side).start()

            @pl.when(k == 1)
            def _():
                gather_system()

            @pl.when(k >= 1)
            def _():
                last = jnp.minimum(k * share, members)
                lax.fori_loop(jnp.minimum((k - 1) * share, members), last, eliminate, 0)

            @pl.when(k == nk - 1)
            def _():
                hand_answer()

        first = (k >= 1) & (k <= nk)

        @pl.when(k >= 1)
        def _():
            localize(
                jnp.where(first, k - 1, k - 1 - nk),
                jnp.where(first, near, 1 - near),
                jnp.where(first, near, 1 - near),
            )

        return carry

    lax.fori_loop(0, 2 * nk + 1, step, 0)

    finish()

    def left(k, carry):
        wait_all_but_one(k, s_go)
        for side in range(2):

            @pl.when(sends[side])
            def _():
                wait_bytes(field.at[k, side], h_go.at[k, side])

        return carry

    lax.fori_loop(0, nk, left, 0)
    wait_bytes(ctrl.at[pl.ds(0, (nteam - 1) * quarter_cols)], f_go)
    wait_bytes(sums.at[pl.ds(0, nteam - 1)], p_go)
    wait_bytes(grams.at[pl.ds(0, nregion - 1)], g_go)
    wait_bytes(answers.at[pl.ds(0, nregion - 1)], w_go)
    wait_bytes(answers.at[pl.ds(0, nregion - 1)], w_in)
    for g in range(nregion):
        w_ref[pl.ds(g, 1), :] = answers[g, :1, :members]
    for side in range(nxl):
        here = (to_z == z) & (to_c == c) & (xl == side)

        @pl.when(jnp.logical_not(here))
        def _():
            wait_bytes(bands.at[side], b_go.at[side])

    @pl.when(jnp.logical_not(stays))
    def _():
        wait_bytes(total, m_go)
        wait_bytes(moved, m_in)

    for j in range(half):
        turned_out[:, j, :] = moved[j].astype(F32)
    o_ref[...] = turned_out[...].astype(BF)


def body(
    ens_coarse,
    col_interp,
    row_weights,
    ctrl_vec,
    band_loc,
    row_loc,
    level_loc,
    hx_pert,
    innov,
    obs_prec,
    obs_region,
):
    nxh, nxl, nz, nc, ny = (lax.axis_size(a) for a in ("xh", "xl", "z", "c", "y"))
    _, members, lev, own_rows, coarse_cols = ens_coarse.shape
    fine_cols = col_interp.shape[0]
    fine_rows = row_weights.shape[1]
    blocks = nz * nc
    cols = fine_cols // blocks
    half = cols // 2
    group = members // (nxh * nxl)
    tiles = nxl * blocks
    coarse = tiles * own_rows
    total_members = hx_pert.shape[1]
    nteam = nxh * nxl * ny
    quarter = half // ny
    lanes = 128

    x = ens_coarse.reshape(members, lev * own_rows, coarse_cols)
    mine = lax.dynamic_slice_in_dim(ctrl_vec[0], lax.axis_index("y") * quarter, quarter, 1)
    mine = jnp.transpose(mine.astype(BF), (1, 2, 0))

    vm = pl.BlockSpec(memory_space=pltpu.VMEM)
    dma = pltpu.SemaphoreType.DMA
    increment, weights = pl.pallas_call(
        lambda *refs: main_kernel((nxh, nxl, nz, nc, ny, 1.0 / (total_members - 1)), refs),
        in_specs=[vm] * 11,
        out_specs=(vm, vm),
        out_shape=(
            jax.ShapeDtypeStruct((lev // ny, half, fine_rows), BF),
            jax.ShapeDtypeStruct((NREG, total_members), F32),
        ),
        scratch_shapes=[
            pltpu.VMEM((2 * lev, 2 * lev), BF),
            pltpu.VMEM((half, lanes), F32),
            pltpu.VMEM((8, fine_rows), F32),
            pltpu.VMEM((own_rows * lev, own_rows * lev), BF),
            pltpu.VMEM((group, nxh * tiles, own_rows, cols, lev), BF),
            pltpu.VMEM((group, nxh, coarse, cols, lev), BF),
            pltpu.VMEM((fine_rows // GR, cols * GR, WIN * cols), BF),
            pltpu.VMEM((quarter, fine_rows, lev), BF),
            pltpu.VMEM((nxh * cols, fine_rows, lev), BF),
            pltpu.VMEM((2, half, lanes), F32),
            pltpu.VMEM((2, half * GR, 3 * half * GR), BF),
            pltpu.VMEM((group, 4, half, fine_rows, lev), BF),
            pltpu.VMEM((group, nxh, cols, fine_rows, lev), BF),
            pltpu.VMEM((half, fine_rows, lev), BF),
            pltpu.VMEM((nxh, cols, fine_rows, lev), F32),
            pltpu.VMEM((nteam, half, lev // ny, fine_rows), BF),
            pltpu.VMEM((nteam, half, lev // ny, fine_rows), BF),
            pltpu.VMEM((half, lev // ny, fine_rows), BF),
            pltpu.VMEM((half, lev // ny, fine_rows), BF),
            pltpu.VMEM((lev // ny, half, fine_rows), F32),
            pltpu.VMEM((NREG, total_members, lanes), F32),
            pltpu.VMEM((NREG, total_members, lanes), F32),
            pltpu.VMEM((total_members, lanes), F32),
            pltpu.VMEM((8, lanes), F32),
            pltpu.VMEM((NREG, 8, lanes), F32),
            dma((group,)),
            dma((group,)),
            dma((group, 2)),
            dma((group, 2)),
            *[dma] * 4,
            dma((2,)),
            dma((2,)),
            dma,
            dma((half,)),
            *[dma] * 6,
        ],
        compiler_params=pltpu.CompilerParams(
            collective_id=0, has_side_effects=True, vmem_limit_bytes=62 << 20
        ),
    )(x, col_interp, row_weights, mine, band_loc, row_loc, level_loc, hx_pert[0], innov, obs_prec, obs_region)
    return (increment.astype(F32)[None], weights)


def solution(mesh):
    shape = (2, 2, mesh.shape["tile"] // 4, 2, mesh.shape["mem"])
    fine_mesh = Mesh(mesh.devices.reshape(shape), ("xh", "xl", "z", "c", "y"))
    tile = ("xl", "z", "c")
    obs = (*tile, "y")
    placed = (
        P("xh", "y", None, tile, None),
        P(),
        P(),
        P("xh", None, tile, None),
        P(tile, None),
        P(),
        P(),
        P("xh", None, obs),
        P("xh", obs),
        P("xh", obs),
        P("xh", obs),
    )
    return jax.shard_map(
        body,
        mesh=fine_mesh,
        in_specs=placed,
        out_specs=(P("xh", "y", tile, None), P(tile, None)),
        check_vma=False,
    )
```

```python
import functools

import jax
import jax.numpy as jnp
from jax import lax
from jax.experimental import pallas as pl
from jax.experimental.pallas import tpu as pltpu
from jax.sharding import Mesh, PartitionSpec as P

NREG = 8
BF = jnp.bfloat16
F32 = jnp.float32
GR = 16
WIN = 10


MESH = pl.DeviceIdType.MESH


def one_hot(shape, of_row, of_col):
    row = lax.broadcasted_iota(jnp.int32, shape, 0)
    col = lax.broadcasted_iota(jnp.int32, shape, 1)
    return (of_row(row) == of_col(col)).astype(BF)


def window_start(group, coarse_rows):
    return min(max(group * GR // 2 - 1, 0), coarse_rows - WIN)


def main_kernel(sizes, refs):
    nxh, nxl, nz, nc, ny, scale = sizes
    x_ref, ci_ref, rw_ref, cv_ref, band_in, row_ref, lev_in, *refs = refs
    hx_ref, innov_ref, prec_ref, region_ref, o_ref, w_ref, *refs = refs
    cq_ref, lev_ref, band_ref, rw_all, perm, sent, land, sten, stage, ctrl, bands, bandf, field, fine, banded, acc, *refs = refs
    parts, sums, total, moved, turned_out, gram, grams, system, answer, answers, *sems = refs
    s_go, s_in, h_go, h_in, c_go, c_in, f_go, f_in, b_go, b_in, p_go, p_in, m_go, m_in, *sems = sems
    g_go, g_in, w_go, w_in = sems

    nk, ndest, own_rows, cols, lev = sent.shape
    coarse = land.shape[2]
    groups = sten.shape[0]
    half = cols // 2
    blocks = nz * nc
    xh, xl, z, c, y = (lax.axis_index(a) for a in ("xh", "xl", "z", "c", "y"))
    shift = nz // 2
    block = (z + nz - shift) % nz * nc + c
    tile = xl * blocks + z * nc + c

    def z_of(b):
        return (b // nc + shift) % nz

    me = (xh * nxl + xl) * blocks + block
    team = (xh * nxl + xl) * ny + y

    def at_dest(d):
        m, b = d // blocks, d % blocks
        return {"xh": m // nxl, "xl": m % nxl, "z": z_of(b), "c": b % nc}

    def at_team(p):
        m = p // ny
        return {"xh": m // nxl, "xl": m % nxl, "y": p % ny}

    barrier = pltpu.get_barrier_semaphore()

    def greet(n, carry):
        pl.semaphore_signal(
            barrier, inc=1, device_id=at_dest((me + n) % ndest), device_id_type=MESH
        )
        return carry

    lax.fori_loop(1, ndest, greet, 0)
    nteam = nxh * nxl * ny

    def greet_team(n, carry):
        p = (team + n) % nteam

        @pl.when(p % ny != y)
        def _():
            pl.semaphore_signal(barrier, inc=1, device_id=at_team(p), device_id_type=MESH)

        return carry

    lax.fori_loop(1, nteam, greet_team, 0)

    flat = own_rows * lev
    perm[...] = one_hot(
        (flat, flat), lambda p: (p % lev) * own_rows + p // lev, lambda q: q
    )

    def spread(k, carry):
        def group_of(m, carry):
            by_row = jnp.dot(
                perm[...], x_ref[m * nk + k], preferred_element_type=F32
            ).astype(BF)
            out = lax.dot_general(
                ci_ref[...], by_row, (((1,), (1,)), ((), ())), preferred_element_type=F32
            ).astype(BF)
            for i in range(own_rows):
                sent[k, pl.ds(m * blocks, blocks), i] = out[:, i * lev : (i + 1) * lev].reshape(
                    blocks, cols, lev
                )
            return carry

        return lax.fori_loop(0, nxh * nxl, group_of, carry)

    def send(k):
        def one(n, carry):
            d = (me + n) % ndest
            pltpu.make_async_remote_copy(
                src_ref=sent.at[k, d],
                dst_ref=land.at[k, xh, pl.ds(tile * own_rows, own_rows)],
                send_sem=s_go.at[k],
                recv_sem=s_in.at[k],
                device_id=at_dest(d),
                device_id_type=MESH,
            ).start()
            return carry

        lax.fori_loop(1, ndest, one, 0)
        land[k, xh, pl.ds(tile * own_rows, own_rows)] = sent[k, me]

    def wait_bytes(ref, sem):
        pltpu.make_async_copy(ref, ref, sem).wait()

    for n in range(cq_ref.shape[0]):
        cq_ref[n] = cv_ref[:, y * cq_ref.shape[0] + n, :].T.astype(BF)
    band_ref[...] = jnp.zeros_like(band_ref)
    band_ref[:, : band_in.shape[1]] = band_in[...].astype(F32)
    spread(0, 0)
    pl.semaphore_wait(barrier, ndest - 1 + nteam - nxh * nxl)

    to_xl, to_z, to_c = c, z_of(xl * nz + z), (xl * nz + z) % nc
    home = (to_xl == xl) & (to_z == z) & (to_c == c)
    quarter = pltpu.make_async_remote_copy(
        src_ref=cq_ref,
        dst_ref=stage,
        send_sem=c_go,
        recv_sem=c_in,
        device_id={"xl": to_xl, "z": to_z, "c": to_c},
        device_id_type=MESH,
    )

    @pl.when(jnp.logical_not(home))
    def _():
        quarter.start()

    @pl.when(home)
    def _():
        stage[...] = cq_ref[...]

    for side in range(nxl):
        here = (to_z == z) & (to_c == c) & (xl == side)

        @pl.when(jnp.logical_not(here))
        def _():
            pltpu.make_async_remote_copy(
                src_ref=band_ref,
                dst_ref=bands.at[c],
                send_sem=b_go.at[side],
                recv_sem=b_in.at[c],
                device_id={"xl": side, "z": to_z, "c": to_c},
                device_id_type=MESH,
            ).start()

        @pl.when(here)
        def _():
            bands[c] = band_ref[...]

    send(0)
    spread(1, 0)
    send(1)

    @pl.when(jnp.logical_not(home))
    def _():
        quarter.wait()

    quarter_cols = cq_ref.shape[0]
    slot = xh * cols + xl * half + y * quarter_cols

    def forward(n, carry):
        p = (team + n) % nteam
        pltpu.make_async_remote_copy(
            src_ref=stage,
            dst_ref=ctrl.at[pl.ds(slot, quarter_cols)],
            send_sem=f_go,
            recv_sem=f_in,
            device_id=at_team(p),
            device_id_type=MESH,
        ).start()
        return carry

    lax.fori_loop(1, nteam, forward, 0)
    ctrl[pl.ds(slot, quarter_cols)] = stage[...]

    def rest(k, carry):
        spread(k, 0)
        send(k)
        return carry

    lax.fori_loop(2, nk, rest, 0)

    members, obs = hx_ref.shape
    lanes = gram.shape[2]
    region = xh * ny + y
    nregion = nxh * ny

    def at_region(g):
        return {"xh": g // ny, "y": g % ny}

    weighted = (hx_ref[...].astype(F32) * prec_ref[...]).astype(BF)
    padded = jnp.concatenate([hx_ref[...], jnp.zeros((lanes - members, obs), BF)], axis=0)
    lane = lax.broadcasted_iota(jnp.int32, (members, lanes), 1)
    row_of = lax.broadcasted_iota(jnp.int32, (members, lanes), 0)
    for g in range(nregion):
        inside = region_ref[...] == g
        masked = jnp.where(inside, weighted.astype(F32), 0.0)
        right = jnp.sum(masked * innov_ref[...], axis=1, keepdims=True)
        product = lax.dot_general(
            masked.astype(BF), padded, (((1,), (1,)), ((), ())), preferred_element_type=F32
        )
        gram[g] = jnp.where(lane == members, right, product)

    def hand_gram(n, carry):
        g = (region + n) % nregion
        pltpu.make_async_remote_copy(
            src_ref=gram.at[g],
            dst_ref=grams.at[region],
            send_sem=g_go,
            recv_sem=g_in,
            device_id=at_region(g),
            device_id_type=MESH,
        ).start()
        return carry

    lax.fori_loop(1, nregion, hand_gram, 0)
    grams[region] = gram[region]

    def gather_system():
        wait_bytes(grams.at[pl.ds(0, nregion - 1)], g_in)
        value = grams[0]
        for g in range(1, nregion):
            value = value + grams[g]
        system[...] = value + jnp.where(lane == row_of, members - 1.0, 0.0)

    def eliminate(j, carry):
        value = system[...]
        pivot_row = system[pl.ds(j, 1), :]
        column = jnp.sum(jnp.where(lane == j, value, 0.0), axis=1, keepdims=True)
        pivot = jnp.sum(jnp.where(lane[:1] == j, pivot_row, 0.0), axis=1, keepdims=True)
        scaled = pivot_row / pivot
        system[...] = jnp.where(row_of == j, scaled, value - column * scaled)
        return carry

    def hand_answer():
        solved = jnp.sum(
            jnp.where(lane == members, system[...], 0.0), axis=1, keepdims=True
        )
        across = jnp.sum(jnp.where(lane == row_of, solved, 0.0), axis=0, keepdims=True)
        answer[...] = jnp.broadcast_to(across, answer.shape)

        def one(n, carry):
            pltpu.make_async_remote_copy(
                src_ref=answer,
                dst_ref=answers.at[region],
                send_sem=w_go,
                recv_sem=w_in,
                device_id=at_region((region + n) % nregion),
                device_id_type=MESH,
            ).start()
            return carry

        lax.fori_loop(1, nregion, one, 0)
        answers[region] = answer[...]

    span = WIN * cols
    p_id = lax.broadcasted_iota(jnp.int32, (cols * GR, span), 0)
    q_id = lax.broadcasted_iota(jnp.int32, (cols * GR, span), 1)
    same = q_id % cols == p_id // GR

    rw_all[...] = jnp.zeros_like(rw_all)
    rw_all[:3, :] = rw_ref[...].astype(F32)
    lev_t = lax.dot_general(
        one_hot((lev, lev), lambda p: p, lambda q: q),
        lev_in[...],
        (((1,), (1,)), ((), ())),
        preferred_element_type=F32,
    ).astype(BF)
    lev_ref[...] = jnp.zeros_like(lev_ref)
    lev_ref[:lev, :lev] = lev_t
    lev_ref[lev:, lev:] = lev_t

    def stencil(g, carry):
        take = (
            lax.broadcasted_iota(jnp.int32, (cols * GR, groups * GR), 1)
            == lax.broadcasted_iota(jnp.int32, (cols * GR, groups * GR), 0) % GR + g * GR
        ).astype(BF)
        w = lax.dot_general(
            take, rw_all[...].astype(BF), (((1,), (1,)), ((), ())), preferred_element_type=F32
        )
        start = jnp.minimum(jnp.maximum(g * (GR // 2) - 1, 0), coarse - WIN)
        full = jnp.zeros((cols * GR, span), F32)
        for s in range(3):
            wanted = g * (GR // 2) - start + (p_id % GR) // 2 + s - 1
            full = jnp.where(same & (q_id // cols == wanted), w[:, s : s + 1], full)
        sten[g] = full.astype(BF)
        return carry

    lax.fori_loop(0, groups, stencil, 0)

    for side in range(2):
        here = (xl == block // nz) & (z == block % nz) & (c == side)

        @pl.when(jnp.logical_not(here))
        def _():
            wait_bytes(bands.at[side], b_in.at[side])

    narrow = jnp.concatenate(
        [bands[0], pltpu.roll(bands[1], half, 1)], axis=0
    ).astype(BF)
    wide_src = 4 * half * GR
    take_src = one_hot((narrow.shape[1], wide_src), lambda m: m, lambda q: q // GR)
    take_col = one_hot((cols * GR, cols), lambda p: p // GR, lambda j: j)
    wide = jnp.dot(narrow, take_src, preferred_element_type=F32).astype(BF)
    full = jnp.dot(take_col, wide, preferred_element_type=F32)
    p_id2 = lax.broadcasted_iota(jnp.int32, full.shape, 0)
    q_id2 = lax.broadcasted_iota(jnp.int32, full.shape, 1)
    full = jnp.where(p_id2 % GR == q_id2 % GR, full, 0.0).astype(BF)
    side_rows = half * GR
    for i in range(2):
        bandf[i] = full[i * side_rows : (i + 1) * side_rows, i * side_rows : (i + 3) * side_rows]

    acc[...] = jnp.zeros_like(acc)

    def refine_group(k, group):
        start = window_start(group, coarse)
        windows = [land[k, t, pl.ds(start, WIN)].reshape(WIN * cols, lev) for t in range(2)]
        out = jnp.dot(
            sten[group], jnp.concatenate(windows, axis=1), preferred_element_type=F32
        ).astype(BF)
        return [out[:, t * lev : (t + 1) * lev].reshape(cols, GR, lev) for t in range(2)]

    def project(k):
        for group in range(groups):
            rows = pl.ds(group * GR, GR)
            first, second = refine_group(k, group)
            fine[k, 0, :, rows, :] = first
            fine[k, 1, :, rows, :] = second
            both = first.astype(F32) * ctrl[pl.ds(0, cols), rows, :].astype(F32)
            both = both + second.astype(F32) * ctrl[pl.ds(cols, cols), rows, :].astype(F32)
            both = both.astype(BF)
            field[k, 1, :, rows, :] = both[:half]
            field[k, 2, :, rows, :] = both[half:]

    def halo_copy(k, side):
        other = block + 1 if side == 0 else block - 1
        return pltpu.make_async_remote_copy(
            src_ref=field.at[k, 2 - side],
            dst_ref=field.at[k, 3 * side],
            send_sem=h_go.at[k, side],
            recv_sem=h_in.at[k, side],
            device_id={"z": z_of(other), "c": other % nc},
            device_id_type=MESH,
        )

    nl, ll = ny, lev // ny

    def hand_columns(i, start, count):
        for j in range(start, start + count):
            for t in range(2):
                turned = acc[t, i * half + j].T.astype(BF)
                for q in range(nl):
                    parts[(t * nxl + i) * ny + q, j] = turned[q * ll : (q + 1) * ll]
        for j in range(start, start + count):
            for t in range(2):
                for q in range(nl):
                    p = (t * nxl + i) * ny + q

                    @pl.when(p != team)
                    def _():
                        pltpu.make_async_remote_copy(
                            src_ref=parts.at[p, j],
                            dst_ref=sums.at[team, j],
                            send_sem=p_go,
                            recv_sem=p_in.at[j],
                            device_id=at_team(p),
                            device_id_type=MESH,
                        ).start()

    sends = (block < blocks - 1, block > 0)
    near = 1 - c
    edge = ((c == 0) & (block == 0)) | ((c == nc - 1) & (block == blocks - 1))

    def localize(k, i, side):
        @pl.when((side == near) | jnp.logical_not(edge))
        def _():
            wait_bytes(field.at[k, 3 * side], h_in.at[k, side])

        @pl.when((side != near) & edge)
        def _():
            field[k, 3 * side] = jnp.zeros(field.shape[2:], BF)

        for group in range(0, groups, 2):
            wide = []
            for g in (group, group + 1):
                rows = pl.ds(g * GR, GR)
                pieces = [field[k, i + n, :, rows, :].reshape(half * GR, lev) for n in range(3)]
                wide.append(jnp.concatenate(pieces, axis=0))
            mixed = jnp.dot(
                bandf[i], jnp.concatenate(wide, axis=1), preferred_element_type=F32
            ).astype(BF)
            for n, g in enumerate((group, group + 1)):
                banded[:, pl.ds(g * GR, GR), :] = mixed[:, n * lev : (n + 1) * lev].reshape(
                    half, GR, lev
                )
        for j in range(0, half, 2):
            pair = jnp.concatenate([banded[j], banded[j + 1]], axis=1)
            mixed = jnp.dot(row_ref[...], pair, preferred_element_type=F32).astype(BF)
            local = jnp.dot(mixed, lev_ref[...], preferred_element_type=F32)
            for n in range(2):
                part = local[:, n * lev : (n + 1) * lev]
                at = i * half + j + n
                for t in range(2):
                    acc[t, at] += fine[k, t, at].astype(F32) * part

            @pl.when(k == nk - 1)
            def _():
                hand_columns(i, j, 2)

    def wait_all_but_one(k, sem):
        wait_bytes(sent.at[k, pl.ds(0, ndest - 1)], sem.at[k])

    dest = block * nxl + xl
    d_block = dest % blocks
    stays = dest == tile

    def finish():
        for j in range(half):
            wait_bytes(sums.at[pl.ds(0, nteam - 1), j], p_in.at[j])
            sums[team, j] = parts[team, j]
            value = sums[0, j].astype(F32)
            for p in range(1, nteam):
                value = value + sums[p, j].astype(F32)
            total[j] = (value * scale).astype(BF)

            @pl.when(jnp.logical_not(stays))
            def _():
                pltpu.make_async_remote_copy(
                    src_ref=total.at[j],
                    dst_ref=moved.at[j],
                    send_sem=m_go,
                    recv_sem=m_in,
                    device_id={"xl": dest // blocks, "z": d_block // nc, "c": d_block % nc},
                    device_id_type=MESH,
                ).start()

            @pl.when(stays)
            def _():
                moved[j] = total[j]

    share = -(-members // (nk - 2))

    def step(n, carry):
        k = jnp.minimum(n, nk - 1)

        @pl.when((n <= nk - 2) | (n == nk + 2))
        def _():
            wait_all_but_one(k, s_in)

            @pl.when(k == 0)
            def _():
                wait_bytes(ctrl.at[pl.ds(0, (nteam - 1) * quarter_cols)], f_in)

            project(k)
            for side in range(2):

                @pl.when(sends[side])
                def _():
                    halo_copy(k, side).start()

        @pl.when(n == 1)
        def _():
            gather_system()

        @pl.when((n >= 1) & (n <= nk - 2))
        def _():
            last = jnp.minimum(n * share, members)
            lax.fori_loop(jnp.minimum((n - 1) * share, members), last, eliminate, 0)

        @pl.when(n == nk - 1)
        def _():
            hand_answer()

        inner = (n <= nk - 1) | (n == nk + 2)
        member = jnp.where(
            inner,
            jnp.where(n <= nk - 1, n - 1, nk - 1),
            jnp.where(n <= nk + 1, n - nk, n - nk - 1),
        )
        which = jnp.where(inner, near, 1 - near)

        @pl.when(n >= 1)
        def _():
            localize(member, which, which)

        return carry

    lax.fori_loop(0, 2 * nk + 1, step, 0)

    finish()

    def left(k, carry):
        wait_all_but_one(k, s_go)
        for side in range(2):

            @pl.when(sends[side])
            def _():
                wait_bytes(field.at[k, side], h_go.at[k, side])

        return carry

    lax.fori_loop(0, nk, left, 0)
    wait_bytes(ctrl.at[pl.ds(0, (nteam - 1) * quarter_cols)], f_go)
    wait_bytes(sums.at[pl.ds(0, nteam - 1)], p_go)
    wait_bytes(grams.at[pl.ds(0, nregion - 1)], g_go)
    wait_bytes(answers.at[pl.ds(0, nregion - 1)], w_go)
    wait_bytes(answers.at[pl.ds(0, nregion - 1)], w_in)
    for g in range(nregion):
        w_ref[pl.ds(g, 1), :] = answers[g, :1, :members]
    for side in range(nxl):
        here = (to_z == z) & (to_c == c) & (xl == side)

        @pl.when(jnp.logical_not(here))
        def _():
            wait_bytes(bands.at[side], b_go.at[side])

    @pl.when(jnp.logical_not(stays))
    def _():
        wait_bytes(total, m_go)
        wait_bytes(moved, m_in)

    for j in range(half):
        turned_out[:, j, :] = moved[j].astype(F32)
    o_ref[...] = turned_out[...].astype(BF)


def body(
    ens_coarse,
    col_interp,
    row_weights,
    ctrl_vec,
    band_loc,
    row_loc,
    level_loc,
    hx_pert,
    innov,
    obs_prec,
    obs_region,
):
    nxh, nxl, nz, nc, ny = (lax.axis_size(a) for a in ("xh", "xl", "z", "c", "y"))
    _, members, lev, own_rows, coarse_cols = ens_coarse.shape
    fine_cols = col_interp.shape[0]
    fine_rows = row_weights.shape[1]
    blocks = nz * nc
    cols = fine_cols // blocks
    half = cols // 2
    group = members // (nxh * nxl)
    tiles = nxl * blocks
    coarse = tiles * own_rows
    total_members = hx_pert.shape[1]
    nteam = nxh * nxl * ny
    quarter = half // ny
    lanes = 128

    x = ens_coarse.reshape(members, lev * own_rows, coarse_cols)

    vm = pl.BlockSpec(memory_space=pltpu.VMEM)
    dma = pltpu.SemaphoreType.DMA
    increment, weights = pl.pallas_call(
        lambda *refs: main_kernel((nxh, nxl, nz, nc, ny, 1.0 / (total_members - 1)), refs),
        in_specs=[vm] * 11,
        out_specs=(vm, vm),
        out_shape=(
            jax.ShapeDtypeStruct((lev // ny, half, fine_rows), BF),
            jax.ShapeDtypeStruct((NREG, total_members), F32),
        ),
        scratch_shapes=[
            pltpu.VMEM((quarter, fine_rows, lev), BF),
            pltpu.VMEM((2 * lev, 2 * lev), BF),
            pltpu.VMEM((half, lanes), F32),
            pltpu.VMEM((8, fine_rows), F32),
            pltpu.VMEM((own_rows * lev, own_rows * lev), BF),
            pltpu.VMEM((group, nxh * tiles, own_rows, cols, lev), BF),
            pltpu.VMEM((group, nxh, coarse, cols, lev), BF),
            pltpu.VMEM((fine_rows // GR, cols * GR, WIN * cols), BF),
            pltpu.VMEM((quarter, fine_rows, lev), BF),
            pltpu.VMEM((nxh * cols, fine_rows, lev), BF),
            pltpu.VMEM((2, half, lanes), F32),
            pltpu.VMEM((2, half * GR, 3 * half * GR), BF),
            pltpu.VMEM((group, 4, half, fine_rows, lev), BF),
            pltpu.VMEM((group, nxh, cols, fine_rows, lev), BF),
            pltpu.VMEM((half, fine_rows, lev), BF),
            pltpu.VMEM((nxh, cols, fine_rows, lev), F32),
            pltpu.VMEM((nteam, half, lev // ny, fine_rows), BF),
            pltpu.VMEM((nteam, half, lev // ny, fine_rows), BF),
            pltpu.VMEM((half, lev // ny, fine_rows), BF),
            pltpu.VMEM((half, lev // ny, fine_rows), BF),
            pltpu.VMEM((lev // ny, half, fine_rows), F32),
            pltpu.VMEM((NREG, total_members, lanes), F32),
            pltpu.VMEM((NREG, total_members, lanes), F32),
            pltpu.VMEM((total_members, lanes), F32),
            pltpu.VMEM((8, lanes), F32),
            pltpu.VMEM((NREG, 8, lanes), F32),
            dma((group,)),
            dma((group,)),
            dma((group, 2)),
            dma((group, 2)),
            *[dma] * 4,
            dma((2,)),
            dma((2,)),
            dma,
            dma((half,)),
            *[dma] * 6,
        ],
        compiler_params=pltpu.CompilerParams(
            collective_id=0, has_side_effects=True, vmem_limit_bytes=62 << 20
        ),
    )(x, col_interp, row_weights, ctrl_vec[0], band_loc, row_loc, level_loc, hx_pert[0], innov, obs_prec, obs_region)
    return (increment.astype(F32)[None], weights)


def solution(mesh):
    shape = (2, 2, mesh.shape["tile"] // 4, 2, mesh.shape["mem"])
    fine_mesh = Mesh(mesh.devices.reshape(shape), ("xh", "xl", "z", "c", "y"))
    tile = ("xl", "z", "c")
    obs = (*tile, "y")
    placed = (
        P("xh", "y", None, tile, None),
        P(),
        P(),
        P("xh", None, tile, None),
        P(tile, None),
        P(),
        P(),
        P("xh", None, obs),
        P("xh", obs),
        P("xh", obs),
        P("xh", obs),
    )
    return jax.shard_map(
        body,
        mesh=fine_mesh,
        in_specs=placed,
        out_specs=(P("xh", "y", tile, None), P(tile, None)),
        check_vma=False,
    )
```

```python
import functools

import jax
import jax.numpy as jnp
from jax import lax
from jax.experimental import pallas as pl
from jax.experimental.pallas import tpu as pltpu
from jax.sharding import Mesh, PartitionSpec as P

NREG = 8
BF = jnp.bfloat16
F32 = jnp.float32
GR = 16
WIN = 10


MESH = pl.DeviceIdType.MESH


def one_hot(shape, of_row, of_col):
    row = lax.broadcasted_iota(jnp.int32, shape, 0)
    col = lax.broadcasted_iota(jnp.int32, shape, 1)
    return (of_row(row) == of_col(col)).astype(BF)


def window_start(group, coarse_rows):
    return min(max(group * GR // 2 - 1, 0), coarse_rows - WIN)


def main_kernel(sizes, refs):
    nxh, nxl, nz, nc, ny, scale = sizes
    x_ref, ci_ref, rw_ref, cv_ref, band_in, row_ref, lev_in, *refs = refs
    hx_ref, innov_ref, prec_ref, region_ref, o_ref, w_ref, *refs = refs
    cq_ref, lev_ref, band_ref, rw_all, perm, sent, land, sten, stage, ctrl, bands, bandf, field, fine, banded, acc, *refs = refs
    parts, sums, total, moved, turned_out, gram, grams, system, answer, answers, *sems = refs
    s_go, s_in, h_go, h_in, c_go, c_in, f_go, f_in, b_go, b_in, p_go, p_in, m_go, m_in, *sems = sems
    g_go, g_in, w_go, w_in = sems

    nk, ndest, own_rows, cols, lev = sent.shape
    coarse = land.shape[2]
    groups = sten.shape[0]
    half = cols // 2
    blocks = nz * nc
    xh, xl, z, c, y = (lax.axis_index(a) for a in ("xh", "xl", "z", "c", "y"))
    shift = nz // 2
    block = (z + nz - shift) % nz * nc + c
    tile = xl * blocks + z * nc + c

    def z_of(b):
        return (b // nc + shift) % nz

    me = (xh * nxl + xl) * blocks + block
    team = (xh * nxl + xl) * ny + y

    def at_dest(d):
        m, b = d // blocks, d % blocks
        return {"xh": m // nxl, "xl": m % nxl, "z": z_of(b), "c": b % nc}

    def at_team(p):
        m = p // ny
        return {"xh": m // nxl, "xl": m % nxl, "y": p % ny}

    barrier = pltpu.get_barrier_semaphore()

    def greet(n, carry):
        pl.semaphore_signal(
            barrier, inc=1, device_id=at_dest((me + n) % ndest), device_id_type=MESH
        )
        return carry

    lax.fori_loop(1, ndest, greet, 0)
    nteam = nxh * nxl * ny

    def greet_team(n, carry):
        p = (team + n) % nteam

        @pl.when(p % ny != y)
        def _():
            pl.semaphore_signal(barrier, inc=1, device_id=at_team(p), device_id_type=MESH)

        return carry

    lax.fori_loop(1, nteam, greet_team, 0)

    flat = own_rows * lev
    perm[...] = one_hot(
        (flat, flat), lambda p: (p % lev) * own_rows + p // lev, lambda q: q
    )

    def spread(k, carry):
        def group_of(m, carry):
            by_row = jnp.dot(
                perm[...], x_ref[m * nk + k], preferred_element_type=F32
            ).astype(BF)
            out = lax.dot_general(
                ci_ref[...], by_row, (((1,), (1,)), ((), ())), preferred_element_type=F32
            ).astype(BF)
            for i in range(own_rows):
                sent[k, pl.ds(m * blocks, blocks), i] = out[:, i * lev : (i + 1) * lev].reshape(
                    blocks, cols, lev
                )
            return carry

        return lax.fori_loop(0, nxh * nxl, group_of, carry)

    def send(k):
        def one(n, carry):
            d = (me + n) % ndest
            pltpu.make_async_remote_copy(
                src_ref=sent.at[k, d],
                dst_ref=land.at[k, xh, pl.ds(tile * own_rows, own_rows)],
                send_sem=s_go.at[k],
                recv_sem=s_in.at[k],
                device_id=at_dest(d),
                device_id_type=MESH,
            ).start()
            return carry

        lax.fori_loop(1, ndest, one, 0)
        land[k, xh, pl.ds(tile * own_rows, own_rows)] = sent[k, me]

    def wait_bytes(ref, sem):
        pltpu.make_async_copy(ref, ref, sem).wait()

    for n in range(cq_ref.shape[0]):
        cq_ref[n] = cv_ref[:, y * cq_ref.shape[0] + n, :].T.astype(BF)
    band_ref[...] = jnp.zeros_like(band_ref)
    band_ref[:, : band_in.shape[1]] = band_in[...].astype(F32)
    spread(0, 0)
    pl.semaphore_wait(barrier, ndest - 1 + nteam - nxh * nxl)

    to_xl, to_z, to_c = c, z_of(xl * nz + z), (xl * nz + z) % nc
    home = (to_xl == xl) & (to_z == z) & (to_c == c)
    quarter = pltpu.make_async_remote_copy(
        src_ref=cq_ref,
        dst_ref=stage,
        send_sem=c_go,
        recv_sem=c_in,
        device_id={"xl": to_xl, "z": to_z, "c": to_c},
        device_id_type=MESH,
    )

    @pl.when(jnp.logical_not(home))
    def _():
        quarter.start()

    @pl.when(home)
    def _():
        stage[...] = cq_ref[...]

    for side in range(nxl):
        here = (to_z == z) & (to_c == c) & (xl == side)

        @pl.when(jnp.logical_not(here))
        def _():
            pltpu.make_async_remote_copy(
                src_ref=band_ref,
                dst_ref=bands.at[c],
                send_sem=b_go.at[side],
                recv_sem=b_in.at[c],
                device_id={"xl": side, "z": to_z, "c": to_c},
                device_id_type=MESH,
            ).start()

        @pl.when(here)
        def _():
            bands[c] = band_ref[...]

    send(0)
    spread(1, 0)
    send(1)

    @pl.when(jnp.logical_not(home))
    def _():
        quarter.wait()

    quarter_cols = cq_ref.shape[0]
    slot = xh * cols + xl * half + y * quarter_cols

    def forward(n, carry):
        p = (team + n) % nteam
        pltpu.make_async_remote_copy(
            src_ref=stage,
            dst_ref=ctrl.at[pl.ds(slot, quarter_cols)],
            send_sem=f_go,
            recv_sem=f_in,
            device_id=at_team(p),
            device_id_type=MESH,
        ).start()
        return carry

    lax.fori_loop(1, nteam, forward, 0)
    ctrl[pl.ds(slot, quarter_cols)] = stage[...]

    def rest(k, carry):
        spread(k, 0)
        send(k)
        return carry

    lax.fori_loop(2, nk, rest, 0)

    members, obs = hx_ref.shape
    lanes = gram.shape[2]
    region = xh * ny + y
    nregion = nxh * ny

    def at_region(g):
        return {"xh": g // ny, "y": g % ny}

    weighted = (hx_ref[...].astype(F32) * prec_ref[...]).astype(BF)
    padded = jnp.concatenate([hx_ref[...], jnp.zeros((lanes - members, obs), BF)], axis=0)
    lane = lax.broadcasted_iota(jnp.int32, (members, lanes), 1)
    row_of = lax.broadcasted_iota(jnp.int32, (members, lanes), 0)
    for g in range(nregion):
        inside = region_ref[...] == g
        masked = jnp.where(inside, weighted.astype(F32), 0.0)
        right = jnp.sum(masked * innov_ref[...], axis=1, keepdims=True)
        product = lax.dot_general(
            masked.astype(BF), padded, (((1,), (1,)), ((), ())), preferred_element_type=F32
        )
        gram[g] = jnp.where(lane == members, right, product)

    def hand_gram(n, carry):
        g = (region + n) % nregion
        pltpu.make_async_remote_copy(
            src_ref=gram.at[g],
            dst_ref=grams.at[region],
            send_sem=g_go,
            recv_sem=g_in,
            device_id=at_region(g),
            device_id_type=MESH,
        ).start()
        return carry

    lax.fori_loop(1, nregion, hand_gram, 0)
    grams[region] = gram[region]

    def gather_system():
        wait_bytes(grams.at[pl.ds(0, nregion - 1)], g_in)
        value = grams[0]
        for g in range(1, nregion):
            value = value + grams[g]
        system[...] = value + jnp.where(lane == row_of, members - 1.0, 0.0)

    def eliminate(j, carry):
        value = system[...]
        pivot_row = system[pl.ds(j, 1), :]
        column = jnp.sum(jnp.where(lane == j, value, 0.0), axis=1, keepdims=True)
        pivot = jnp.sum(jnp.where(lane[:1] == j, pivot_row, 0.0), axis=1, keepdims=True)
        scaled = pivot_row / pivot
        system[...] = jnp.where(row_of == j, scaled, value - column * scaled)
        return carry

    def hand_answer():
        solved = jnp.sum(
            jnp.where(lane == members, system[...], 0.0), axis=1, keepdims=True
        )
        across = jnp.sum(jnp.where(lane == row_of, solved, 0.0), axis=0, keepdims=True)
        answer[...] = jnp.broadcast_to(across, answer.shape)

        def one(n, carry):
            pltpu.make_async_remote_copy(
                src_ref=answer,
                dst_ref=answers.at[region],
                send_sem=w_go,
                recv_sem=w_in,
                device_id=at_region((region + n) % nregion),
                device_id_type=MESH,
            ).start()
            return carry

        lax.fori_loop(1, nregion, one, 0)
        answers[region] = answer[...]

    span = WIN * cols
    p_id = lax.broadcasted_iota(jnp.int32, (cols * GR, span), 0)
    q_id = lax.broadcasted_iota(jnp.int32, (cols * GR, span), 1)
    same = q_id % cols == p_id // GR

    rw_all[...] = jnp.zeros_like(rw_all)
    rw_all[:3, :] = rw_ref[...].astype(F32)
    lev_t = lax.dot_general(
        one_hot((lev, lev), lambda p: p, lambda q: q),
        lev_in[...],
        (((1,), (1,)), ((), ())),
        preferred_element_type=F32,
    ).astype(BF)
    lev_ref[...] = jnp.zeros_like(lev_ref)
    lev_ref[:lev, :lev] = lev_t
    lev_ref[lev:, lev:] = lev_t

    def stencil(g, carry):
        take = (
            lax.broadcasted_iota(jnp.int32, (cols * GR, groups * GR), 1)
            == lax.broadcasted_iota(jnp.int32, (cols * GR, groups * GR), 0) % GR + g * GR
        ).astype(BF)
        w = lax.dot_general(
            take, rw_all[...].astype(BF), (((1,), (1,)), ((), ())), preferred_element_type=F32
        )
        start = jnp.minimum(jnp.maximum(g * (GR // 2) - 1, 0), coarse - WIN)
        full = jnp.zeros((cols * GR, span), F32)
        for s in range(3):
            wanted = g * (GR // 2) - start + (p_id % GR) // 2 + s - 1
            full = jnp.where(same & (q_id // cols == wanted), w[:, s : s + 1], full)
        sten[g] = full.astype(BF)
        return carry

    lax.fori_loop(0, groups, stencil, 0)

    for side in range(2):
        here = (xl == block // nz) & (z == block % nz) & (c == side)

        @pl.when(jnp.logical_not(here))
        def _():
            wait_bytes(bands.at[side], b_in.at[side])

    narrow = jnp.concatenate(
        [bands[0], pltpu.roll(bands[1], half, 1)], axis=0
    ).astype(BF)
    wide_src = 4 * half * GR
    take_src = one_hot((narrow.shape[1], wide_src), lambda m: m, lambda q: q // GR)
    take_col = one_hot((cols * GR, cols), lambda p: p // GR, lambda j: j)
    wide = jnp.dot(narrow, take_src, preferred_element_type=F32).astype(BF)
    full = jnp.dot(take_col, wide, preferred_element_type=F32)
    p_id2 = lax.broadcasted_iota(jnp.int32, full.shape, 0)
    q_id2 = lax.broadcasted_iota(jnp.int32, full.shape, 1)
    full = jnp.where(p_id2 % GR == q_id2 % GR, full, 0.0).astype(BF)
    side_rows = half * GR
    for i in range(2):
        bandf[i] = full[i * side_rows : (i + 1) * side_rows, i * side_rows : (i + 3) * side_rows]

    acc[...] = jnp.zeros_like(acc)

    def refine_group(k, group):
        start = window_start(group, coarse)
        windows = [land[k, t, pl.ds(start, WIN)].reshape(WIN * cols, lev) for t in range(2)]
        out = jnp.dot(
            sten[group], jnp.concatenate(windows, axis=1), preferred_element_type=F32
        ).astype(BF)
        return [out[:, t * lev : (t + 1) * lev].reshape(cols, GR, lev) for t in range(2)]

    def project(k):
        for group in range(groups):
            rows = pl.ds(group * GR, GR)
            first, second = refine_group(k, group)
            fine[k, 0, :, rows, :] = first
            fine[k, 1, :, rows, :] = second
            both = first.astype(F32) * ctrl[pl.ds(0, cols), rows, :].astype(F32)
            both = both + second.astype(F32) * ctrl[pl.ds(cols, cols), rows, :].astype(F32)
            both = both.astype(BF)
            field[k, 1, :, rows, :] = both[:half]
            field[k, 2, :, rows, :] = both[half:]

    def halo_copy(k, side):
        other = block + 1 if side == 0 else block - 1
        return pltpu.make_async_remote_copy(
            src_ref=field.at[k, 2 - side],
            dst_ref=field.at[k, 3 * side],
            send_sem=h_go.at[k, side],
            recv_sem=h_in.at[k, side],
            device_id={"z": z_of(other), "c": other % nc},
            device_id_type=MESH,
        )

    nl, ll = ny, lev // ny

    def hand_columns(i, start, count):
        for j in range(start, start + count):
            for t in range(2):
                turned = acc[t, i * half + j].T.astype(BF)
                for q in range(nl):
                    parts[(t * nxl + i) * ny + q, j] = turned[q * ll : (q + 1) * ll]
        for j in range(start, start + count):
            for t in range(2):
                for q in range(nl):
                    p = (t * nxl + i) * ny + q

                    @pl.when(p != team)
                    def _():
                        pltpu.make_async_remote_copy(
                            src_ref=parts.at[p, j],
                            dst_ref=sums.at[team, j],
                            send_sem=p_go,
                            recv_sem=p_in.at[j],
                            device_id=at_team(p),
                            device_id_type=MESH,
                        ).start()

    sends = (block < blocks - 1, block > 0)
    near = 1 - c
    edge = ((c == 0) & (block == 0)) | ((c == nc - 1) & (block == blocks - 1))

    def localize(k, i, side):
        @pl.when((side == near) | jnp.logical_not(edge))
        def _():
            wait_bytes(field.at[k, 3 * side], h_in.at[k, side])

        @pl.when((side != near) & edge)
        def _():
            field[k, 3 * side] = jnp.zeros(field.shape[2:], BF)

        for group in range(0, groups, 2):
            wide = []
            for g in (group, group + 1):
                rows = pl.ds(g * GR, GR)
                pieces = [field[k, i + n, :, rows, :].reshape(half * GR, lev) for n in range(3)]
                wide.append(jnp.concatenate(pieces, axis=0))
            mixed = jnp.dot(
                bandf[i], jnp.concatenate(wide, axis=1), preferred_element_type=F32
            ).astype(BF)
            for n, g in enumerate((group, group + 1)):
                banded[:, pl.ds(g * GR, GR), :] = mixed[:, n * lev : (n + 1) * lev].reshape(
                    half, GR, lev
                )
        for j in range(0, half, 2):
            pair = jnp.concatenate([banded[j], banded[j + 1]], axis=1)
            mixed = jnp.dot(row_ref[...], pair, preferred_element_type=F32).astype(BF)
            local = jnp.dot(mixed, lev_ref[...], preferred_element_type=F32)
            for n in range(2):
                part = local[:, n * lev : (n + 1) * lev]
                at = i * half + j + n
                for t in range(2):
                    acc[t, at] += fine[k, t, at].astype(F32) * part

            @pl.when(k == nk - 1)
            def _():
                hand_columns(i, j, 2)

    def wait_all_but_one(k, sem):
        wait_bytes(sent.at[k, pl.ds(0, ndest - 1)], sem.at[k])

    dest = block * nxl + xl
    d_block = dest % blocks
    stays = dest == tile

    def finish():
        for j in range(half):
            wait_bytes(sums.at[pl.ds(0, nteam - 1), j], p_in.at[j])
            sums[team, j] = parts[team, j]
            value = sums[0, j].astype(F32)
            for p in range(1, nteam):
                value = value + sums[p, j].astype(F32)
            total[j] = (value * scale).astype(BF)

            @pl.when(jnp.logical_not(stays))
            def _():
                pltpu.make_async_remote_copy(
                    src_ref=total.at[j],
                    dst_ref=moved.at[j],
                    send_sem=m_go,
                    recv_sem=m_in,
                    device_id={"xl": dest // blocks, "z": d_block // nc, "c": d_block % nc},
                    device_id_type=MESH,
                ).start()

            @pl.when(stays)
            def _():
                moved[j] = total[j]

    share = -(-members // (nk - 2))

    def step(k, carry):
        @pl.when(k < nk)
        def _():
            wait_all_but_one(k, s_in)

            @pl.when(k == 0)
            def _():
                wait_bytes(ctrl.at[pl.ds(0, (nteam - 1) * quarter_cols)], f_in)

            project(k)
            for side in range(2):

                @pl.when(sends[side])
                def _():
                    halo_copy(k, side).start()

            @pl.when(k == 1)
            def _():
                gather_system()

            @pl.when(k >= 1)
            def _():
                last = jnp.minimum(k * share, members)
                lax.fori_loop(jnp.minimum((k - 1) * share, members), last, eliminate, 0)

            @pl.when(k == nk - 1)
            def _():
                hand_answer()

        first = (k >= 1) & (k <= nk)

        @pl.when(k >= 1)
        def _():
            localize(
                jnp.where(first, k - 1, k - 1 - nk),
                jnp.where(first, near, 1 - near),
                jnp.where(first, near, 1 - near),
            )

        return carry

    lax.fori_loop(0, 2 * nk + 1, step, 0)

    finish()

    def left(k, carry):
        wait_all_but_one(k, s_go)
        for side in range(2):

            @pl.when(sends[side])
            def _():
                wait_bytes(field.at[k, side], h_go.at[k, side])

        return carry

    lax.fori_loop(0, nk, left, 0)
    wait_bytes(ctrl.at[pl.ds(0, (nteam - 1) * quarter_cols)], f_go)
    wait_bytes(sums.at[pl.ds(0, nteam - 1)], p_go)
    wait_bytes(grams.at[pl.ds(0, nregion - 1)], g_go)
    wait_bytes(answers.at[pl.ds(0, nregion - 1)], w_go)
    wait_bytes(answers.at[pl.ds(0, nregion - 1)], w_in)
    for g in range(nregion):
        w_ref[pl.ds(g, 1), :] = answers[g, :1, :members]
    for side in range(nxl):
        here = (to_z == z) & (to_c == c) & (xl == side)

        @pl.when(jnp.logical_not(here))
        def _():
            wait_bytes(bands.at[side], b_go.at[side])

    @pl.when(jnp.logical_not(stays))
    def _():
        wait_bytes(total, m_go)
        wait_bytes(moved, m_in)

    for j in range(half):
        turned_out[:, j, :] = moved[j].astype(F32)
    o_ref[...] = turned_out[...].astype(BF)


def body(
    ens_coarse,
    col_interp,
    row_weights,
    ctrl_vec,
    band_loc,
    row_loc,
    level_loc,
    hx_pert,
    innov,
    obs_prec,
    obs_region,
):
    nxh, nxl, nz, nc, ny = (lax.axis_size(a) for a in ("xh", "xl", "z", "c", "y"))
    _, members, lev, own_rows, coarse_cols = ens_coarse.shape
    fine_cols = col_interp.shape[0]
    fine_rows = row_weights.shape[1]
    blocks = nz * nc
    cols = fine_cols // blocks
    half = cols // 2
    group = members // (nxh * nxl)
    tiles = nxl * blocks
    coarse = tiles * own_rows
    total_members = hx_pert.shape[1]
    nteam = nxh * nxl * ny
    quarter = half // ny
    lanes = 128

    x = ens_coarse.reshape(members, lev * own_rows, coarse_cols)

    vm = pl.BlockSpec(memory_space=pltpu.VMEM)
    dma = pltpu.SemaphoreType.DMA
    increment, weights = pl.pallas_call(
        lambda *refs: main_kernel((nxh, nxl, nz, nc, ny, 1.0 / (total_members - 1)), refs),
        in_specs=[vm] * 11,
        out_specs=(vm, vm),
        out_shape=(
            jax.ShapeDtypeStruct((lev // ny, half, fine_rows), BF),
            jax.ShapeDtypeStruct((NREG, total_members), F32),
        ),
        scratch_shapes=[
            pltpu.VMEM((quarter, fine_rows, lev), BF),
            pltpu.VMEM((2 * lev, 2 * lev), BF),
            pltpu.VMEM((half, lanes), F32),
            pltpu.VMEM((8, fine_rows), F32),
            pltpu.VMEM((own_rows * lev, own_rows * lev), BF),
            pltpu.VMEM((group, nxh * tiles, own_rows, cols, lev), BF),
            pltpu.VMEM((group, nxh, coarse, cols, lev), BF),
            pltpu.VMEM((fine_rows // GR, cols * GR, WIN * cols), BF),
            pltpu.VMEM((quarter, fine_rows, lev), BF),
            pltpu.VMEM((nxh * cols, fine_rows, lev), BF),
            pltpu.VMEM((2, half, lanes), F32),
            pltpu.VMEM((2, half * GR, 3 * half * GR), BF),
            pltpu.VMEM((group, 4, half, fine_rows, lev), BF),
            pltpu.VMEM((group, nxh, cols, fine_rows, lev), BF),
            pltpu.VMEM((half, fine_rows, lev), BF),
            pltpu.VMEM((nxh, cols, fine_rows, lev), F32),
            pltpu.VMEM((nteam, half, lev // ny, fine_rows), BF),
            pltpu.VMEM((nteam, half, lev // ny, fine_rows), BF),
            pltpu.VMEM((half, lev // ny, fine_rows), BF),
            pltpu.VMEM((half, lev // ny, fine_rows), BF),
            pltpu.VMEM((lev // ny, half, fine_rows), F32),
            pltpu.VMEM((NREG, total_members, lanes), F32),
            pltpu.VMEM((NREG, total_members, lanes), F32),
            pltpu.VMEM((total_members, lanes), F32),
            pltpu.VMEM((8, lanes), F32),
            pltpu.VMEM((NREG, 8, lanes), F32),
            dma((group,)),
            dma((group,)),
            dma((group, 2)),
            dma((group, 2)),
            *[dma] * 4,
            dma((2,)),
            dma((2,)),
            dma,
            dma((half,)),
            *[dma] * 6,
        ],
        compiler_params=pltpu.CompilerParams(
            collective_id=0, has_side_effects=True, vmem_limit_bytes=62 << 20
        ),
    )(x, col_interp, row_weights, ctrl_vec[0], band_loc, row_loc, level_loc, hx_pert[0], innov, obs_prec, obs_region)
    return (increment.astype(F32)[None], weights)


def solution(mesh):
    shape = (2, 2, mesh.shape["tile"] // 4, 2, mesh.shape["mem"])
    fine_mesh = Mesh(mesh.devices.reshape(shape), ("xh", "xl", "z", "c", "y"))
    tile = ("xl", "z", "c")
    obs = (*tile, "y")
    placed = (
        P("xh", "y", None, tile, None),
        P(),
        P(),
        P("xh", None, tile, None),
        P(tile, None),
        P(),
        P(),
        P("xh", None, obs),
        P("xh", obs),
        P("xh", obs),
        P("xh", obs),
    )
    return jax.shard_map(
        body,
        mesh=fine_mesh,
        in_specs=placed,
        out_specs=(P("xh", "y", tile, None), P(tile, None)),
        check_vma=False,
    )
```
